32 devices in a mesh: ctx: 8 (over z, x), wsh: 4 (over y, core).
Axes of the slice: x: 2, y: 2, z: 4, core: 2. Of those that a mesh axis runs over, the one named last changes fastest.
Arguments:
- inputs: bfloat16 [2048, 2, 2048], P(('ctx', 'wsh')), may hold values from -6 to 6
- pair_map: int32 [8], replicated, may hold values from 0 to 7, each once
- norm_gain: float32 [2048], replicated, may hold values from 0.25 to 1.75
- query_weight: bfloat16 [2048, 4096], P('ctx', 'wsh'), may hold values from -0.125 to 0.125
- key_weight: bfloat16 [2048, 512], P('ctx', 'wsh'), may hold values from -0.125 to 0.125
- value_weight: bfloat16 [2048, 512], P('ctx', 'wsh'), may hold values from -0.125 to 0.125
- query_gain: float32 [128], replicated, may hold values from 0.5 to 2
- key_gain: float32 [128], replicated, may hold values from 0.5 to 2
- out_weight: bfloat16 [4096, 2048], P('wsh', 'ctx'), may hold values from -3 to 3
- moe_gain: float32 [2048], replicated, may hold values from 0.25 to 1.75
- router: bfloat16 [2048, 32], replicated
- expert_gate: bfloat16 [32, 2048, 768], P(('ctx', 'wsh')), may hold values from -0.125 to 0.125
- expert_up: bfloat16 [32, 2048, 768], P(('ctx', 'wsh')), may hold values from -0.125 to 0.125
- expert_down: bfloat16 [32, 768, 2048], P(('ctx', 'wsh')), may hold values from -0.21875 to 0.21875
- expert_ids: int32 [2048, 2, 8], P(('ctx', 'wsh')), may hold values from 0 to 31, as said below
- dispatch_slot: int32 [2048, 2, 8], P(('ctx', 'wsh')), may hold values from -1 to 47, as said below
- cotangent: float32 [2048, 2, 2048], P(('ctx', 'wsh')), may hold values from -6 to 6
Outputs:
- outputs: bfloat16 [2048, 2, 2048], P(('ctx', 'wsh'))
- input_grad: float32 [2048, 2, 2048], P(('ctx', 'wsh'))
- norm_gain_grad: float32 [2048], replicated
- query_weight_grad: float32 [2048, 4096], P('ctx', 'wsh')
- key_weight_grad: float32 [2048, 512], P('ctx', 'wsh')
- value_weight_grad: float32 [2048, 512], P('ctx', 'wsh')
- query_gain_grad: float32 [128], replicated
- key_gain_grad: float32 [128], replicated
- out_weight_grad: float32 [4096, 2048], P('wsh', 'ctx')
- moe_gain_grad: float32 [2048], replicated
- router_grad: float32 [2048, 32], replicated
- gate_grad: float32 [32, 2048, 768], P(('ctx', 'wsh'))
- up_grad: float32 [32, 2048, 768], P(('ctx', 'wsh'))
- down_grad: float32 [32, 768, 2048], P(('ctx', 'wsh'))
The draws below stay inside these ranges and needn't reach their ends.
Inputs may be any that keep to these rules, and one draw needn't show every extreme that they name: `expert_ids`: each token names 8 different experts; in every draw one expert is named by every token. `dispatch_slot`: among the routes of the rows of one device to one expert, in token order, the first 48 hold the slots 0, 1, ... in that order and the others hold -1; in every draw some expert gets 48 routes from the rows of every device.
All inputs are finite; a program needn't handle non-finite values.
Results may differ from the reference program's by a relative error of at most 0.02.
Values may be sent and summed in bfloat16 or wider, within the bound.
A program may use at most 256 MiB of HBM per device.

```python
import math
import jax
import jax.numpy as jnp
from jax import lax

D = 2048
H = 32
KV = 4
HD = 128
FF = 768
TOPK = 8
NSEQ = 2
BLK = 128
SEQ = 2048
EXPERTS = 32
CAPS = 48
N_CTX = 8
N_WSH = 4


def routing_table(key):
    device_count = N_CTX * N_WSH
    per_device = SEQ * NSEQ // device_count
    level = jax.random.randint(jax.random.fold_in(key, 11), (device_count, 1, EXPERTS), 0, 4)
    local_hot = jax.random.randint(jax.random.fold_in(key, 12), (device_count, 1, 1), 0, EXPERTS)
    global_hot = jax.random.randint(jax.random.fold_in(key, 13), (1, 1, 1), 0, EXPERTS)
    noise = jax.random.randint(jax.random.fold_in(key, 14), (device_count, per_device, EXPERTS), 0, 4096)
    column = jnp.arange(EXPERTS, dtype=jnp.int32)[None, None, :]
    offset = level * 512 + jnp.where(column == local_hot, 65536, 0) + jnp.where(column == global_hot, 65536, 0)
    scores = (offset + noise) * EXPERTS + column
    chosen = lax.top_k(scores, TOPK)[1].astype(jnp.int32)
    onehot = (chosen[..., None] == column[:, None]).astype(jnp.int32)
    flat_hot = onehot.reshape(device_count, per_device * TOPK, EXPERTS)
    earlier = jnp.cumsum(flat_hot, axis=1) - flat_hot
    slot_rank = jnp.sum(earlier * flat_hot, axis=-1).reshape(device_count, per_device, TOPK)
    slot_rank = jnp.where(slot_rank < CAPS, slot_rank, -1).astype(jnp.int32)
    return (chosen.reshape(SEQ, NSEQ, TOPK), slot_rank.reshape(SEQ, NSEQ, TOPK))


def draw_expert_ids(key, part):
    return routing_table(key)[0]


def draw_dispatch_slot(key, part):
    return routing_table(key)[1]


def head_gain(key):
    return jnp.exp(jax.random.uniform(key, (HD,), jnp.float32, math.log(0.5), math.log(2.0)))


def draw_query_gain(key, part):
    return head_gain(jax.random.fold_in(key, 21))


def draw_key_gain(key, part):
    return head_gain(jax.random.fold_in(key, 22))


def draw_router(key, part):
    base = jnp.clip(jax.random.normal(jax.random.fold_in(key, 31), (D, EXPERTS), jnp.float32), -4.0, 4.0) * D ** (-0.5)
    return base.astype(jnp.bfloat16)


def shard_levels(key, dims, cuts, smallest, top_value):
    def one(position, blocks):
        heights = jax.random.uniform(jax.random.fold_in(jax.random.fold_in(key, 6), position), (blocks,), jnp.float32, smallest / len(cuts), top_value / len(cuts))
        return jnp.repeat(jnp.exp(heights), dims[position] // blocks).reshape((-1,) + (1,) * (len(dims) - position - 1))

    loudness = one(*cuts[0])
    for cut in cuts[1:]:
        loudness = loudness * one(*cut)
    return loudness


def gaussian(rng, extent, width, reach, split=(), kind=jnp.bfloat16):
    array = jax.random.normal(rng, extent, jnp.float32) * width
    if len(split) > 0:
        array = shard_levels(rng, extent, split, -0.22, 0.18) * array
    return jnp.clip(array, min=-reach, max=reach).astype(kind)


def setup_inputs(seed: int = 0) -> dict:
    key_of = jax.random.split(jax.random.key(seed), 18)
    return {
        "inputs": gaussian(key_of[0], (SEQ, NSEQ, D), 1.0, 6.0, ((0, 32),)),
        "pair_map": jax.random.permutation(key_of[1], N_CTX).astype(jnp.int32),
        "norm_gain": jnp.clip(1.0 + 0.15 * jax.random.normal(key_of[2], (D,), jnp.float32), 0.25, 1.75),
        "query_weight": gaussian(key_of[3], (D, H * HD), D ** -0.5, 0.125, ((0, 8), (1, 4))),
        "key_weight": gaussian(key_of[4], (D, KV * HD), D ** -0.5, 0.125, ((0, 8), (1, 4))),
        "value_weight": gaussian(key_of[5], (D, KV * HD), D ** -0.5, 0.125, ((0, 8), (1, 4))),
        "query_gain": draw_query_gain(jax.random.fold_in(key_of[17], 71), 0),
        "key_gain": draw_key_gain(jax.random.fold_in(key_of[17], 71), 0),
        "out_weight": gaussian(key_of[8], (H * HD, D), (max(1, H * HD // 1024)) ** -0.5, 3.0, ((0, 4), (1, 8))),
        "moe_gain": jnp.clip(1.0 + 0.15 * jax.random.normal(key_of[9], (D,), jnp.float32), 0.25, 1.75),
        "router": draw_router(jax.random.fold_in(key_of[17], 71), 0),
        "expert_gate": gaussian(key_of[11], (EXPERTS, D, FF), D ** -0.5, 0.125, ((0, 32),)),
        "expert_up": gaussian(key_of[12], (EXPERTS, D, FF), D ** -0.5, 0.125, ((0, 32),)),
        "expert_down": gaussian(key_of[13], (EXPERTS, FF, D), FF ** -0.5, 0.21875, ((0, 32),)),
        "expert_ids": draw_expert_ids(jax.random.fold_in(key_of[17], 71), 0),
        "dispatch_slot": draw_dispatch_slot(jax.random.fold_in(key_of[17], 71), 0),
        "cotangent": gaussian(key_of[16], (SEQ, NSEQ, D), 1.0, 6.0, ((0, 32),), jnp.float32),
    }


EPSILON = 1e-06
ROPE_BASE = 1000000.0
MASKED = -1e+30

def rounded(tensor):
    return lax.optimization_barrier(tensor.astype(jnp.bfloat16)).astype(jnp.float32)

def positions_of(pair_map, seq_len, block_len, group_count):
    row_index = jnp.arange(seq_len, dtype=jnp.int32)
    owner_group = row_index // (2 * block_len)
    inner_row = row_index % (2 * block_len)
    group_table = jnp.arange(group_count, dtype=jnp.int32)
    pair_index = lax.optimization_barrier(jnp.sum(jnp.where(owner_group[:, None] == group_table[None, :], pair_map[None, :], 0), axis=1)).astype(jnp.int32)
    block_index = jnp.where(inner_row < block_len, pair_index, 2 * group_count - 1 - pair_index)
    return (block_index * block_len + inner_row % block_len).astype(jnp.int32)

def rope_tables(positions, head_dim):
    half_dim = head_dim // 2
    frequency = ROPE_BASE ** (-(jnp.arange(half_dim, dtype=jnp.float32) * 2.0) / head_dim)
    angles = positions.astype(jnp.float32)[:, None] * frequency[None, :]
    return (jnp.cos(angles), jnp.sin(angles))

def rotate(tensor, cosine, sine_table):
    half_dim = tensor.shape[-1] // 2
    first_half = tensor[..., :half_dim]
    second_half = tensor[..., half_dim:]
    return jnp.concatenate([first_half * cosine - second_half * sine_table, second_half * cosine + first_half * sine_table], axis=-1)

def unrotate(gradient, cosine, sine_table):
    half_dim = gradient.shape[-1] // 2
    first_half = gradient[..., :half_dim]
    second_half = gradient[..., half_dim:]
    return jnp.concatenate([first_half * cosine + second_half * sine_table, second_half * cosine - first_half * sine_table], axis=-1)

def rms_forward(tensor, gain_vector):
    inverse = lax.rsqrt(lax.optimization_barrier(jnp.mean(tensor * tensor, axis=-1, keepdims=True)) + EPSILON)
    return (tensor * inverse * gain_vector, inverse)

def rms_backward(tensor, inverse, gain_vector, gradient):
    weighted = gradient * gain_vector
    inner_mean = lax.optimization_barrier(jnp.mean(weighted * tensor, axis=-1, keepdims=True))
    tensor_grad = inverse * weighted - tensor * inverse ** 3 * inner_mean
    gain_grad = lax.optimization_barrier(jnp.sum((gradient * tensor * inverse).reshape(-1, tensor.shape[-1]), axis=0))
    return (tensor_grad, gain_grad)

def expert_forward(rows_in, gate_w, up_w, down_w):
    gate_pre = jnp.dot(rows_in, gate_w, preferred_element_type=jnp.float32)
    up_pre = jnp.dot(rows_in, up_w, preferred_element_type=jnp.float32)
    activation = (gate_pre * jax.nn.sigmoid(gate_pre) * up_pre).astype(jnp.bfloat16)
    return jnp.dot(activation, down_w, preferred_element_type=jnp.float32).astype(jnp.bfloat16)

def expert_backward(rows_in, route_cot, gate_w, up_w, down_w):
    gate_pre = jnp.dot(rows_in, gate_w, preferred_element_type=jnp.float32)
    up_pre = jnp.dot(rows_in, up_w, preferred_element_type=jnp.float32)
    sigmoid = jax.nn.sigmoid(gate_pre)
    swish = gate_pre * sigmoid
    activation = (swish * up_pre).astype(jnp.bfloat16)
    down_grad = jnp.dot(activation.T, route_cot, preferred_element_type=jnp.float32)
    act_cot = jnp.dot(route_cot, down_w.T, preferred_element_type=jnp.float32)
    gate_cot = (act_cot * up_pre * sigmoid * (1.0 + gate_pre * (1.0 - sigmoid))).astype(jnp.bfloat16)
    up_cot = (act_cot * swish).astype(jnp.bfloat16)
    gate_grad = jnp.dot(rows_in.T, gate_cot, preferred_element_type=jnp.float32)
    up_grad = jnp.dot(rows_in.T, up_cot, preferred_element_type=jnp.float32)
    row_cot = jnp.dot(gate_cot, gate_w.T, preferred_element_type=jnp.float32) + jnp.dot(up_cot, up_w.T, preferred_element_type=jnp.float32)
    return (row_cot.astype(jnp.bfloat16), gate_grad, up_grad, down_grad)

def attend_forward(query_rows, key_rows, value_rows, positions):
    query_block = math.gcd(SEQ, 512)
    block_count = SEQ // query_block
    scaling = HD ** (-0.5)
    key_float = key_rows.astype(jnp.float32)
    value_float = value_rows.astype(jnp.float32)

    def one_block(block_id):
        start = block_id * query_block
        query_part = lax.dynamic_slice_in_dim(query_rows, start, query_block, 0).astype(jnp.float32)
        query_pos = lax.dynamic_slice_in_dim(positions, start, query_block, 0)
        scores = jnp.einsum('qgd,kd->gqk', query_part, key_float) * scaling
        allowed = positions[None, None, :] <= query_pos[None, :, None]
        row_top = lax.optimization_barrier(jnp.max(jnp.where(allowed, scores, MASKED), axis=-1, keepdims=True))
        expo = jnp.where(allowed, jnp.exp(scores - row_top), 0.0)
        row_total = lax.optimization_barrier(jnp.sum(expo, axis=-1, keepdims=True))
        mixed = jnp.einsum('gqk,kd->gqd', rounded(expo), value_float) / row_total
        log_total = (row_top + jnp.log(row_total))[..., 0]
        return (jnp.transpose(mixed, (1, 0, 2)).astype(jnp.bfloat16), jnp.transpose(log_total, (1, 0)))
    outcome, log_totals = lax.map(one_block, jnp.arange(block_count, dtype=jnp.int32))
    heads = query_rows.shape[1]
    return (outcome.reshape(SEQ, heads, HD), log_totals.reshape(SEQ, heads))

def attend_backward(query_rows, key_rows, value_rows, attn_rows, attn_cot, log_totals, positions):
    query_block = math.gcd(SEQ, 512)
    block_count = SEQ // query_block
    scaling = HD ** (-0.5)
    key_float = key_rows.astype(jnp.float32)
    value_float = value_rows.astype(jnp.float32)

    def one_block(carry, block_id):
        key_cot, value_cot = carry
        start = block_id * query_block
        query_part = lax.dynamic_slice_in_dim(query_rows, start, query_block, 0).astype(jnp.float32)
        query_pos = lax.dynamic_slice_in_dim(positions, start, query_block, 0)
        out_part = lax.dynamic_slice_in_dim(attn_rows, start, query_block, 0).astype(jnp.float32)
        cot_part = lax.dynamic_slice_in_dim(attn_cot, start, query_block, 0).astype(jnp.float32)
        log_part = jnp.transpose(lax.dynamic_slice_in_dim(log_totals, start, query_block, 0), (1, 0))
        scores = jnp.einsum('qgd,kd->gqk', query_part, key_float) * scaling
        allowed = positions[None, None, :] <= query_pos[None, :, None]
        weights_back = jnp.where(allowed, jnp.exp(scores - log_part[..., None]), 0.0)
        prob_cot = jnp.einsum('qgd,kd->gqk', cot_part, value_float)
        delta = jnp.transpose(lax.optimization_barrier(jnp.sum(cot_part * out_part, axis=-1)), (1, 0))
        score_cot = weights_back * (prob_cot - delta[..., None])
        value_cot = value_cot + jnp.einsum('gqk,qgd->kd', rounded(weights_back), cot_part)
        score_low = rounded(score_cot)
        query_cot = jnp.einsum('gqk,kd->qgd', score_low, key_float) * scaling
        key_cot = key_cot + jnp.einsum('gqk,qgd->kd', score_low, query_part) * scaling
        return ((key_cot, value_cot), query_cot)
    start_carry = (jnp.zeros((SEQ, HD), jnp.float32), jnp.zeros((SEQ, HD), jnp.float32))
    (key_cot, value_cot), query_cot = lax.scan(one_block, start_carry, jnp.arange(block_count, dtype=jnp.int32))
    heads = query_rows.shape[1]
    return (query_cot.reshape(SEQ, heads, HD), key_cot, value_cot)

def reference(inputs, pair_map, norm_gain, query_weight, key_weight, value_weight, query_gain, key_gain, out_weight, moe_gain, router, expert_gate, expert_up, expert_down, expert_ids, dispatch_slot, cotangent):
    group = H // KV
    tokens = SEQ * NSEQ
    device_count = N_CTX * N_WSH
    per_device = tokens // device_count
    positions = positions_of(pair_map, SEQ, BLK, N_CTX)
    cosine, sine_table = rope_tables(positions, HD)
    cosine = cosine[:, None, None, :]
    sine_table = sine_table[:, None, None, :]
    inputs_f = inputs.astype(jnp.float32)
    normed_f, inverse_one = rms_forward(inputs_f, norm_gain)
    normed = normed_f.astype(jnp.bfloat16)
    normed_flat = normed.reshape(tokens, D)
    queries = jnp.dot(normed_flat, query_weight, preferred_element_type=jnp.float32).reshape(SEQ, NSEQ, H, HD)
    keys_raw = jnp.dot(normed_flat, key_weight, preferred_element_type=jnp.float32).reshape(SEQ, NSEQ, KV, HD)
    value_rows = jnp.dot(normed_flat, value_weight, preferred_element_type=jnp.float32).astype(jnp.bfloat16).reshape(SEQ, NSEQ, KV, HD)
    query_normed, query_inverse = rms_forward(queries, query_gain)
    key_normed, key_inverse = rms_forward(keys_raw, key_gain)
    query_rot = rotate(query_normed, cosine, sine_table).astype(jnp.bfloat16)
    key_rot = rotate(key_normed, cosine, sine_table).astype(jnp.bfloat16)
    attn_seqs, log_seqs = ([], [])
    for seq_index in range(NSEQ):
        attn_heads, log_heads = ([], [])
        for head_index in range(KV):
            outcome, log_totals = attend_forward(query_rot[:, seq_index, head_index * group:(head_index + 1) * group], key_rot[:, seq_index, head_index], value_rows[:, seq_index, head_index], positions)
            attn_heads.append(outcome)
            log_heads.append(log_totals)
        attn_seqs.append(jnp.concatenate(attn_heads, axis=1))
        log_seqs.append(jnp.concatenate(log_heads, axis=1))
    attention = jnp.stack(attn_seqs, axis=1)
    attention_flat = attention.reshape(tokens, H * HD)
    residual = inputs_f + jnp.dot(attention_flat, out_weight, preferred_element_type=jnp.float32).reshape(SEQ, NSEQ, D)
    moe_normed_f, inverse_two = rms_forward(residual, moe_gain)
    moe_flat = moe_normed_f.astype(jnp.bfloat16).reshape(tokens, D)
    logits = jnp.dot(moe_flat, router, preferred_element_type=jnp.float32)
    route_ids = expert_ids.reshape(tokens, TOPK)
    slots = dispatch_slot.reshape(tokens, TOPK)
    expert_onehot = route_ids[:, :, None] == jnp.arange(EXPERTS, dtype=jnp.int32)[None, None, :]
    chosen = lax.optimization_barrier(jnp.sum(jnp.where(expert_onehot, logits[:, None, :], 0.0), axis=-1))
    chosen_top = lax.optimization_barrier(jnp.max(chosen, axis=-1, keepdims=True))
    chosen_exp = jnp.exp(chosen - chosen_top)
    route_weight = chosen_exp / lax.optimization_barrier(jnp.sum(chosen_exp, axis=-1, keepdims=True))
    slot_count = device_count * CAPS
    route_total = tokens * TOPK
    kept_route = slots >= 0
    source_device = (jnp.arange(tokens, dtype=jnp.int32) // per_device)[:, None]
    placement = jnp.where(kept_route, route_ids * slot_count + source_device * CAPS + slots, EXPERTS * slot_count).astype(jnp.int32)
    route_table = jnp.full((EXPERTS * slot_count,), route_total, jnp.int32)
    route_table = route_table.at[placement.reshape(-1)].set(jnp.arange(route_total, dtype=jnp.int32), mode='drop')
    route_table = route_table.reshape(EXPERTS, slot_count)
    normed_pad = jnp.concatenate([moe_flat, jnp.zeros((1, D), jnp.bfloat16)], axis=0)
    cot_flat = cotangent.reshape(tokens, D)
    cot_pad = jnp.concatenate([cot_flat, jnp.zeros((1, D), jnp.float32)], axis=0)
    weight_pad = jnp.concatenate([route_weight.reshape(-1), jnp.zeros((1,), jnp.float32)], axis=0)

    def expert_pass(carry, operands):
        moe_sum, weight_cot = carry
        routes, gate_w, up_w, down_w = operands
        token_rows = routes // TOPK
        produced = expert_forward(normed_pad[token_rows], gate_w, up_w, down_w).astype(jnp.float32)
        moe_sum = moe_sum.at[token_rows].add(weight_pad[routes][:, None] * produced, mode='drop')
        weight_cot = weight_cot.at[routes].set(lax.optimization_barrier(jnp.sum(cot_pad[token_rows] * produced, axis=-1)), mode='drop')
        return ((moe_sum, weight_cot), None)
    start_carry = (jnp.zeros((tokens, D), jnp.float32), jnp.zeros((route_total,), jnp.float32))
    (moe_sum, weight_cot), _ = lax.scan(expert_pass, start_carry, (route_table, expert_gate, expert_up, expert_down))
    outputs = (residual.reshape(tokens, D) + moe_sum).reshape(SEQ, NSEQ, D).astype(jnp.bfloat16)
    weight_cot = weight_cot.reshape(tokens, TOPK)
    chosen_cot = route_weight * (weight_cot - lax.optimization_barrier(jnp.sum(route_weight * weight_cot, axis=-1, keepdims=True)))
    logit_cot = lax.optimization_barrier(jnp.sum(jnp.where(expert_onehot, chosen_cot[:, :, None], 0.0), axis=1)).astype(jnp.bfloat16)
    router_grad = jnp.dot(moe_flat.T, logit_cot, preferred_element_type=jnp.float32)
    normed_two_cot = jnp.dot(logit_cot, router.T, preferred_element_type=jnp.float32)

    def expert_back(carry, operands):
        routes, gate_w, up_w, down_w = operands
        token_rows = routes // TOPK
        route_cot = (weight_pad[routes][:, None] * cot_pad[token_rows]).astype(jnp.bfloat16)
        row_cot, gate_grad, up_grad, down_grad = expert_backward(normed_pad[token_rows], route_cot, gate_w, up_w, down_w)
        carry = carry.at[token_rows].add(row_cot.astype(jnp.float32), mode='drop')
        return (carry, (gate_grad, up_grad, down_grad))
    normed_two_cot, (gate_grad, up_grad, down_grad) = lax.scan(expert_back, normed_two_cot, (route_table, expert_gate, expert_up, expert_down))
    residual_norm_cot, moe_gain_grad = rms_backward(residual, inverse_two, moe_gain, normed_two_cot.reshape(SEQ, NSEQ, D))
    residual_cot = cotangent + residual_norm_cot
    residual_low = residual_cot.astype(jnp.bfloat16).reshape(tokens, D)
    out_weight_grad = jnp.dot(attention_flat.T, residual_low, preferred_element_type=jnp.float32)
    attention_cot = jnp.dot(residual_low, out_weight.T, preferred_element_type=jnp.float32).astype(jnp.bfloat16).reshape(SEQ, NSEQ, H, HD)
    query_seqs, key_seqs, value_seqs = ([], [], [])
    for seq_index in range(NSEQ):
        query_heads, key_heads, value_heads = ([], [], [])
        for head_index in range(KV):
            head_slice = slice(head_index * group, (head_index + 1) * group)
            query_part, key_part, value_part = attend_backward(query_rot[:, seq_index, head_slice], key_rot[:, seq_index, head_index], value_rows[:, seq_index, head_index], attention[:, seq_index, head_slice], attention_cot[:, seq_index, head_slice], log_seqs[seq_index][:, head_slice], positions)
            query_heads.append(query_part)
            key_heads.append(key_part)
            value_heads.append(value_part)
        query_seqs.append(jnp.concatenate(query_heads, axis=1))
        key_seqs.append(jnp.stack(key_heads, axis=1))
        value_seqs.append(jnp.stack(value_heads, axis=1))
    query_rot_cot = jnp.stack(query_seqs, axis=1)
    key_rot_cot = jnp.stack(key_seqs, axis=1)
    value_cot = jnp.stack(value_seqs, axis=1)
    query_cot, query_gain_grad = rms_backward(queries, query_inverse, query_gain, unrotate(query_rot_cot, cosine, sine_table))
    key_cot, key_gain_grad = rms_backward(keys_raw, key_inverse, key_gain, unrotate(key_rot_cot, cosine, sine_table))
    query_low = query_cot.astype(jnp.bfloat16).reshape(tokens, H * HD)
    key_low = key_cot.astype(jnp.bfloat16).reshape(tokens, KV * HD)
    value_low = value_cot.astype(jnp.bfloat16).reshape(tokens, KV * HD)
    query_weight_grad = jnp.dot(normed_flat.T, query_low, preferred_element_type=jnp.float32)
    key_weight_grad = jnp.dot(normed_flat.T, key_low, preferred_element_type=jnp.float32)
    value_weight_grad = jnp.dot(normed_flat.T, value_low, preferred_element_type=jnp.float32)
    normed_cot = jnp.dot(query_low, query_weight.T, preferred_element_type=jnp.float32)
    normed_cot = normed_cot + jnp.dot(key_low, key_weight.T, preferred_element_type=jnp.float32)
    normed_cot = normed_cot + jnp.dot(value_low, value_weight.T, preferred_element_type=jnp.float32)
    input_norm_cot, norm_gain_grad = rms_backward(inputs_f, inverse_one, norm_gain, normed_cot.reshape(SEQ, NSEQ, D))
    input_grad = residual_cot + input_norm_cot
    return (outputs, input_grad, norm_gain_grad, query_weight_grad, key_weight_grad, value_weight_grad, query_gain_grad, key_gain_grad, out_weight_grad, moe_gain_grad, router_grad, gate_grad, up_grad, down_grad)
```

```python
import functools
import math

import jax
import jax.numpy as jnp
from jax import lax
from jax.experimental import pallas as pl
from jax.experimental.pallas import tpu as pltpu
from jax.sharding import PartitionSpec as P

EPSILON = 1e-06
ROPE_BASE = 1000000.0
MASKED = -1e30


def positions_of(pair_map, seq_len, block_len, group_count):
    row_index = jnp.arange(seq_len, dtype=jnp.int32)
    owner_group = row_index // (2 * block_len)
    inner_row = row_index % (2 * block_len)
    group_table = jnp.arange(group_count, dtype=jnp.int32)
    pair_index = jnp.sum(
        jnp.where(owner_group[:, None] == group_table[None, :], pair_map[None, :], 0), axis=1
    )
    block_index = jnp.where(inner_row < block_len, pair_index, 2 * group_count - 1 - pair_index)
    return block_index * block_len + inner_row % block_len


def rope_tables(positions, head_dim):
    half_dim = head_dim // 2
    frequency = ROPE_BASE ** (-(jnp.arange(half_dim, dtype=jnp.float32) * 2.0) / head_dim)
    angles = positions.astype(jnp.float32)[:, None] * frequency[None, :]
    return (jnp.cos(angles), jnp.sin(angles))


def rotate(tensor, cosine, sine_table):
    half_dim = tensor.shape[-1] // 2
    first_half = tensor[..., :half_dim]
    second_half = tensor[..., half_dim:]
    return jnp.concatenate(
        [
            first_half * cosine - second_half * sine_table,
            second_half * cosine + first_half * sine_table,
        ],
        axis=-1,
    )


def unrotate(gradient, cosine, sine_table):
    half_dim = gradient.shape[-1] // 2
    first_half = gradient[..., :half_dim]
    second_half = gradient[..., half_dim:]
    return jnp.concatenate(
        [
            first_half * cosine + second_half * sine_table,
            second_half * cosine - first_half * sine_table,
        ],
        axis=-1,
    )


def rms_forward(tensor, gain_vector):
    inverse = lax.rsqrt(jnp.mean(tensor * tensor, axis=-1, keepdims=True) + EPSILON)
    return (tensor * inverse * gain_vector, inverse)


def rms_backward(tensor, inverse, gain_vector, gradient):
    weighted = gradient * gain_vector
    inner_mean = jnp.mean(weighted * tensor, axis=-1, keepdims=True)
    tensor_grad = inverse * weighted - tensor * inverse**3 * inner_mean
    gain_grad = jnp.sum((gradient * tensor * inverse).reshape(-1, tensor.shape[-1]), axis=0)
    return (tensor_grad, gain_grad)


MESH_ID = pl.DeviceIdType.MESH


class Place:
    def __init__(self, nz, ux, uy, uc):
        ci, wi = lax.axis_index("ctx"), lax.axis_index("wsh")
        self.nz, self.ux, self.uy, self.uc = nz, ux, uy, uc
        self.z, self.x, self.y, self.c = ci // 2, ci % 2, wi // 2, wi % 2

    def dev(self, z, x, y, c):
        return (z * 2 + x, y * 2 + c)

    def blk(self, z, x, y, c):
        if self.ux and self.uc:
            return (z * 2 + x) * 4 + y * 2 + c
        if self.ux:
            return z * 2 + x
        return y * 2 + c

    def greet(self):
        z, x, y, c, nz = self.z, self.x, self.y, self.c, self.nz
        barrier = pltpu.get_barrier_semaphore()
        count = 0
        if nz > 1:
            for step in (-1, 1):
                ok = jnp.logical_and(z + step >= 0, z + step < nz)

                @pl.when(ok)
                def _():
                    pl.semaphore_signal(
                        barrier, inc=1, device_id=self.dev(z + step, x, y, c), device_id_type=MESH_ID
                    )

                count = count + ok.astype(jnp.int32)
        for use, place in (
            (self.ux, (z, 1 - x, y, c)),
            (self.uy, (z, x, 1 - y, c)),
            (self.uc, (z, x, y, 1 - c)),
        ):
            if use:
                pl.semaphore_signal(
                    barrier, inc=1, device_id=self.dev(*place), device_id_type=MESH_ID
                )
                count = count + 1
        pl.semaphore_wait(barrier, count)

    def line_steps(self):
        steps = [(0, 0, self.z, None)]
        for d in range(1, self.nz):
            steps.append((d, 0, self.z - d, self.z - d >= 0))
            steps.append((d, 1, self.z + d, self.z + d < self.nz))
        return steps


def when(cond, fn):
    if cond is None:
        fn()
    else:
        pl.when(cond)(fn)


def ag_kernel(nz, ux, uy, uc, x_ref, o_ref, ssem, rsem, lsem):
    pc = Place(nz, ux, uy, uc)
    z, x, y, c = pc.z, pc.x, pc.y, pc.c
    rows = x_ref.shape[0]
    half = rows // 2
    pc.greet()
    to_x, to_y, to_c = pc.dev(z, 1 - x, y, c), pc.dev(z, x, 1 - y, c), pc.dev(z, x, y, 1 - c)

    def part(b, p):
        if p == 0:
            return o_ref.at[b]
        return o_ref.at[b, pl.ds((p - 1) * half, half)]

    def sid(d, side, kind):
        return (d * 2 + side) * 10 + kind

    def copy(b, p, sidx, ridx, device, src=None):
        return pltpu.make_async_remote_copy(
            src_ref=part(b, p) if src is None else src,
            dst_ref=part(b, p),
            send_sem=ssem.at[sidx],
            recv_sem=rsem.at[ridx],
            device_id=device,
            device_id_type=MESH_ID,
        )

    own = pltpu.make_async_copy(x_ref, o_ref.at[pc.blk(z, x, y, c)], lsem)
    own.start()

    def hops(d, side, s):
        out = []
        if nz > 1:
            b = pc.blk(s, x, y, c)
            src = x_ref if d == 0 else None
            if d == 0 or side == 0:
                if d + 1 < nz:
                    out.append(
                        (z + 1 < nz, copy(b, 0, sid(d, 0, 0), sid(d + 1, 0, 0), pc.dev(z + 1, x, y, c), src))
                    )
            if d == 0 or side == 1:
                if d + 1 < nz:
                    out.append(
                        (z >= 1, copy(b, 0, sid(d, 1, 0), sid(d + 1, 1, 0), pc.dev(z - 1, x, y, c), src))
                    )
        return out

    def spread(d, side, s):
        b = pc.blk(s, x, y, c)
        src = x_ref if d == 0 else None
        out = []
        if ux:
            out.append(copy(b, 0, sid(d, side, 1), sid(d, side, 1), to_x, src))
        if uy:
            out.append(copy(b, 0, sid(d, side, 2), sid(d, side, 2), to_y, src))
        if uc:
            out.append(copy(b, 0, sid(d, side, 5), sid(d, side, 5), to_c, src))
        return out

    def passed(d, side, s):
        out = []
        if ux:
            b = pc.blk(s, 1 - x, y, c)
            arrive = copy(b, 0, sid(d, side, 1), sid(d, side, 1), to_x)
            go = []
            if uy:
                go.append(copy(b, 1, sid(d, side, 3), sid(d, side, 3), to_y))
            if uc:
                go.append(copy(b, 0, sid(d, side, 6), sid(d, side, 6), to_c))
            out.append((arrive, go))
        if uy:
            b = pc.blk(s, x, 1 - y, c)
            arrive = copy(b, 0, sid(d, side, 2), sid(d, side, 2), to_y)
            go = []
            if ux:
                go.append(copy(b, 2, sid(d, side, 4), sid(d, side, 4), to_x))
            if uc:
                go.append(copy(b, 0, sid(d, side, 7), sid(d, side, 7), to_c))
            out.append((arrive, go))
        return out

    def across(d, side, s):
        out = []
        if ux and uy:
            b = pc.blk(s, 1 - x, 1 - y, c)
            arrive = copy(b, 1, sid(d, side, 3), sid(d, side, 3), to_y)
            go = [copy(b, 1, sid(d, side, 8), sid(d, side, 8), to_c)] if uc else []
            out.append((arrive, go))
            arrive = copy(b, 2, sid(d, side, 4), sid(d, side, 4), to_x)
            go = [copy(b, 2, sid(d, side, 9), sid(d, side, 9), to_c)] if uc else []
            out.append((arrive, go))
        return out

    def partner(d, side, s):
        out = []
        if uc:
            out.append(copy(pc.blk(s, x, y, 1 - c), 0, 0, sid(d, side, 5), to_c))
            if ux:
                out.append(copy(pc.blk(s, 1 - x, y, 1 - c), 0, 0, sid(d, side, 6), to_c))
            if uy:
                out.append(copy(pc.blk(s, x, 1 - y, 1 - c), 0, 0, sid(d, side, 7), to_c))
            if ux and uy:
                b = pc.blk(s, 1 - x, 1 - y, 1 - c)
                out.append(copy(b, 1, 0, sid(d, side, 8), to_c))
                out.append(copy(b, 2, 0, sid(d, side, 9), to_c))
        return out

    steps = pc.line_steps()

    def do_line(step):
        d, side, s, ok = step

        def fn():
            if d > 0:
                copy(pc.blk(s, x, y, c), 0, 0, sid(d, side, 0), to_x).wait_recv()
            for cond, cp in hops(d, side, s):
                when(cond, cp.start)
            for cp in spread(d, side, s):
                cp.start()

        when(ok, fn)

    def do_pass(step, which):
        d, side, s, ok = step

        def fn():
            for arrive, go in which(d, side, s):
                arrive.wait_recv()
                for cp in go:
                    cp.start()

        when(ok, fn)

    groups = [[st for st in steps if st[0] == d] for d in range(nz)]
    for t in range(nz + 2):
        if t < nz:
            for st in groups[t]:
                do_line(st)
        if 0 <= t - 1 < nz:
            for st in groups[t - 1]:
                do_pass(st, passed)
        if 0 <= t - 2 < nz:
            for st in groups[t - 2]:
                do_pass(st, across)

    for st in steps:
        d, side, s, ok = st

        def fn():
            for cp in partner(d, side, s):
                cp.wait_recv()
            for cond, cp in hops(d, side, s):
                when(cond, cp.wait_send)
            for cp in spread(d, side, s):
                cp.wait_send()
            for which in (passed, across):
                for _, go in which(d, side, s):
                    for cp in go:
                        cp.wait_send()

        when(ok, fn)
    own.wait()


def all_gather(shard, nz, ux, uy, uc, collective_id, name):
    group = (nz * 2 if ux else 1) * (4 if uc else 1)
    nsem = nz * 20
    return pl.pallas_call(
        functools.partial(ag_kernel, nz, ux, uy, uc),
        out_shape=jax.ShapeDtypeStruct((group,) + shard.shape, shard.dtype),
        in_specs=[pl.BlockSpec(memory_space=pl.ANY)],
        out_specs=pl.BlockSpec(memory_space=pl.ANY),
        scratch_shapes=[
            pltpu.SemaphoreType.DMA((nsem,)),
            pltpu.SemaphoreType.DMA((nsem,)),
            pltpu.SemaphoreType.DMA,
        ],
        compiler_params=pltpu.CompilerParams(collective_id=collective_id, has_side_effects=True),
        name=name,
    )(shard)


def rs_kernel(nz, ux, uy, uc, p_ref, o_ref, acc, rc, rx, ry, ra, rb, rz, ssem, rsem, lsem):
    pc = Place(nz, ux, uy, uc)
    z, x, y, c = pc.z, pc.x, pc.y, pc.c
    rows, cols = o_ref.shape
    half = rows // 2
    chunk = math.gcd(half, 32)
    f32 = jnp.float32
    pc.greet()
    to_x, to_y, to_c = pc.dev(z, 1 - x, y, c), pc.dev(z, x, 1 - y, c), pc.dev(z, x, y, 1 - c)
    rels = [(0, x, y)]
    if ux:
        rels.append((1, 1 - x, y))
    if uy:
        rels.append((2, x, 1 - y))
    if ux and uy:
        rels.append((3, 1 - x, 1 - y))
    KINDS = 12

    def slot(s):
        return s if nz > 1 else 0

    def sid(s, kind):
        return slot(s) * KINDS + kind

    def hf(ref, h):
        return ref.at[pl.ds(h * half, half)]

    def rcopy(src, dst, s, kind, device):
        return pltpu.make_async_remote_copy(
            src_ref=src,
            dst_ref=dst,
            send_sem=ssem.at[sid(s, kind)],
            recv_sem=rsem.at[sid(s, kind)],
            device_id=device,
            device_id_type=MESH_ID,
        )

    def load(s, rel, px, py):
        return pltpu.make_async_copy(
            p_ref.at[pc.blk(s, px, py, c)], acc.at[slot(s) * 4 + rel], lsem.at[slot(s) * 4 + rel]
        )

    def give(s, rel, px, py):
        return rcopy(
            p_ref.at[pc.blk(s, px, py, 1 - c)], rc.at[slot(s) * 4 + rel], s, rel, to_c
        )

    def fold(dst, lo, n, srcs):
        def body(i, _):
            r = pl.multiple_of(i * chunk, chunk)
            total = dst[pl.ds(lo + r, chunk), :].astype(f32)
            for ref, at in srcs:
                total = total + ref[pl.ds(at + r, chunk), :].astype(f32)
            dst[pl.ds(lo + r, chunk), :] = total.astype(dst.dtype)
            return 0

        lax.fori_loop(0, n // chunk, body, 0)

    def over_a(s):
        return rcopy(hf(acc.at[slot(s) * 4 + 3], 0), ra.at[slot(s)], s, 4, to_y)

    def over_b(s):
        return rcopy(hf(acc.at[slot(s) * 4 + 3], 1), rb.at[slot(s)], s, 5, to_x)

    def x_half(s, h):
        return rcopy(hf(acc.at[slot(s) * 4 + 1], h), hf(rx.at[slot(s)], h), s, 6 + h, to_x)

    def y_half(s, h):
        return rcopy(hf(acc.at[slot(s) * 4 + 2], h), hf(ry.at[slot(s)], h), s, 8 + h, to_y)

    def z_send(s, up):
        return rcopy(
            acc.at[slot(s) * 4],
            rz.at[slot(s)] if up is None else rz.at[slot(s)],
            s,
            10,
            pc.dev(z + (1 if up else -1), x, y, c),
        )

    def z_last(s, up):
        return pltpu.make_async_remote_copy(
            src_ref=acc.at[slot(s) * 4],
            dst_ref=rz.at[slot(s)] if up else rz.at[nz],
            send_sem=ssem.at[sid(s, 10)],
            recv_sem=rsem.at[sid(s, 10)] if up else rsem.at[sid(s, 11)],
            device_id=pc.dev(z + (1 if up else -1), x, y, c),
            device_id_type=MESH_ID,
        )

    steps = list(reversed(pc.line_steps()))

    for d, side, s, ok in steps:

        def fn():
            for rel, px, py in reversed(rels):
                load(s, rel, px, py).start()
                if uc:
                    give(s, rel, px, py).start()

        when(ok, fn)

    def first(step):
        d, side, s, ok = step

        def fn():
            for rel, px, py in reversed(rels):
                load(s, rel, px, py).wait()
                if uc:
                    give(s, rel, px, py).wait_recv()
                    fold(acc.at[slot(s) * 4 + rel], 0, rows, [(rc.at[slot(s) * 4 + rel], 0)])
                if rel == 3:
                    over_a(s).start()
                    over_b(s).start()
                if rel == 2:
                    y_half(s, 0).start()
                    if not ux:
                        y_half(s, 1).start()
                if rel == 1:
                    x_half(s, 1).start()
                    if not uy:
                        x_half(s, 0).start()

        when(ok, fn)

    def second(step):
        d, side, s, ok = step

        def fn():
            if ux and uy:
                over_a(s).wait_recv()
                fold(acc.at[slot(s) * 4 + 1], 0, half, [(ra.at[slot(s)], 0)])
                x_half(s, 0).start()
                over_b(s).wait_recv()
                fold(acc.at[slot(s) * 4 + 2], half, half, [(rb.at[slot(s)], 0)])
                y_half(s, 1).start()

        when(ok, fn)

    def third(step):
        d, side, s, ok = step

        def fn():
            srcs = []
            if ux:
                x_half(s, 0).wait_recv()
                x_half(s, 1).wait_recv()
                srcs.append((rx.at[slot(s)], 0))
            if uy:
                y_half(s, 0).wait_recv()
                y_half(s, 1).wait_recv()
                srcs.append((ry.at[slot(s)], 0))
            if d > 0:
                more = (z + 1 < nz) if side == 0 else (z >= 1)

                @pl.when(more)
                def _():
                    z_send(s, side == 1).wait_recv()
                    fold(acc.at[slot(s) * 4], 0, rows, srcs + [(rz.at[slot(s)], 0)])

                if srcs:

                    @pl.when(jnp.logical_not(more))
                    def _():
                        fold(acc.at[slot(s) * 4], 0, rows, srcs)

                if d == 1:
                    z_last(s, side == 1).start()
                else:
                    z_send(s, side == 1).start()
            else:

                def body(use_lo, use_hi):
                    terms = list(srcs)
                    if use_lo:
                        z_last(s, True).wait_recv()
                        terms.append((rz.at[slot(s)], 0))
                    if use_hi:
                        z_last(s, False).wait_recv()
                        terms.append((rz.at[nz], 0))

                    def step_(i, _):
                        r = pl.multiple_of(i * chunk, chunk)
                        total = acc[slot(s) * 4, pl.ds(r, chunk), :].astype(f32)
                        for ref, at in terms:
                            total = total + ref[pl.ds(at + r, chunk), :].astype(f32)
                        o_ref[pl.ds(r, chunk), :] = total.astype(o_ref.dtype)
                        return 0

                    lax.fori_loop(0, rows // chunk, step_, 0)

                if nz == 1:
                    body(False, False)
                else:
                    lo, hi = z >= 1, z + 1 < nz
                    pl.when(jnp.logical_and(lo, hi))(lambda: body(True, True))
                    pl.when(jnp.logical_and(lo, jnp.logical_not(hi)))(lambda: body(True, False))
                    pl.when(jnp.logical_and(jnp.logical_not(lo), hi))(lambda: body(False, True))

        when(ok, fn)

    groups = [[st for st in steps if st[0] == d] for d in reversed(range(nz))]
    for t in range(nz + 2):
        if t < nz:
            for st in groups[t]:
                first(st)
        if 0 <= t - 1 < nz:
            for st in groups[t - 1]:
                second(st)
        if 0 <= t - 2 < nz:
            for st in groups[t - 2]:
                third(st)

    for d, side, s, ok in steps:

        def fn():
            for rel, px, py in rels:
                if uc:
                    give(s, rel, px, py).wait_send()
            if ux and uy:
                over_a(s).wait_send()
                over_b(s).wait_send()
            if ux:
                x_half(s, 0).wait_send()
                x_half(s, 1).wait_send()
            if uy:
                y_half(s, 0).wait_send()
                y_half(s, 1).wait_send()
            if d > 0:
                z_send(s, side == 1).wait_send()

        when(ok, fn)


def reduce_scatter(parts, nz, ux, uy, uc, out_dtype, collective_id, name):
    group, rows, cols = parts.shape
    dt = parts.dtype
    lines = nz
    buf = lambda n, r: pltpu.VMEM((n, r, cols), dt)
    return pl.pallas_call(
        functools.partial(rs_kernel, nz, ux, uy, uc),
        out_shape=jax.ShapeDtypeStruct((rows, cols), out_dtype),
        in_specs=[pl.BlockSpec(memory_space=pl.ANY)],
        out_specs=pl.BlockSpec(memory_space=pltpu.VMEM),
        scratch_shapes=[
            buf(lines * 4, rows),
            buf(lines * 4 if uc else 1, rows if uc else 16),
            buf(lines if ux else 1, rows if ux else 16),
            buf(lines if uy else 1, rows if uy else 16),
            buf(lines if ux and uy else 1, rows // 2 if ux and uy else 16),
            buf(lines if ux and uy else 1, rows // 2 if ux and uy else 16),
            buf(lines + 1 if nz > 1 else 1, rows if nz > 1 else 16),
            pltpu.SemaphoreType.DMA((lines * 12,)),
            pltpu.SemaphoreType.DMA((lines * 12,)),
            pltpu.SemaphoreType.DMA((lines * 4,)),
        ],
        compiler_params=pltpu.CompilerParams(
            collective_id=collective_id, has_side_effects=True, vmem_limit_bytes=60 * 1024 * 1024
        ),
        name=name,
    )(parts)


def score_block(query_rot, key_piece, scaling):
    return (
        jnp.einsum("qsagd,ksad->sagqk", query_rot, key_piece, preferred_element_type=jnp.float32)
        * scaling
    )


def attend_keys(query_rot, query_pos, key_all, value_all, key_pos, scaling):
    length = key_all.shape[0]
    key_block = math.gcd(length, 512)
    block_count = length // key_block
    query_rows, seq_count, kv_count, group, head_dim = query_rot.shape
    start_carry = (
        jnp.full((seq_count, kv_count, group, query_rows), MASKED, jnp.float32),
        jnp.zeros((seq_count, kv_count, group, query_rows), jnp.float32),
        jnp.zeros((seq_count, kv_count, group, query_rows, head_dim), jnp.float32),
    )

    def step(block_id, carry):
        row_top, row_total, accum = carry
        start = block_id * key_block
        key_piece = lax.dynamic_slice_in_dim(key_all, start, key_block, 0)
        value_piece = lax.dynamic_slice_in_dim(value_all, start, key_block, 0)
        piece_pos = lax.dynamic_slice_in_dim(key_pos, start, key_block, 0)
        scores = score_block(query_rot, key_piece, scaling)
        allowed = piece_pos[None, :] <= query_pos[:, None]
        new_top = jnp.maximum(row_top, jnp.max(jnp.where(allowed, scores, MASKED), axis=-1))
        expo = jnp.where(allowed, jnp.exp(scores - new_top[..., None]), 0.0)
        decay = jnp.exp(row_top - new_top)
        row_total = row_total * decay + jnp.sum(expo, axis=-1)
        accum = accum * decay[..., None] + jnp.einsum(
            "sagqk,ksad->sagqd",
            expo.astype(jnp.bfloat16),
            value_piece,
            preferred_element_type=jnp.float32,
        )
        return (new_top, row_total, accum)

    return lax.fori_loop(0, block_count, step, start_carry)


def attend_grads(
    query_rot, query_pos, key_all, value_all, key_pos, attn_cot, delta, log_total, scaling
):
    length = key_all.shape[0]
    key_block = math.gcd(length, 512)
    block_count = length // key_block
    query_rows, seq_count, kv_count, group, head_dim = query_rot.shape

    def step(query_cot, block_id):
        start = block_id * key_block
        key_piece = lax.dynamic_slice_in_dim(key_all, start, key_block, 0)
        value_piece = lax.dynamic_slice_in_dim(value_all, start, key_block, 0)
        piece_pos = lax.dynamic_slice_in_dim(key_pos, start, key_block, 0)
        scores = score_block(query_rot, key_piece, scaling)
        allowed = piece_pos[None, :] <= query_pos[:, None]
        weights_back = jnp.where(allowed, jnp.exp(scores - log_total[..., None]), 0.0)
        prob_cot = jnp.einsum(
            "qsagd,ksad->sagqk", attn_cot, value_piece, preferred_element_type=jnp.float32
        )
        score_cot = weights_back * (prob_cot - delta[..., None])
        value_cot = jnp.einsum(
            "sagqk,qsagd->ksad",
            weights_back.astype(jnp.bfloat16),
            attn_cot,
            preferred_element_type=jnp.float32,
        )
        score_low = score_cot.astype(jnp.bfloat16)
        query_cot = (
            query_cot
            + jnp.einsum(
                "sagqk,ksad->qsagd", score_low, key_piece, preferred_element_type=jnp.float32
            )
            * scaling
        )
        key_cot = (
            jnp.einsum(
                "sagqk,qsagd->ksad", score_low, query_rot, preferred_element_type=jnp.float32
            )
            * scaling
        )
        return (query_cot, (key_cot, value_cot))

    start_carry = jnp.zeros((query_rows, seq_count, kv_count, group, head_dim), jnp.float32)
    query_cot, (key_cot, value_cot) = lax.scan(
        step, start_carry, jnp.arange(block_count, dtype=jnp.int32)
    )
    return (
        query_cot,
        key_cot.reshape(length, seq_count, kv_count * head_dim),
        value_cot.reshape(length, seq_count, kv_count * head_dim),
    )


def gather_ctx(shard, name, ident):
    if lax.axis_size("ctx") == 8 and lax.axis_size("wsh") == 4:
        return all_gather(shard, 4, True, False, False, ident, name)
    return lax.all_gather(shard, "ctx", axis=0)


def gather_wsh(shard, name, ident):
    if lax.axis_size("ctx") == 8 and lax.axis_size("wsh") == 4:
        return all_gather(shard, 1, False, True, True, ident, name)
    return lax.all_gather(shard, "wsh", axis=0)


def gather_all(shard, name, ident):
    if lax.axis_size("ctx") == 8 and lax.axis_size("wsh") == 4:
        return all_gather(shard, 4, True, True, True, ident, name)
    return lax.all_gather(shard, ("ctx", "wsh"), axis=0)


def scatter_ctx(parts, name, ident):
    if lax.axis_size("ctx") == 8 and lax.axis_size("wsh") == 4:
        return reduce_scatter(parts, 4, True, False, False, jnp.float32, ident, name)
    return lax.psum_scatter(parts, "ctx", scatter_dimension=0, tiled=False).astype(jnp.float32)


def scatter_wsh(parts, name, ident):
    if lax.axis_size("ctx") == 8 and lax.axis_size("wsh") == 4:
        return reduce_scatter(parts, 1, False, True, True, jnp.float32, ident, name)
    return lax.psum_scatter(parts, "wsh", scatter_dimension=0, tiled=False).astype(jnp.float32)


def scatter_all(parts, name, ident):
    if lax.axis_size("ctx") == 8 and lax.axis_size("wsh") == 4:
        return reduce_scatter(parts, 4, True, True, True, jnp.float32, ident, name)
    return lax.psum_scatter(
        parts, ("ctx", "wsh"), scatter_dimension=0, tiled=False
    ).astype(jnp.float32)


def exchange(pieces):
    return lax.all_to_all(pieces, ("ctx", "wsh"), split_axis=0, concat_axis=0, tiled=True)


def to_everyone(value, device_count):
    return exchange(jnp.broadcast_to(value[None], (device_count,) + value.shape))


def local(
    inputs,
    pair_map,
    norm_gain,
    query_weight,
    key_weight,
    value_weight,
    query_gain,
    key_gain,
    out_weight,
    moe_gain,
    router,
    expert_gate,
    expert_up,
    expert_down,
    expert_ids,
    dispatch_slot,
    cotangent,
):
    f32, bf16 = jnp.float32, jnp.bfloat16
    rows_dev, seq_count, width = inputs.shape
    ctx_count = lax.axis_size("ctx")
    wsh_count = lax.axis_size("wsh")
    device_count = ctx_count * wsh_count
    head_dim = query_gain.shape[0]
    group_rows = rows_dev * wsh_count
    block_len = group_rows // 2
    seq_len = group_rows * ctx_count
    tokens = rows_dev * seq_count
    group_tokens = tokens * wsh_count
    top_count = expert_ids.shape[-1]
    expert_count = router.shape[1]
    capacity = max(2, 3 * top_count * block_len // (2 * device_count))
    scaling = head_dim ** (-0.5)
    positions = positions_of(pair_map, seq_len, block_len, pair_map.shape[0])
    query_pos = lax.dynamic_slice_in_dim(
        positions, lax.axis_index("ctx") * group_rows, group_rows, 0
    )
    cosine, sine_table = rope_tables(query_pos, head_dim)
    cosine = cosine[:, None, None, :]
    sine_table = sine_table[:, None, None, :]

    inputs_f = inputs.astype(f32)
    normed_f, inverse_one = rms_forward(inputs_f, norm_gain)
    normed = normed_f.astype(bf16)
    normed_flat = gather_wsh(normed.reshape(tokens, width), "ag_normed", 1).reshape(
        group_tokens, width
    )
    q_cols, kv_cols = query_weight.shape[1], key_weight.shape[1]
    qkv_shard = jnp.concatenate([query_weight, key_weight, value_weight], axis=1)
    qkv_full = gather_ctx(qkv_shard, "ag_qkv", 2).reshape(width, q_cols + 2 * kv_cols)
    out_shard = out_weight.T
    out_full = lax.all_gather(out_shard, "ctx", axis=0, tiled=True)
    cot_flat = cotangent.reshape(tokens, width)
    cot_all = lax.all_gather(cot_flat.astype(bf16), ("ctx", "wsh"), axis=0)
    heads_loc = q_cols // head_dim
    kv_loc = kv_cols // head_dim
    group = heads_loc // kv_loc
    projected = jnp.dot(normed_flat, qkv_full, preferred_element_type=f32)
    queries = projected[:, :q_cols].reshape(group_rows, seq_count, heads_loc, head_dim)
    keys_raw = projected[:, q_cols : q_cols + kv_cols].reshape(
        group_rows, seq_count, kv_loc, head_dim
    )
    value_rows = projected[:, q_cols + kv_cols :].astype(bf16)
    query_normed, query_inverse = rms_forward(queries, query_gain)
    key_normed, key_inverse = rms_forward(keys_raw, key_gain)
    query_rot = (
        rotate(query_normed, cosine, sine_table)
        .astype(bf16)
        .reshape(group_rows, seq_count, kv_loc, group, head_dim)
    )
    key_rot = rotate(key_normed, cosine, sine_table).astype(bf16)
    kv_width = seq_count * kv_cols
    kv_own = jnp.concatenate(
        [key_rot.reshape(group_rows, kv_width), value_rows.reshape(group_rows, kv_width)], axis=1
    )
    kv_all = gather_ctx(kv_own, "ag_kv", 3).reshape(seq_len, 2 * kv_width)
    key_all = kv_all[:, :kv_width].reshape(seq_len, seq_count, kv_loc, head_dim)
    value_all = kv_all[:, kv_width:].reshape(seq_len, seq_count, kv_loc, head_dim)

    row_top, row_total, accum = attend_keys(
        query_rot, query_pos, key_all, value_all, positions, scaling
    )
    log_total = row_top + jnp.log(row_total)
    attention = (accum / row_total[..., None]).astype(bf16)
    attention_flat = attention.transpose(3, 0, 1, 2, 4).reshape(
        group_tokens, heads_loc * head_dim
    )
    mixed = jnp.einsum("tc,dc->td", attention_flat, out_full, preferred_element_type=f32)
    residual = inputs_f.reshape(tokens, width) + scatter_wsh(
        mixed.astype(bf16).reshape(wsh_count, tokens, width), "rs_mixed", 4
    )

    moe_normed_f, inverse_two = rms_forward(residual, moe_gain)
    moe_flat = moe_normed_f.astype(bf16)
    moe_all = gather_all(moe_flat, "ag_moe", 5)
    logits = jnp.dot(moe_flat, router, preferred_element_type=f32)
    route_ids = expert_ids.reshape(tokens, top_count)
    slots = dispatch_slot.reshape(tokens, top_count)
    expert_onehot = (
        route_ids[:, :, None] == jnp.arange(expert_count, dtype=jnp.int32)[None, None, :]
    )
    named = jnp.any(expert_onehot, axis=1)
    slot_dense = jnp.sum(jnp.where(expert_onehot, slots[:, :, None] + 1, 0), axis=1) - 1
    chosen_top = jnp.max(jnp.where(named, logits, MASKED), axis=-1, keepdims=True)
    chosen_exp = jnp.where(named, jnp.exp(jnp.where(named, logits - chosen_top, 0.0)), 0.0)
    weight_dense = chosen_exp / jnp.sum(chosen_exp, axis=-1, keepdims=True)
    routing = exchange(jnp.stack([slot_dense.astype(f32).T, weight_dense.T], axis=1))
    slot_mine = routing[:, 0, :].astype(jnp.int32)
    weight_mine = routing[:, 1, :]
    picks = slot_mine[:, None, :] == jnp.arange(capacity, dtype=jnp.int32)[None, :, None]
    picks_low = picks.astype(bf16)
    slot_weight = jnp.sum(jnp.where(picks, weight_mine[:, None, :], 0.0), axis=-1)

    def take(everyone):
        return (
            jnp.einsum("dct,dtw->dcw", picks_low, everyone, preferred_element_type=f32)
            .astype(bf16)
            .reshape(device_count * capacity, width)
        )

    def put(rows):
        return jnp.einsum(
            "dct,dcw->dtw",
            picks_low,
            rows.reshape(device_count, capacity, width),
            preferred_element_type=f32,
        ).astype(bf16)

    gate_w, up_w, down_w = (expert_gate[0], expert_up[0], expert_down[0])
    rows_in = take(moe_all)
    cot_rows = take(cot_all).astype(f32)
    weight_rows = slot_weight.reshape(device_count * capacity, 1)
    route_cot = (weight_rows * cot_rows).astype(bf16)
    gate_pre = jnp.dot(rows_in, gate_w, preferred_element_type=f32)
    up_pre = jnp.dot(rows_in, up_w, preferred_element_type=f32)
    sigmoid = jax.nn.sigmoid(gate_pre)
    swish = gate_pre * sigmoid
    activation = (swish * up_pre).astype(bf16)
    produced = jnp.dot(activation, down_w, preferred_element_type=f32).astype(bf16).astype(f32)
    out_parts = put((weight_rows * produced).astype(bf16))
    slot_cot = jnp.sum(cot_rows * produced, axis=-1).reshape(device_count, capacity)
    cot_mine = jnp.sum(jnp.where(picks, slot_cot[:, :, None], 0.0), axis=1)
    weight_cot = exchange(cot_mine).T
    down_grad = jnp.einsum("rf,rd->fd", activation, route_cot, preferred_element_type=f32)
    act_cot = jnp.einsum("rd,fd->rf", route_cot, down_w, preferred_element_type=f32)
    gate_cot = (act_cot * up_pre * sigmoid * (1.0 + gate_pre * (1.0 - sigmoid))).astype(bf16)
    up_cot = (act_cot * swish).astype(bf16)
    gate_grad = jnp.einsum("rd,rf->df", rows_in, gate_cot, preferred_element_type=f32)
    up_grad = jnp.einsum("rd,rf->df", rows_in, up_cot, preferred_element_type=f32)
    row_cot = jnp.einsum("rf,df->rd", gate_cot, gate_w, preferred_element_type=f32)
    row_cot = row_cot + jnp.einsum("rf,df->rd", up_cot, up_w, preferred_element_type=f32)
    row_sum = scatter_all(put(row_cot.astype(bf16)), "rs_rows", 6)
    moe_sum = scatter_all(out_parts, "rs_outputs", 7)
    outputs = (residual + moe_sum).reshape(rows_dev, seq_count, width).astype(bf16)

    chosen_cot = weight_dense * (
        weight_cot - jnp.sum(weight_dense * weight_cot, axis=-1, keepdims=True)
    )
    logit_cot = chosen_cot.astype(bf16)
    if device_count > 32:
        router_grad = lax.psum(
            jnp.einsum("td,te->de", moe_flat, logit_cot, preferred_element_type=f32),
            ("ctx", "wsh"),
        )
    else:
        router_grad = jnp.einsum(
            "td,te->de",
            moe_all.reshape(device_count * tokens, width),
            to_everyone(logit_cot, device_count).reshape(device_count * tokens, expert_count),
            preferred_element_type=f32,
        )
    normed_two_cot = (
        jnp.einsum("te,de->td", logit_cot, router, preferred_element_type=f32) + row_sum
    )
    residual_norm_cot, moe_gain_grad = rms_backward(
        residual, inverse_two, moe_gain, normed_two_cot
    )
    residual_cot = cot_flat + residual_norm_cot
    residual_low = residual_cot.astype(bf16)
    residual_flat = gather_wsh(residual_low, "ag_residual", 8).reshape(group_tokens, width)

    out_grad = jnp.einsum(
        "td,tc->dc", residual_flat, attention_flat, preferred_element_type=f32
    ).astype(bf16)
    out_weight_grad = (
        lax.psum_scatter(out_grad, "ctx", scatter_dimension=0, tiled=True).astype(f32).T
    )
    attention_cot = jnp.einsum(
        "td,dc->tc", residual_flat, out_full, preferred_element_type=f32
    ).astype(bf16)
    attention_cot = attention_cot.reshape(group_rows, seq_count, kv_loc, group, head_dim)
    attention_q = attention_flat.reshape(group_rows, seq_count, kv_loc, group, head_dim)
    delta = jnp.sum(attention_cot.astype(f32) * attention_q.astype(f32), axis=-1).transpose(
        1, 2, 3, 0
    )
    query_rot_cot, key_cot_all, value_cot_all = attend_grads(
        query_rot,
        query_pos,
        key_all,
        value_all,
        positions,
        attention_cot,
        delta,
        log_total,
        scaling,
    )
    kv_cot_all = jnp.concatenate(
        [key_cot_all.reshape(seq_len, kv_width), value_cot_all.reshape(seq_len, kv_width)], axis=1
    ).astype(bf16)
    kv_cot = scatter_ctx(kv_cot_all.reshape(ctx_count, group_rows, 2 * kv_width), "rs_kv", 9)
    key_cot_own = kv_cot[:, :kv_width]
    value_cot_own = kv_cot[:, kv_width:]
    query_cot, query_gain_grad = rms_backward(
        queries,
        query_inverse,
        query_gain,
        unrotate(
            query_rot_cot.reshape(group_rows, seq_count, heads_loc, head_dim), cosine, sine_table
        ),
    )
    key_cot, key_gain_grad = rms_backward(
        keys_raw,
        key_inverse,
        key_gain,
        unrotate(key_cot_own.reshape(group_rows, seq_count, kv_loc, head_dim), cosine, sine_table),
    )
    query_low = query_cot.astype(bf16).reshape(group_tokens, q_cols)
    key_low = key_cot.astype(bf16).reshape(group_tokens, kv_cols)
    value_low = value_cot_own.astype(bf16).reshape(group_tokens, kv_cols)
    low = jnp.concatenate([query_low, key_low, value_low], axis=1)
    summed = jnp.einsum("tq,cq->tc", low, qkv_full, preferred_element_type=f32)
    normed_cot = scatter_wsh(
        summed.astype(bf16).reshape(wsh_count, tokens, width), "rs_normed", 10
    )
    qkv_grad = jnp.einsum("tc,tq->cq", normed_flat, low, preferred_element_type=f32).astype(bf16)
    qkv_grad = scatter_ctx(
        qkv_grad.reshape(ctx_count, width // ctx_count, q_cols + 2 * kv_cols), "rs_qkv", 11
    )
    inputs_flat = inputs_f.reshape(tokens, width)
    input_norm_cot, norm_gain_grad = rms_backward(
        inputs_flat, inverse_one.reshape(tokens, 1), norm_gain, normed_cot
    )
    input_grad = (residual_cot + input_norm_cot).reshape(rows_dev, seq_count, width)
    gains = jnp.concatenate([norm_gain_grad, moe_gain_grad, query_gain_grad, key_gain_grad])
    gains = jnp.sum(to_everyone(gains, device_count), axis=0)
    return (
        outputs,
        input_grad,
        gains[:width],
        qkv_grad[:, :q_cols],
        qkv_grad[:, q_cols : q_cols + kv_cols],
        qkv_grad[:, q_cols + kv_cols :],
        gains[2 * width : 2 * width + head_dim],
        gains[2 * width + head_dim :],
        out_weight_grad,
        gains[width : 2 * width],
        router_grad,
        gate_grad[None],
        up_grad[None],
        down_grad[None],
    )


def solution(mesh):
    return jax.shard_map(
        local,
        mesh=mesh,
        in_specs=(
            P(("ctx", "wsh"), None, None),
            P(),
            P(),
            P("ctx", "wsh"),
            P("ctx", "wsh"),
            P("ctx", "wsh"),
            P(),
            P(),
            P("wsh", "ctx"),
            P(),
            P(),
            P(("ctx", "wsh"), None, None),
            P(("ctx", "wsh"), None, None),
            P(("ctx", "wsh"), None, None),
            P(("ctx", "wsh"), None, None),
            P(("ctx", "wsh"), None, None),
            P(("ctx", "wsh"), None, None),
        ),
        out_specs=(
            P(("ctx", "wsh"), None, None),
            P(("ctx", "wsh"), None, None),
            P(),
            P("ctx", "wsh"),
            P("ctx", "wsh"),
            P("ctx", "wsh"),
            P(),
            P(),
            P("wsh", "ctx"),
            P(),
            P(),
            P(("ctx", "wsh"), None, None),
            P(("ctx", "wsh"), None, None),
            P(("ctx", "wsh"), None, None),
        ),
        check_vma=False,
    )
```

```python
import functools
import math

import jax
import jax.numpy as jnp
from jax import lax
from jax.experimental import pallas as pl
from jax.experimental.pallas import tpu as pltpu
from jax.sharding import PartitionSpec as P


EPSILON = 1e-06
ROPE_BASE = 1000000.0
MASKED = -1e30


def positions_of(pair_map, seq_len, block_len, group_count):
    row_index = jnp.arange(seq_len, dtype=jnp.int32)
    owner_group = row_index // (2 * block_len)
    inner_row = row_index % (2 * block_len)
    group_table = jnp.arange(group_count, dtype=jnp.int32)
    pair_index = jnp.sum(
        jnp.where(owner_group[:, None] == group_table[None, :], pair_map[None, :], 0), axis=1
    )
    block_index = jnp.where(inner_row < block_len, pair_index, 2 * group_count - 1 - pair_index)
    return block_index * block_len + inner_row % block_len


def rope_tables(positions, head_dim):
    half_dim = head_dim // 2
    frequency = ROPE_BASE ** (-(jnp.arange(half_dim, dtype=jnp.float32) * 2.0) / head_dim)
    angles = positions.astype(jnp.float32)[:, None] * frequency[None, :]
    return (jnp.cos(angles), jnp.sin(angles))


def rms_forward(tensor, gain_vector):
    inverse = lax.rsqrt(jnp.mean(tensor * tensor, axis=-1, keepdims=True) + EPSILON)
    return (tensor * inverse * gain_vector, inverse)


def rms_backward(tensor, inverse, gain_vector, gradient):
    weighted = gradient * gain_vector
    inner_mean = jnp.mean(weighted * tensor, axis=-1, keepdims=True)
    tensor_grad = inverse * weighted - tensor * inverse**3 * inner_mean
    gain_grad = jnp.sum((gradient * tensor * inverse).reshape(-1, tensor.shape[-1]), axis=0)
    return (tensor_grad, gain_grad)


MESH_ID = pl.DeviceIdType.MESH


class Place:
    def __init__(self, nz, ux, uy, uc):
        ci, wi = lax.axis_index("ctx"), lax.axis_index("wsh")
        self.nz, self.ux, self.uy, self.uc = nz, ux, uy, uc
        self.z, self.x, self.y, self.c = ci // 2, ci % 2, wi // 2, wi % 2

    def dev(self, z, x, y, c):
        return (z * 2 + x, y * 2 + c)

    def blk(self, z, x, y, c):
        if self.ux and self.uc:
            return (z * 2 + x) * 4 + y * 2 + c
        if self.ux:
            return z * 2 + x
        return y * 2 + c

    def greet(self):
        z, x, y, c, nz = self.z, self.x, self.y, self.c, self.nz
        barrier = pltpu.get_barrier_semaphore()
        count = 0
        if nz > 1:
            for step in (-1, 1):
                ok = jnp.logical_and(z + step >= 0, z + step < nz)

                @pl.when(ok)
                def _():
                    pl.semaphore_signal(
                        barrier, inc=1, device_id=self.dev(z + step, x, y, c), device_id_type=MESH_ID
                    )

                count = count + ok.astype(jnp.int32)
        for use, place in (
            (self.ux, (z, 1 - x, y, c)),
            (self.uy, (z, x, 1 - y, c)),
            (self.uc, (z, x, y, 1 - c)),
        ):
            if use:
                pl.semaphore_signal(
                    barrier, inc=1, device_id=self.dev(*place), device_id_type=MESH_ID
                )
                count = count + 1
        pl.semaphore_wait(barrier, count)

    def line_steps(self):
        steps = [(0, 0, self.z, None)]
        for d in range(1, self.nz):
            steps.append((d, 0, self.z - d, self.z - d >= 0))
            steps.append((d, 1, self.z + d, self.z + d < self.nz))
        return steps


def when(cond, fn):
    if cond is None:
        fn()
    else:
        pl.when(cond)(fn)


def gather_job(axes, x_ref, o_ref, ssem, rsem, lsem):
    nz, ux, uy, uc = axes
    pc = Place(nz, ux, uy, uc)
    z, x, y, c = pc.z, pc.x, pc.y, pc.c
    rows = x_ref.shape[0]
    half = rows // 2
    to_x, to_y, to_c = pc.dev(z, 1 - x, y, c), pc.dev(z, x, 1 - y, c), pc.dev(z, x, y, 1 - c)

    def part(b, p):
        if p == 0:
            return o_ref.at[b]
        return o_ref.at[b, pl.ds((p - 1) * half, half)]

    def sid(d, side, kind):
        return (d * 2 + side) * 10 + kind

    def copy(b, p, sidx, ridx, device, src=None):
        return pltpu.make_async_remote_copy(
            src_ref=part(b, p) if src is None else src,
            dst_ref=part(b, p),
            send_sem=ssem.at[sidx],
            recv_sem=rsem.at[ridx],
            device_id=device,
            device_id_type=MESH_ID,
        )

    own = pltpu.make_async_copy(x_ref, o_ref.at[pc.blk(z, x, y, c)], lsem)

    def hops(d, side, s):
        out = []
        if nz > 1:
            b = pc.blk(s, x, y, c)
            src = x_ref if d == 0 else None
            if d == 0 or side == 0:
                if d + 1 < nz:
                    out.append(
                        (z + 1 < nz, copy(b, 0, sid(d, 0, 0), sid(d + 1, 0, 0), pc.dev(z + 1, x, y, c), src))
                    )
            if d == 0 or side == 1:
                if d + 1 < nz:
                    out.append(
                        (z >= 1, copy(b, 0, sid(d, 1, 0), sid(d + 1, 1, 0), pc.dev(z - 1, x, y, c), src))
                    )
        return out

    def spread(d, side, s):
        b = pc.blk(s, x, y, c)
        src = x_ref if d == 0 else None
        out = []
        if ux:
            out.append(copy(b, 0, sid(d, side, 1), sid(d, side, 1), to_x, src))
        if uy:
            out.append(copy(b, 0, sid(d, side, 2), sid(d, side, 2), to_y, src))
        if uc:
            out.append(copy(b, 0, sid(d, side, 5), sid(d, side, 5), to_c, src))
        return out

    def passed(d, side, s):
        out = []
        if ux:
            b = pc.blk(s, 1 - x, y, c)
            arrive = copy(b, 0, sid(d, side, 1), sid(d, side, 1), to_x)
            go = []
            if uy:
                go.append(copy(b, 1, sid(d, side, 3), sid(d, side, 3), to_y))
            if uc:
                go.append(copy(b, 0, sid(d, side, 6), sid(d, side, 6), to_c))
            out.append((arrive, go))
        if uy:
            b = pc.blk(s, x, 1 - y, c)
            arrive = copy(b, 0, sid(d, side, 2), sid(d, side, 2), to_y)
            go = []
            if ux:
                go.append(copy(b, 2, sid(d, side, 4), sid(d, side, 4), to_x))
            if uc:
                go.append(copy(b, 0, sid(d, side, 7), sid(d, side, 7), to_c))
            out.append((arrive, go))
        return out

    def across(d, side, s):
        out = []
        if ux and uy:
            b = pc.blk(s, 1 - x, 1 - y, c)
            arrive = copy(b, 1, sid(d, side, 3), sid(d, side, 3), to_y)
            go = [copy(b, 1, sid(d, side, 8), sid(d, side, 8), to_c)] if uc else []
            out.append((arrive, go))
            arrive = copy(b, 2, sid(d, side, 4), sid(d, side, 4), to_x)
            go = [copy(b, 2, sid(d, side, 9), sid(d, side, 9), to_c)] if uc else []
            out.append((arrive, go))
        return out

    def partner(d, side, s):
        out = []
        if uc:
            out.append(copy(pc.blk(s, x, y, 1 - c), 0, 0, sid(d, side, 5), to_c))
            if ux:
                out.append(copy(pc.blk(s, 1 - x, y, 1 - c), 0, 0, sid(d, side, 6), to_c))
            if uy:
                out.append(copy(pc.blk(s, x, 1 - y, 1 - c), 0, 0, sid(d, side, 7), to_c))
            if ux and uy:
                b = pc.blk(s, 1 - x, 1 - y, 1 - c)
                out.append(copy(b, 1, 0, sid(d, side, 8), to_c))
                out.append(copy(b, 2, 0, sid(d, side, 9), to_c))
        return out

    steps = pc.line_steps()

    def do_line(step):
        d, side, s, ok = step

        def fn():
            if d > 0:
                copy(pc.blk(s, x, y, c), 0, 0, sid(d, side, 0), to_x).wait_recv()
            for cond, cp in hops(d, side, s):
                when(cond, cp.start)
            for cp in spread(d, side, s):
                cp.start()

        when(ok, fn)

    def do_pass(step, which):
        d, side, s, ok = step

        def fn():
            for arrive, go in which(d, side, s):
                arrive.wait_recv()
                for cp in go:
                    cp.start()

        when(ok, fn)

    groups = [[st for st in steps if st[0] == d] for d in range(nz)]

    def phase(t):
        if t < nz:
            for st in groups[t]:
                do_line(st)
        if 0 <= t - 1 < nz:
            for st in groups[t - 1]:
                do_pass(st, passed)
        if 0 <= t - 2 < nz:
            for st in groups[t - 2]:
                do_pass(st, across)

    def last():
        for st in steps:
            d, side, s, ok = st

            def fn():
                for cp in partner(d, side, s):
                    cp.wait_recv()
                for cond, cp in hops(d, side, s):
                    when(cond, cp.wait_send)
                for cp in spread(d, side, s):
                    cp.wait_send()
                for which in (passed, across):
                    for _, go in which(d, side, s):
                        for cp in go:
                            cp.wait_send()

            when(ok, fn)
        own.wait()

    return own.start, [functools.partial(phase, t) for t in range(nz + 2)], last


WSH_AXES = (1, False, True, True)
CTX_AXES = (4, True, False, False)
ALL_AXES = (4, True, True, True)


def run_jobs(axes_list, jobs):
    Place(
        max(a[0] for a in axes_list),
        any(a[1] for a in axes_list),
        any(a[2] for a in axes_list),
        any(a[3] for a in axes_list),
    ).greet()
    for begin, _, _ in jobs:
        begin()
    for t in range(max(len(phases) for _, phases, _ in jobs)):
        for _, phases, _ in jobs:
            if t < len(phases):
                phases[t]()
    for _, _, last in jobs:
        last()


def group_of(axes):
    return (axes[0] * 2 if axes[1] else 1) * (4 if axes[3] else 1)


def gather_kernel(axes_list, *refs):
    n = len(axes_list)
    jobs = [
        gather_job(axes_list[i], refs[i], refs[n + i], *refs[2 * n + 3 * i : 2 * n + 3 * i + 3])
        for i in range(n)
    ]
    run_jobs(axes_list, jobs)


def gather_sems(axes):
    return [
        pltpu.SemaphoreType.DMA((axes[0] * 20,)),
        pltpu.SemaphoreType.DMA((axes[0] * 20,)),
        pltpu.SemaphoreType.DMA,
    ]


def all_gather(shards, axes_list, collective_id):
    return pl.pallas_call(
        functools.partial(gather_kernel, axes_list),
        out_shape=[
            jax.ShapeDtypeStruct((group_of(axes),) + shard.shape, shard.dtype)
            for shard, axes in zip(shards, axes_list)
        ],
        in_specs=[pl.BlockSpec(memory_space=pl.ANY)] * len(shards),
        out_specs=[pl.BlockSpec(memory_space=pl.ANY)] * len(shards),
        scratch_shapes=[x for axes in axes_list for x in gather_sems(axes)],
        compiler_params=pltpu.CompilerParams(collective_id=collective_id, has_side_effects=True),
    )(*shards)


def scatter_job(axes, p_ref, o_ref, acc, rc, rx, ry, ra, rb, rz, ssem, rsem, lsem):
    nz, ux, uy, uc = axes
    pc = Place(nz, ux, uy, uc)
    z, x, y, c = pc.z, pc.x, pc.y, pc.c
    rows, _ = o_ref.shape
    half = rows // 2
    chunk = math.gcd(half, 32)
    f32 = jnp.float32
    to_x, to_y, to_c = pc.dev(z, 1 - x, y, c), pc.dev(z, x, 1 - y, c), pc.dev(z, x, y, 1 - c)
    rels = [(0, x, y)]
    if ux:
        rels.append((1, 1 - x, y))
    if uy:
        rels.append((2, x, 1 - y))
    if ux and uy:
        rels.append((3, 1 - x, 1 - y))
    KINDS = 12

    def slot(s):
        return s if nz > 1 else 0

    def sid(s, kind):
        return slot(s) * KINDS + kind

    def hf(ref, h):
        return ref.at[pl.ds(h * half, half)]

    def rcopy(src, dst, s, kind, device):
        return pltpu.make_async_remote_copy(
            src_ref=src,
            dst_ref=dst,
            send_sem=ssem.at[sid(s, kind)],
            recv_sem=rsem.at[sid(s, kind)],
            device_id=device,
            device_id_type=MESH_ID,
        )

    def load(s, rel, px, py):
        return pltpu.make_async_copy(
            p_ref.at[pc.blk(s, px, py, c)], acc.at[slot(s) * 4 + rel], lsem.at[slot(s) * 4 + rel]
        )

    def give(s, rel, px, py):
        return rcopy(
            p_ref.at[pc.blk(s, px, py, 1 - c)], rc.at[slot(s) * 4 + rel], s, rel, to_c
        )

    def fold(dst, lo, n, srcs):
        def body(i, _):
            r = pl.multiple_of(i * chunk, chunk)
            total = dst[pl.ds(lo + r, chunk), :].astype(f32)
            for ref, at in srcs:
                total = total + ref[pl.ds(at + r, chunk), :].astype(f32)
            dst[pl.ds(lo + r, chunk), :] = total.astype(dst.dtype)
            return 0

        lax.fori_loop(0, n // chunk, body, 0)

    def over_a(s):
        return rcopy(hf(acc.at[slot(s) * 4 + 3], 0), ra.at[slot(s)], s, 4, to_y)

    def over_b(s):
        return rcopy(hf(acc.at[slot(s) * 4 + 3], 1), rb.at[slot(s)], s, 5, to_x)

    def x_half(s, h):
        return rcopy(hf(acc.at[slot(s) * 4 + 1], h), hf(rx.at[slot(s)], h), s, 6 + h, to_x)

    def y_half(s, h):
        return rcopy(hf(acc.at[slot(s) * 4 + 2], h), hf(ry.at[slot(s)], h), s, 8 + h, to_y)

    def z_send(s, up):
        return rcopy(
            acc.at[slot(s) * 4],
            rz.at[slot(s)],
            s,
            10,
            pc.dev(z + (1 if up else -1), x, y, c),
        )

    def z_last(s, up):
        return pltpu.make_async_remote_copy(
            src_ref=acc.at[slot(s) * 4],
            dst_ref=rz.at[slot(s)] if up else rz.at[nz],
            send_sem=ssem.at[sid(s, 10)],
            recv_sem=rsem.at[sid(s, 10)] if up else rsem.at[sid(s, 11)],
            device_id=pc.dev(z + (1 if up else -1), x, y, c),
            device_id_type=MESH_ID,
        )

    steps = list(reversed(pc.line_steps()))

    def begin():
        for d, side, s, ok in steps:

            def fn():
                for rel, px, py in reversed(rels):
                    load(s, rel, px, py).start()
                    if uc:
                        give(s, rel, px, py).start()

            when(ok, fn)

    def first(step):
        _, _, s, ok = step

        def fn():
            for rel, px, py in reversed(rels):
                load(s, rel, px, py).wait()
                if uc:
                    give(s, rel, px, py).wait_recv()
                    fold(acc.at[slot(s) * 4 + rel], 0, rows, [(rc.at[slot(s) * 4 + rel], 0)])
                if rel == 3:
                    over_a(s).start()
                    over_b(s).start()
                if rel == 2:
                    y_half(s, 0).start()
                    if not ux:
                        y_half(s, 1).start()
                if rel == 1:
                    x_half(s, 1).start()
                    if not uy:
                        x_half(s, 0).start()

        when(ok, fn)

    def second(step):
        _, _, s, ok = step

        def fn():
            if ux and uy:
                over_a(s).wait_recv()
                fold(acc.at[slot(s) * 4 + 1], 0, half, [(ra.at[slot(s)], 0)])
                x_half(s, 0).start()
                over_b(s).wait_recv()
                fold(acc.at[slot(s) * 4 + 2], half, half, [(rb.at[slot(s)], 0)])
                y_half(s, 1).start()

        when(ok, fn)

    def third(step):
        d, side, s, ok = step

        def fn():
            srcs = []
            if ux:
                x_half(s, 0).wait_recv()
                x_half(s, 1).wait_recv()
                srcs.append((rx.at[slot(s)], 0))
            if uy:
                y_half(s, 0).wait_recv()
                y_half(s, 1).wait_recv()
                srcs.append((ry.at[slot(s)], 0))
            if d > 0:
                more = (z + 1 < nz) if side == 0 else (z >= 1)

                @pl.when(more)
                def _():
                    z_send(s, side == 1).wait_recv()
                    fold(acc.at[slot(s) * 4], 0, rows, srcs + [(rz.at[slot(s)], 0)])

                if srcs:

                    @pl.when(jnp.logical_not(more))
                    def _():
                        fold(acc.at[slot(s) * 4], 0, rows, srcs)

                if d == 1:
                    z_last(s, side == 1).start()
                else:
                    z_send(s, side == 1).start()
            else:

                def body(use_lo, use_hi):
                    terms = list(srcs)
                    if use_lo:
                        z_last(s, True).wait_recv()
                        terms.append((rz.at[slot(s)], 0))
                    if use_hi:
                        z_last(s, False).wait_recv()
                        terms.append((rz.at[nz], 0))

                    def step_(i, _):
                        r = pl.multiple_of(i * chunk, chunk)
                        total = acc[slot(s) * 4, pl.ds(r, chunk), :].astype(f32)
                        for ref, at in terms:
                            total = total + ref[pl.ds(at + r, chunk), :].astype(f32)
                        o_ref[pl.ds(r, chunk), :] = total.astype(o_ref.dtype)
                        return 0

                    lax.fori_loop(0, rows // chunk, step_, 0)

                if nz == 1:
                    body(False, False)
                else:
                    lo, hi = z >= 1, z + 1 < nz
                    pl.when(jnp.logical_and(lo, hi))(lambda: body(True, True))
                    pl.when(jnp.logical_and(lo, jnp.logical_not(hi)))(lambda: body(True, False))
                    pl.when(jnp.logical_and(jnp.logical_not(lo), hi))(lambda: body(False, True))

        when(ok, fn)

    groups = [[st for st in steps if st[0] == d] for d in reversed(range(nz))]

    def phase(t):
        if t < nz:
            for st in groups[t]:
                first(st)
        if 0 <= t - 1 < nz:
            for st in groups[t - 1]:
                second(st)
        if 0 <= t - 2 < nz:
            for st in groups[t - 2]:
                third(st)

    def last():
        for d, side, s, ok in steps:

            def fn():
                for rel, px, py in rels:
                    if uc:
                        give(s, rel, px, py).wait_send()
                if ux and uy:
                    over_a(s).wait_send()
                    over_b(s).wait_send()
                if ux:
                    x_half(s, 0).wait_send()
                    x_half(s, 1).wait_send()
                if uy:
                    y_half(s, 0).wait_send()
                    y_half(s, 1).wait_send()
                if d > 0:
                    z_send(s, side == 1).wait_send()

            when(ok, fn)

    return begin, [functools.partial(phase, t) for t in range(nz + 2)], last


def scatter_kernel(axes_list, *refs):
    n = len(axes_list)
    jobs = [
        scatter_job(axes_list[i], refs[i], refs[n + i], *refs[2 * n + 10 * i : 2 * n + 10 * i + 10])
        for i in range(n)
    ]
    run_jobs(axes_list, jobs)


def scatter_scratch(axes, rows, cols, dt):
    nz, ux, uy, uc = axes
    few = lambda use, n, r: pltpu.VMEM((n, r, cols) if use else (1, 16, cols), dt)
    return [
        few(True, nz * 4, rows),
        few(uc, nz * 4, rows),
        few(ux, nz, rows),
        few(uy, nz, rows),
        few(ux and uy, nz, rows // 2),
        few(ux and uy, nz, rows // 2),
        few(nz > 1, nz + 1, rows),
        pltpu.SemaphoreType.DMA((nz * 12,)),
        pltpu.SemaphoreType.DMA((nz * 12,)),
        pltpu.SemaphoreType.DMA((nz * 4,)),
    ]


def reduce_scatter(parts, axes_list, collective_id):
    return pl.pallas_call(
        functools.partial(scatter_kernel, axes_list),
        out_shape=[jax.ShapeDtypeStruct(p.shape[1:], jnp.float32) for p in parts],
        in_specs=[pl.BlockSpec(memory_space=pl.ANY)] * len(parts),
        out_specs=[pl.BlockSpec(memory_space=pltpu.VMEM)] * len(parts),
        scratch_shapes=[
            x
            for axes, p in zip(axes_list, parts)
            for x in scatter_scratch(axes, p.shape[1], p.shape[2], p.dtype)
        ],
        compiler_params=pltpu.CompilerParams(
            collective_id=collective_id, has_side_effects=True, vmem_limit_bytes=60 * 1024 * 1024
        ),
    )(*parts)


LOG2E = 1.4426950408889634


def lane_swap(tensor):
    return pltpu.roll(tensor, tensor.shape[-1] // 2, tensor.ndim - 1)


def head_norm(tensor, gain, cos2, sin2):
    inverse = lax.rsqrt(jnp.mean(tensor * tensor, axis=-1, keepdims=True) + EPSILON)
    scaled = tensor * inverse * gain
    return scaled * cos2 + lane_swap(scaled) * sin2


def head_norm_back(tensor, gain, cos2, sin2, gradient):
    inverse = lax.rsqrt(jnp.mean(tensor * tensor, axis=-1, keepdims=True) + EPSILON)
    turned = gradient * cos2 - lane_swap(gradient) * sin2
    weighted = turned * gain
    inner = jnp.mean(weighted * tensor, axis=-1, keepdims=True)
    return (
        inverse * weighted - tensor * (inverse * inverse * inverse) * inner,
        turned * tensor * inverse,
    )


def token_rows(piece, seq, seq_count, rows_dev):
    return (piece * seq_count + seq) * rows_dev


def kv_prep_kernel(pieces, seqs, proj_ref, gain_ref, cos_ref, sin_ref, o_ref):
    hd = gain_ref.shape[-1]
    rows = proj_ref.shape[0] // (pieces * seqs)
    for piece in range(pieces):
        cos2 = cos_ref[piece * rows : (piece + 1) * rows, :]
        sin2 = sin_ref[piece * rows : (piece + 1) * rows, :]
        for seq in range(seqs):
            at = token_rows(piece, seq, seqs, rows)
            raw = proj_ref[at : at + rows, :hd]
            o_ref[at : at + rows, :hd] = head_norm(raw, gain_ref[...], cos2, sin2).astype(
                o_ref.dtype
            )
            o_ref[at : at + rows, hd:] = proj_ref[at : at + rows, hd:].astype(o_ref.dtype)


def kv_prep(projected, key_gain, cos2, sin2, heads, pieces, seqs):
    rows, _ = projected.shape
    hd = key_gain.shape[0]
    whole = lambda *shape: pl.BlockSpec(shape, lambda i: (0,) * len(shape))
    return pl.pallas_call(
        functools.partial(kv_prep_kernel, pieces, seqs),
        grid=(1,),
        out_shape=jax.ShapeDtypeStruct((rows, 2 * hd), jnp.bfloat16),
        in_specs=[
            pl.BlockSpec((rows, 2 * hd), lambda i: (0, heads // 2)),
            whole(1, hd),
            whole(*cos2.shape),
            whole(*sin2.shape),
        ],
        out_specs=whole(rows, 2 * hd),
        name="kv_prep",
    )(projected, key_gain.reshape(1, hd), cos2, sin2)


def kv_back_kernel(pieces, seqs, proj_ref, cot_ref, gain_ref, cos_ref, sin_ref, _, low_ref, gg_ref):
    hd = gain_ref.shape[-1]
    rows = proj_ref.shape[0] // (pieces * seqs)
    total = jnp.zeros((1, hd), jnp.float32)
    for piece in range(pieces):
        cos2 = cos_ref[piece * rows : (piece + 1) * rows, :]
        sin2 = sin_ref[piece * rows : (piece + 1) * rows, :]
        for seq in range(seqs):
            at = token_rows(piece, seq, seqs, rows)
            grad, terms = head_norm_back(
                proj_ref[at : at + rows, :hd],
                gain_ref[...],
                cos2,
                sin2,
                cot_ref[at : at + rows, :hd],
            )
            low_ref[at : at + rows, :hd] = grad.astype(low_ref.dtype)
            low_ref[at : at + rows, hd:] = cot_ref[at : at + rows, hd:].astype(low_ref.dtype)
            total = total + jnp.sum(terms, axis=0, keepdims=True)
    gg_ref[...] = total


def kv_back(projected, kv_cot, key_gain, cos2, sin2, low, heads, pieces, seqs):
    rows, _ = projected.shape
    hd = key_gain.shape[0]
    whole = lambda *shape: pl.BlockSpec(shape, lambda i: (0,) * len(shape))
    return pl.pallas_call(
        functools.partial(kv_back_kernel, pieces, seqs),
        grid=(1,),
        out_shape=(
            jax.ShapeDtypeStruct(low.shape, low.dtype),
            jax.ShapeDtypeStruct((1, hd), jnp.float32),
        ),
        in_specs=[
            pl.BlockSpec((rows, 2 * hd), lambda i: (0, heads // 2)),
            whole(rows, 2 * hd),
            whole(1, hd),
            whole(*cos2.shape),
            whole(*sin2.shape),
            pl.BlockSpec(memory_space=pl.ANY),
        ],
        out_specs=(pl.BlockSpec((rows, 2 * hd), lambda i: (0, heads // 2)), whole(1, hd)),
        input_output_aliases={5: 0},
        name="kv_back",
    )(projected, kv_cot, key_gain.reshape(1, hd), cos2, sin2, low)


def sort_blocks(loc_ref, kv_ref, dst, seqs, rows, pieces, hd, lo, blocks):
    per_half = pieces // 2

    def body(b, _):
        loc = loc_ref[b]
        chunk, half = loc // 2, loc % 2
        for seq in range(seqs):
            for i in range(per_half):
                at = ((half * per_half + i) * seqs + seq) * rows
                dst[seq, pl.ds(b * (per_half * rows) + i * rows, rows), :] = kv_ref[
                    chunk, pl.ds(at, rows), lo : lo + hd
                ]
        return 0

    lax.fori_loop(0, blocks, body, 0)


def attend_kernel(
    heads, pieces, seqs, scale, loc_ref, own_ref, proj_ref, kv_ref, gain_ref, cos_ref, sin_ref,
    attn_ref, lse_ref, qs_ref, ks, vs, acc, tot,
):
    f32, bf16 = jnp.float32, jnp.bfloat16
    hd = gain_ref.shape[-1]
    rows = proj_ref.shape[0] // (pieces * seqs)
    per_half = pieces // 2
    block = per_half * rows
    blocks = 2 * kv_ref.shape[0]
    pair = 2 * block
    tile = 2 * block
    sort_blocks(loc_ref, kv_ref, ks, seqs, rows, pieces, hd, 0, blocks)
    sort_blocks(loc_ref, kv_ref, vs, seqs, rows, pieces, hd, hd, blocks)
    for seq in range(seqs):
        for half in range(2):
            unit = seq * 2 + half
            for h in range(heads):
                for i in range(per_half):
                    piece = half * per_half + i
                    at = token_rows(piece, seq, seqs, rows)
                    turned = head_norm(
                        proj_ref[at : at + rows, h * hd : (h + 1) * hd],
                        gain_ref[...],
                        cos_ref[piece * rows : (piece + 1) * rows, :],
                        sin_ref[piece * rows : (piece + 1) * rows, :],
                    )
                    qs_ref[unit, h * block + i * rows : h * block + (i + 1) * rows, :] = (
                        turned.astype(bf16)
                    )
            acc[...] = jnp.zeros_like(acc)
            tot[...] = jnp.zeros_like(tot)
            mine = own_ref[half]

            def step(j, masked):
                keys = ks[seq, pl.ds(j * pair, pair), :]
                values = vs[seq, pl.ds(j * pair, pair), :]
                for t in range(heads * block // tile):
                    cols = slice(t * tile, (t + 1) * tile)
                    scores = lax.dot_general(
                        keys,
                        qs_ref[unit, cols, :],
                        (((1,), (1,)), ((), ())),
                        preferred_element_type=f32,
                    )
                    expo = jnp.exp2(scores * (scale * LOG2E))
                    if masked:
                        key_pos = j * pair + lax.broadcasted_iota(jnp.int32, expo.shape, 0)
                        query_pos = mine * block + (
                            lax.broadcasted_iota(jnp.int32, expo.shape, 1) % block
                        )
                        expo = jnp.where(key_pos <= query_pos, expo, 0.0)
                    tot[:, cols] += jnp.sum(expo.reshape(pair // 8, 8, tile), axis=0)
                    acc[:, cols] += lax.dot_general(
                        values,
                        expo.astype(bf16),
                        (((0,), (0,)), ((), ())),
                        preferred_element_type=f32,
                    )

            def body(j, _):
                step(j, False)
                return 0

            lax.fori_loop(0, mine // 2, body, 0)
            step(mine // 2, True)
            total = jnp.sum(tot[...], axis=0, keepdims=True)
            lse_ref[unit, :, :] = jnp.log(total)
            share = 1.0 / total
            for h in range(heads):
                cols = slice(h * block, (h + 1) * block)
                out = jnp.transpose(acc[:, cols] * share[:, cols]).astype(bf16)
                for i in range(per_half):
                    at = token_rows(half * per_half + i, seq, seqs, rows)
                    attn_ref[at : at + rows, h * hd : (h + 1) * hd] = out[
                        i * rows : (i + 1) * rows, :
                    ]


def attend(projected, kv_all, query_gain, cos2, sin2, loc, own, heads, pieces, seqs):
    rows = projected.shape[0]
    hd = query_gain.shape[0]
    units = 2 * seqs
    block = rows // units
    keys = kv_all.shape[0] * kv_all.shape[1] // seqs
    whole = lambda *shape: pl.BlockSpec(shape, lambda i, *_: (0,) * len(shape))
    f32, bf16 = jnp.float32, jnp.bfloat16
    return pl.pallas_call(
        functools.partial(attend_kernel, heads, pieces, seqs, hd**-0.5),
        grid_spec=pltpu.PrefetchScalarGridSpec(
            num_scalar_prefetch=2,
            grid=(1,),
            in_specs=[
                pl.BlockSpec((rows, heads * hd), lambda i, *_: (0, 0)),
                whole(*kv_all.shape),
                whole(1, hd),
                whole(*cos2.shape),
                whole(*sin2.shape),
            ],
            out_specs=[
                whole(rows, heads * hd),
                whole(units, 1, heads * block),
                whole(units, heads * block, hd),
            ],
            scratch_shapes=[
                pltpu.VMEM((seqs, keys, hd), bf16),
                pltpu.VMEM((seqs, keys, hd), bf16),
                pltpu.VMEM((hd, heads * block), f32),
                pltpu.VMEM((8, heads * block), f32),
            ],
        ),
        out_shape=(
            jax.ShapeDtypeStruct((rows, heads * hd), bf16),
            jax.ShapeDtypeStruct((units, 1, heads * block), f32),
            jax.ShapeDtypeStruct((units, heads * block, hd), bf16),
        ),
        compiler_params=pltpu.CompilerParams(vmem_limit_bytes=56 * 1024 * 1024),
        name="attend",
    )(loc, own, projected, kv_all, query_gain.reshape(1, hd), cos2, sin2)


def attend_back_kernel(
    heads, pieces, seqs, scale, loc_ref, own_ref, proj_ref, kv_ref, qs_ref, attn_ref, cot_ref,
    lse_ref, gain_ref, cos_ref, sin_ref, low_ref, dkv_ref, gg_ref, ks, vs, dk, dv, dq, cs, dl,
):
    f32, bf16 = jnp.float32, jnp.bfloat16
    hd = gain_ref.shape[-1]
    rows = proj_ref.shape[0] // (pieces * seqs)
    per_half = pieces // 2
    block = per_half * rows
    blocks = 2 * kv_ref.shape[0]
    pair = 2 * block
    tile = 2 * block
    sort_blocks(loc_ref, kv_ref, ks, seqs, rows, pieces, hd, 0, blocks)
    sort_blocks(loc_ref, kv_ref, vs, seqs, rows, pieces, hd, hd, blocks)
    dk[...] = jnp.zeros_like(dk)
    dv[...] = jnp.zeros_like(dv)
    gain_total = jnp.zeros((1, hd), f32)
    ones = jnp.ones((8, hd), bf16)
    nt = (((1,), (1,)), ((), ()))
    for seq in range(seqs):
        for half in range(2):
            unit = seq * 2 + half
            for h in range(heads):
                for i in range(per_half):
                    at = token_rows(half * per_half + i, seq, seqs, rows)
                    to = slice(h * block + i * rows, h * block + (i + 1) * rows)
                    part = cot_ref[at : at + rows, h * hd : (h + 1) * hd]
                    cs[to, :] = part
                    prod = part.astype(f32) * attn_ref[
                        at : at + rows, h * hd : (h + 1) * hd
                    ].astype(f32)
                    dq[to, :] = prod
            for t in range(heads * block // tile):
                cols = slice(t * tile, (t + 1) * tile)
                prod = dq[cols, :]
                high = prod.astype(bf16)
                rest = (prod - high.astype(f32)).astype(bf16)
                dl[:, cols] = lax.dot_general(
                    ones, high, nt, preferred_element_type=f32
                ) + lax.dot_general(ones, rest, nt, preferred_element_type=f32)
            dq[...] = jnp.zeros_like(dq)
            mine = own_ref[half]

            def step(j, masked):
                at = pl.ds(j * pair, pair)
                keys = ks[seq, at, :]
                values = vs[seq, at, :]
                key_sum = jnp.zeros((pair, hd), f32)
                value_sum = jnp.zeros((pair, hd), f32)
                for t in range(heads * block // tile):
                    cols = slice(t * tile, (t + 1) * tile)
                    query = qs_ref[unit, cols, :]
                    cot = cs[cols, :]
                    scores = lax.dot_general(keys, query, nt, preferred_element_type=f32)
                    weights = jnp.exp2(
                        scores * (scale * LOG2E) - lse_ref[unit, :, cols] * LOG2E
                    )
                    if masked:
                        key_pos = j * pair + lax.broadcasted_iota(jnp.int32, weights.shape, 0)
                        query_pos = mine * block + (
                            lax.broadcasted_iota(jnp.int32, weights.shape, 1) % block
                        )
                        weights = jnp.where(key_pos <= query_pos, weights, 0.0)
                    prob_cot = lax.dot_general(values, cot, nt, preferred_element_type=f32)
                    low = (weights * (prob_cot - dl[0:1, cols])).astype(bf16)
                    value_sum = value_sum + jnp.dot(
                        weights.astype(bf16), cot, preferred_element_type=f32
                    )
                    key_sum = key_sum + jnp.dot(low, query, preferred_element_type=f32)
                    dq[cols, :] += lax.dot_general(
                        low, keys, (((0,), (0,)), ((), ())), preferred_element_type=f32
                    )
                dk[seq, at, :] += key_sum
                dv[seq, at, :] += value_sum

            def body(j, _):
                step(j, False)
                return 0

            lax.fori_loop(0, mine // 2, body, 0)
            step(mine // 2, True)
            for h in range(heads):
                for i in range(per_half):
                    piece = half * per_half + i
                    at = token_rows(piece, seq, seqs, rows)
                    grad, terms = head_norm_back(
                        proj_ref[at : at + rows, h * hd : (h + 1) * hd],
                        gain_ref[...],
                        cos_ref[piece * rows : (piece + 1) * rows, :],
                        sin_ref[piece * rows : (piece + 1) * rows, :],
                        dq[h * block + i * rows : h * block + (i + 1) * rows, :] * scale,
                    )
                    low_ref[at : at + rows, h * hd : (h + 1) * hd] = grad.astype(bf16)
                    gain_total = gain_total + jnp.sum(terms, axis=0, keepdims=True)
    gg_ref[...] = gain_total

    def unsort(b, _):
        loc = loc_ref[b]
        chunk, half = loc // 2, loc % 2
        for seq in range(seqs):
            for i in range(per_half):
                at = pl.ds(((half * per_half + i) * seqs + seq) * rows, rows)
                here = pl.ds(b * block + i * rows, rows)
                dkv_ref[chunk, at, 0:hd] = (dk[seq, here, :] * scale).astype(bf16)
                dkv_ref[chunk, at, hd : 2 * hd] = dv[seq, here, :].astype(bf16)
        return 0

    lax.fori_loop(0, blocks, unsort, 0)


def attend_back(
    projected, kv_all, rotated, attention, attention_cot, log_total, query_gain, cos2, sin2, loc,
    own, heads, pieces, seqs,
):
    rows, all_cols = projected.shape
    hd = query_gain.shape[0]
    units = 2 * seqs
    block = rows // units
    keys = kv_all.shape[0] * kv_all.shape[1] // seqs
    whole = lambda *shape: pl.BlockSpec(shape, lambda i, *_: (0,) * len(shape))
    f32, bf16 = jnp.float32, jnp.bfloat16
    return pl.pallas_call(
        functools.partial(attend_back_kernel, heads, pieces, seqs, hd**-0.5),
        grid_spec=pltpu.PrefetchScalarGridSpec(
            num_scalar_prefetch=2,
            grid=(1,),
            in_specs=[
                pl.BlockSpec((rows, heads * hd), lambda i, *_: (0, 0)),
                whole(*kv_all.shape),
                whole(*rotated.shape),
                whole(rows, heads * hd),
                whole(rows, heads * hd),
                whole(*log_total.shape),
                whole(1, hd),
                whole(*cos2.shape),
                whole(*sin2.shape),
            ],
            out_specs=[
                pl.BlockSpec((rows, heads * hd), lambda i, *_: (0, 0)),
                whole(*kv_all.shape),
                whole(1, hd),
            ],
            scratch_shapes=[
                pltpu.VMEM((seqs, keys, hd), bf16),
                pltpu.VMEM((seqs, keys, hd), bf16),
                pltpu.VMEM((seqs, keys, hd), f32),
                pltpu.VMEM((seqs, keys, hd), f32),
                pltpu.VMEM((heads * block, hd), f32),
                pltpu.VMEM((heads * block, hd), bf16),
                pltpu.VMEM((8, heads * block), f32),
            ],
        ),
        out_shape=(
            jax.ShapeDtypeStruct((rows, all_cols), bf16),
            jax.ShapeDtypeStruct(kv_all.shape, bf16),
            jax.ShapeDtypeStruct((1, hd), f32),
        ),
        compiler_params=pltpu.CompilerParams(vmem_limit_bytes=60 * 1024 * 1024),
        name="attend_back",
    )(
        loc, own, projected, kv_all, rotated, attention, attention_cot, log_total,
        query_gain.reshape(1, hd), cos2, sin2,
    )


def own_kernels():
    return lax.axis_size("ctx") == 8 and lax.axis_size("wsh") == 4


AXIS_NAMES = {WSH_AXES: "wsh", CTX_AXES: "ctx", ALL_AXES: ("ctx", "wsh")}


def gather(shards, axes_list, ident):
    if own_kernels():
        return all_gather(shards, axes_list, ident)
    return [lax.all_gather(x, AXIS_NAMES[axes], axis=0) for x, axes in zip(shards, axes_list)]


def scatter(parts, axes_list, ident):
    if own_kernels():
        return reduce_scatter(parts, axes_list, ident)
    return [
        lax.psum_scatter(x, AXIS_NAMES[axes], scatter_dimension=0, tiled=False).astype(jnp.float32)
        for x, axes in zip(parts, axes_list)
    ]


def exchange(pieces):
    return lax.all_to_all(pieces, ("ctx", "wsh"), split_axis=0, concat_axis=0, tiled=True)


def to_everyone(value, device_count):
    return exchange(jnp.broadcast_to(value[None], (device_count,) + value.shape))


def local(
    inputs,
    pair_map,
    norm_gain,
    query_weight,
    key_weight,
    value_weight,
    query_gain,
    key_gain,
    out_weight,
    moe_gain,
    router,
    expert_gate,
    expert_up,
    expert_down,
    expert_ids,
    dispatch_slot,
    cotangent,
):
    f32, bf16 = jnp.float32, jnp.bfloat16
    rows_dev, seq_count, width = inputs.shape
    ctx_count = lax.axis_size("ctx")
    wsh_count = lax.axis_size("wsh")
    device_count = ctx_count * wsh_count
    head_dim = query_gain.shape[0]
    group_rows = rows_dev * wsh_count
    block_len = group_rows // 2
    seq_len = group_rows * ctx_count
    tokens = rows_dev * seq_count
    group_tokens = tokens * wsh_count
    top_count = expert_ids.shape[-1]
    expert_count = router.shape[1]
    capacity = max(2, 3 * top_count * block_len // (2 * device_count))
    positions = positions_of(pair_map, seq_len, block_len, pair_map.shape[0])
    me_ctx = lax.axis_index("ctx")
    query_pos = lax.dynamic_slice_in_dim(positions, me_ctx * group_rows, group_rows, 0)
    cosine, sine_table = rope_tables(query_pos, head_dim)
    cos2 = jnp.concatenate([cosine, cosine], axis=1)
    sin2 = jnp.concatenate([-sine_table, sine_table], axis=1)
    block_ids = jnp.arange(2 * ctx_count, dtype=jnp.int32)
    blocks_by_loc = jnp.stack([pair_map, 2 * ctx_count - 1 - pair_map], axis=1).reshape(-1)
    loc = jnp.sum(
        jnp.where(blocks_by_loc[None, :] == block_ids[:, None], block_ids[None, :], 0), axis=1
    ).astype(jnp.int32)
    own_blocks = lax.dynamic_slice_in_dim(blocks_by_loc, 2 * me_ctx, 2, 0)

    inputs_f = inputs.transpose(1, 0, 2).reshape(tokens, width).astype(f32)
    cot_flat = cotangent.transpose(1, 0, 2).reshape(tokens, width)
    normed_f, inverse_one = rms_forward(inputs_f, norm_gain)
    q_cols, kv_cols = query_weight.shape[1], key_weight.shape[1]
    heads_loc = q_cols // head_dim
    qkv_shard = jnp.concatenate([query_weight, key_weight, value_weight], axis=1)
    normed_flat, qkv_full = gather([normed_f.astype(bf16), qkv_shard], [WSH_AXES, CTX_AXES], 1)
    normed_flat = normed_flat.reshape(group_tokens, width)
    qkv_full = qkv_full.reshape(width, q_cols + 2 * kv_cols)
    out_shard, qkv_full = lax.optimization_barrier((out_weight.T, qkv_full))
    out_full = lax.all_gather(out_shard, "ctx", axis=0, tiled=True)
    projected = jnp.dot(normed_flat, qkv_full, preferred_element_type=f32)
    kv_own = kv_prep(projected, key_gain, cos2, sin2, heads_loc, wsh_count, seq_count)
    (kv_all,) = gather([kv_own], [CTX_AXES], 3)
    cot_low, kv_all = lax.optimization_barrier((cot_flat.astype(bf16), kv_all))
    cot_all = lax.all_gather(cot_low, ("ctx", "wsh"), axis=0)

    attention, log_total, rotated = attend(
        projected, kv_all, query_gain, cos2, sin2, loc, own_blocks, heads_loc, wsh_count, seq_count
    )
    mixed = jnp.einsum("tc,dc->td", attention, out_full, preferred_element_type=f32)
    (mixed,) = scatter([mixed.astype(bf16).reshape(wsh_count, tokens, width)], [WSH_AXES], 4)
    residual = inputs_f + mixed

    def rows_first(value):
        return value.reshape(seq_count, rows_dev, width).transpose(1, 0, 2)

    moe_normed_f, inverse_two = rms_forward(residual, moe_gain)
    moe_flat = moe_normed_f.astype(bf16)
    (moe_all,) = gather([moe_flat], [ALL_AXES], 5)
    logits = jnp.dot(moe_flat, router, preferred_element_type=f32)
    route_ids = expert_ids.transpose(1, 0, 2).reshape(tokens, top_count)
    slots = dispatch_slot.transpose(1, 0, 2).reshape(tokens, top_count)
    expert_onehot = (
        route_ids[:, :, None] == jnp.arange(expert_count, dtype=jnp.int32)[None, None, :]
    )
    named = jnp.any(expert_onehot, axis=1)
    slot_dense = jnp.sum(jnp.where(expert_onehot, slots[:, :, None] + 1, 0), axis=1) - 1
    chosen_top = jnp.max(jnp.where(named, logits, MASKED), axis=-1, keepdims=True)
    chosen_exp = jnp.where(named, jnp.exp(jnp.where(named, logits - chosen_top, 0.0)), 0.0)
    weight_dense = chosen_exp / jnp.sum(chosen_exp, axis=-1, keepdims=True)
    routing = exchange(jnp.stack([slot_dense.astype(f32).T, weight_dense.T], axis=1))
    slot_mine = routing[:, 0, :].astype(jnp.int32)
    weight_mine = routing[:, 1, :]
    picks = slot_mine[:, None, :] == jnp.arange(capacity, dtype=jnp.int32)[None, :, None]
    picks_low = picks.astype(bf16)
    slot_weight = jnp.sum(jnp.where(picks, weight_mine[:, None, :], 0.0), axis=-1)

    def take(everyone):
        return (
            jnp.einsum("dct,dtw->dcw", picks_low, everyone, preferred_element_type=f32)
            .astype(bf16)
            .reshape(device_count * capacity, width)
        )

    def put(rows):
        return jnp.einsum(
            "dct,dcw->dtw",
            picks_low,
            rows.reshape(device_count, capacity, width),
            preferred_element_type=f32,
        ).astype(bf16)

    gate_w, up_w, down_w = (expert_gate[0], expert_up[0], expert_down[0])
    rows_in = take(moe_all)
    cot_rows = take(cot_all).astype(f32)
    weight_rows = slot_weight.reshape(device_count * capacity, 1)
    route_cot = (weight_rows * cot_rows).astype(bf16)
    gate_pre = jnp.dot(rows_in, gate_w, preferred_element_type=f32)
    up_pre = jnp.dot(rows_in, up_w, preferred_element_type=f32)
    sigmoid = jax.nn.sigmoid(gate_pre)
    swish = gate_pre * sigmoid
    activation = (swish * up_pre).astype(bf16)
    produced = jnp.dot(activation, down_w, preferred_element_type=f32).astype(bf16).astype(f32)
    out_parts = put((weight_rows * produced).astype(bf16))
    slot_cot = jnp.sum(cot_rows * produced, axis=-1).reshape(device_count, capacity)
    cot_mine = jnp.sum(jnp.where(picks, slot_cot[:, :, None], 0.0), axis=1)
    weight_cot = exchange(cot_mine).T
    down_grad = jnp.einsum("rf,rd->fd", activation, route_cot, preferred_element_type=f32)
    act_cot = jnp.einsum("rd,fd->rf", route_cot, down_w, preferred_element_type=f32)
    gate_cot = (act_cot * up_pre * sigmoid * (1.0 + gate_pre * (1.0 - sigmoid))).astype(bf16)
    up_cot = (act_cot * swish).astype(bf16)
    gate_grad = jnp.einsum("rd,rf->df", rows_in, gate_cot, preferred_element_type=f32)
    up_grad = jnp.einsum("rd,rf->df", rows_in, up_cot, preferred_element_type=f32)
    row_cot = jnp.einsum("rf,df->rd", gate_cot, gate_w, preferred_element_type=f32)
    row_cot = row_cot + jnp.einsum("rf,df->rd", up_cot, up_w, preferred_element_type=f32)
    (row_sum,) = scatter([put(row_cot.astype(bf16))], [ALL_AXES], 6)
    out_parts, row_sum = lax.optimization_barrier((out_parts, row_sum))
    moe_sum = lax.psum_scatter(
        out_parts, ("ctx", "wsh"), scatter_dimension=0, tiled=False
    ).astype(f32)

    chosen_cot = weight_dense * (
        weight_cot - jnp.sum(weight_dense * weight_cot, axis=-1, keepdims=True)
    )
    logit_cot = chosen_cot.astype(bf16)
    if device_count > 32:
        router_grad = lax.psum(
            jnp.einsum("td,te->de", moe_flat, logit_cot, preferred_element_type=f32),
            ("ctx", "wsh"),
        )
    else:
        router_grad = jnp.einsum(
            "td,te->de",
            moe_all.reshape(device_count * tokens, width),
            to_everyone(logit_cot, device_count).reshape(device_count * tokens, expert_count),
            preferred_element_type=f32,
        )
    normed_two_cot = (
        jnp.einsum("te,de->td", logit_cot, router, preferred_element_type=f32) + row_sum
    )
    residual_norm_cot, moe_gain_grad = rms_backward(
        residual, inverse_two, moe_gain, normed_two_cot
    )
    residual_cot = cot_flat + residual_norm_cot
    residual_low = residual_cot.astype(bf16)
    (residual_flat,) = gather([residual_low], [WSH_AXES], 8)
    residual_flat = residual_flat.reshape(group_tokens, width)

    attention_cot = jnp.einsum(
        "td,dc->tc", residual_flat, out_full, preferred_element_type=f32
    ).astype(bf16)
    low, kv_sums, query_gain_grad = attend_back(
        projected,
        kv_all,
        rotated,
        attention,
        attention_cot,
        log_total,
        query_gain,
        cos2,
        sin2,
        loc,
        own_blocks,
        heads_loc,
        wsh_count,
        seq_count,
    )
    out_grad = jnp.einsum("td,tc->dc", residual_flat, attention, preferred_element_type=f32).astype(
        bf16
    )
    out_grad, kv_sums = lax.optimization_barrier((out_grad, kv_sums))
    out_weight_grad = lax.psum_scatter(out_grad, "ctx", scatter_dimension=0, tiled=True)
    out_weight_grad = out_weight_grad.astype(f32).T
    (kv_cot,) = scatter([kv_sums], [CTX_AXES], 9)
    low, key_gain_grad = kv_back(
        projected, kv_cot, key_gain, cos2, sin2, low, heads_loc, wsh_count, seq_count
    )
    summed = jnp.einsum("tq,cq->tc", low, qkv_full, preferred_element_type=f32)
    qkv_grad = jnp.einsum("tc,tq->cq", normed_flat, low, preferred_element_type=f32).astype(bf16)
    normed_cot, qkv_grad = scatter(
        [
            summed.astype(bf16).reshape(wsh_count, tokens, width),
            qkv_grad.reshape(ctx_count, width // ctx_count, q_cols + 2 * kv_cols),
        ],
        [WSH_AXES, CTX_AXES],
        10,
    )
    value_weight_grad = qkv_grad[:, q_cols + kv_cols :]
    moe_sum, value_weight_grad = lax.optimization_barrier((moe_sum, value_weight_grad))
    outputs = rows_first((residual + moe_sum).astype(bf16))
    input_norm_cot, norm_gain_grad = rms_backward(inputs_f, inverse_one, norm_gain, normed_cot)
    input_grad = rows_first(residual_cot + input_norm_cot)
    query_gain_grad = query_gain_grad.reshape(head_dim)
    key_gain_grad = key_gain_grad.reshape(head_dim)
    gains = jnp.concatenate([norm_gain_grad, moe_gain_grad, query_gain_grad, key_gain_grad])
    gains = jnp.sum(to_everyone(gains, device_count), axis=0)
    return (
        outputs,
        input_grad,
        gains[:width],
        qkv_grad[:, :q_cols],
        qkv_grad[:, q_cols : q_cols + kv_cols],
        value_weight_grad,
        gains[2 * width : 2 * width + head_dim],
        gains[2 * width + head_dim :],
        out_weight_grad,
        gains[width : 2 * width],
        router_grad,
        gate_grad[None],
        up_grad[None],
        down_grad[None],
    )


def solution(mesh):
    return jax.shard_map(
        local,
        mesh=mesh,
        in_specs=(
            P(("ctx", "wsh"), None, None),
            P(),
            P(),
            P("ctx", "wsh"),
            P("ctx", "wsh"),
            P("ctx", "wsh"),
            P(),
            P(),
            P("wsh", "ctx"),
            P(),
            P(),
            P(("ctx", "wsh"), None, None),
            P(("ctx", "wsh"), None, None),
            P(("ctx", "wsh"), None, None),
            P(("ctx", "wsh"), None, None),
            P(("ctx", "wsh"), None, None),
            P(("ctx", "wsh"), None, None),
        ),
        out_specs=(
            P(("ctx", "wsh"), None, None),
            P(("ctx", "wsh"), None, None),
            P(),
            P("ctx", "wsh"),
            P("ctx", "wsh"),
            P("ctx", "wsh"),
            P(),
            P(),
            P("wsh", "ctx"),
            P(),
            P(),
            P(("ctx", "wsh"), None, None),
            P(("ctx", "wsh"), None, None),
            P(("ctx", "wsh"), None, None),
        ),
        check_vma=False,
    )
```

```python
import functools
import math

import jax
import jax.numpy as jnp
from jax import lax
from jax.experimental import pallas as pl
from jax.experimental.pallas import tpu as pltpu
from jax.sharding import PartitionSpec as P


EPSILON = 1e-06
ROPE_BASE = 1000000.0
MASKED = -1e30


def positions_of(pair_map, seq_len, block_len, group_count):
    row_index = jnp.arange(seq_len, dtype=jnp.int32)
    owner_group = row_index // (2 * block_len)
    inner_row = row_index % (2 * block_len)
    group_table = jnp.arange(group_count, dtype=jnp.int32)
    pair_index = jnp.sum(
        jnp.where(owner_group[:, None] == group_table[None, :], pair_map[None, :], 0), axis=1
    )
    block_index = jnp.where(inner_row < block_len, pair_index, 2 * group_count - 1 - pair_index)
    return block_index * block_len + inner_row % block_len


def rope_tables(positions, head_dim):
    half_dim = head_dim // 2
    frequency = ROPE_BASE ** (-(jnp.arange(half_dim, dtype=jnp.float32) * 2.0) / head_dim)
    angles = positions.astype(jnp.float32)[:, None] * frequency[None, :]
    return (jnp.cos(angles), jnp.sin(angles))


def rms_forward(tensor, gain_vector):
    inverse = lax.rsqrt(jnp.mean(tensor * tensor, axis=-1, keepdims=True) + EPSILON)
    return (tensor * inverse * gain_vector, inverse)


def rms_backward(tensor, inverse, gain_vector, gradient):
    weighted = gradient * gain_vector
    inner_mean = jnp.mean(weighted * tensor, axis=-1, keepdims=True)
    tensor_grad = inverse * weighted - tensor * inverse**3 * inner_mean
    gain_grad = jnp.sum((gradient * tensor * inverse).reshape(-1, tensor.shape[-1]), axis=0)
    return (tensor_grad, gain_grad)


MESH_ID = pl.DeviceIdType.MESH


class Place:
    def __init__(self, nz, ux, uy, uc):
        ci, wi = lax.axis_index("ctx"), lax.axis_index("wsh")
        self.nz, self.ux, self.uy, self.uc = nz, ux, uy, uc
        self.z, self.x, self.y, self.c = ci // 2, ci % 2, wi // 2, wi % 2

    def dev(self, z, x, y, c):
        return (z * 2 + x, y * 2 + c)

    def blk(self, z, x, y, c):
        if self.ux and self.uc:
            return (z * 2 + x) * 4 + y * 2 + c
        if self.ux:
            return z * 2 + x
        return y * 2 + c

    def greet(self):
        z, x, y, c, nz = self.z, self.x, self.y, self.c, self.nz
        barrier = pltpu.get_barrier_semaphore()
        count = 0
        if nz > 1:
            for step in (-1, 1):
                ok = jnp.logical_and(z + step >= 0, z + step < nz)

                @pl.when(ok)
                def _():
                    pl.semaphore_signal(
                        barrier, inc=1, device_id=self.dev(z + step, x, y, c), device_id_type=MESH_ID
                    )

                count = count + ok.astype(jnp.int32)
        for use, place in (
            (self.ux, (z, 1 - x, y, c)),
            (self.uy, (z, x, 1 - y, c)),
            (self.uc, (z, x, y, 1 - c)),
        ):
            if use:
                pl.semaphore_signal(
                    barrier, inc=1, device_id=self.dev(*place), device_id_type=MESH_ID
                )
                count = count + 1
        pl.semaphore_wait(barrier, count)

    def line_steps(self):
        steps = [(0, 0, self.z, None)]
        for d in range(1, self.nz):
            steps.append((d, 0, self.z - d, self.z - d >= 0))
            steps.append((d, 1, self.z + d, self.z + d < self.nz))
        return steps


def both(a, b):
    if a is None or b is None:
        return a if b is None else b
    return a.astype(jnp.int32) * b.astype(jnp.int32) > 0


def when(cond, fn):
    if cond is None:
        fn()
    else:
        pl.when(cond)(fn)


def gather_line_first(axes, lo, rows, x_ref, o_ref, ssem, rsem):
    nz, ux, uy, uc = axes
    pc = Place(nz, ux, uy, uc)
    z, x, y, c = pc.z, pc.x, pc.y, pc.c
    half = rows // 2
    x_ref = x_ref.at[pl.ds(lo, rows)]
    to_x, to_y, to_c = pc.dev(z, 1 - x, y, c), pc.dev(z, x, 1 - y, c), pc.dev(z, x, y, 1 - c)

    def part(b, p):
        if p == 0:
            return o_ref.at[b, pl.ds(lo, rows)]
        return o_ref.at[b, pl.ds(lo + (p - 1) * half, half)]

    def sid(d, side, kind):
        return (d * 2 + side) * 10 + kind

    def copy(b, p, sidx, ridx, device, src=None):
        return pltpu.make_async_remote_copy(
            src_ref=part(b, p) if src is None else src,
            dst_ref=part(b, p),
            send_sem=ssem.at[sidx],
            recv_sem=rsem.at[ridx],
            device_id=device,
            device_id_type=MESH_ID,
        )

    def hops(d, side, s):
        out = []
        if nz > 1:
            b = pc.blk(s, x, y, c)
            src = x_ref if d == 0 else None
            if d == 0 or side == 0:
                if d + 1 < nz:
                    out.append(
                        (z + 1 < nz, copy(b, 0, sid(d, 0, 0), sid(d + 1, 0, 0), pc.dev(z + 1, x, y, c), src))
                    )
            if d == 0 or side == 1:
                if d + 1 < nz:
                    out.append(
                        (z >= 1, copy(b, 0, sid(d, 1, 0), sid(d + 1, 1, 0), pc.dev(z - 1, x, y, c), src))
                    )
        return out

    def spread(d, side, s):
        b = pc.blk(s, x, y, c)
        src = x_ref if d == 0 else None
        out = []
        if ux:
            out.append(copy(b, 0, sid(d, side, 1), sid(d, side, 1), to_x, src))
        if uy:
            out.append(copy(b, 0, sid(d, side, 2), sid(d, side, 2), to_y, src))
        if uc:
            out.append(copy(b, 0, sid(d, side, 5), sid(d, side, 5), to_c, src))
        return out

    def passed(d, side, s):
        out = []
        if ux:
            b = pc.blk(s, 1 - x, y, c)
            arrive = copy(b, 0, sid(d, side, 1), sid(d, side, 1), to_x)
            go = []
            if uy:
                go.append(copy(b, 1, sid(d, side, 3), sid(d, side, 3), to_y))
            if uc:
                go.append(copy(b, 0, sid(d, side, 6), sid(d, side, 6), to_c))
            out.append((arrive, go))
        if uy:
            b = pc.blk(s, x, 1 - y, c)
            arrive = copy(b, 0, sid(d, side, 2), sid(d, side, 2), to_y)
            go = []
            if ux:
                go.append(copy(b, 2, sid(d, side, 4), sid(d, side, 4), to_x))
            if uc:
                go.append(copy(b, 0, sid(d, side, 7), sid(d, side, 7), to_c))
            out.append((arrive, go))
        return out

    def across(d, side, s):
        out = []
        if ux and uy:
            b = pc.blk(s, 1 - x, 1 - y, c)
            arrive = copy(b, 1, sid(d, side, 3), sid(d, side, 3), to_y)
            go = [copy(b, 1, sid(d, side, 8), sid(d, side, 8), to_c)] if uc else []
            out.append((arrive, go))
            arrive = copy(b, 2, sid(d, side, 4), sid(d, side, 4), to_x)
            go = [copy(b, 2, sid(d, side, 9), sid(d, side, 9), to_c)] if uc else []
            out.append((arrive, go))
        return out

    def partner(d, side, s):
        out = []
        if uc:
            out.append(copy(pc.blk(s, x, y, 1 - c), 0, 0, sid(d, side, 5), to_c))
            if ux:
                out.append(copy(pc.blk(s, 1 - x, y, 1 - c), 0, 0, sid(d, side, 6), to_c))
            if uy:
                out.append(copy(pc.blk(s, x, 1 - y, 1 - c), 0, 0, sid(d, side, 7), to_c))
            if ux and uy:
                b = pc.blk(s, 1 - x, 1 - y, 1 - c)
                out.append(copy(b, 1, 0, sid(d, side, 8), to_c))
                out.append(copy(b, 2, 0, sid(d, side, 9), to_c))
        return out

    steps = pc.line_steps()

    def do_line(step):
        d, side, s, ok = step

        def fn():
            if d > 0:
                copy(pc.blk(s, x, y, c), 0, 0, sid(d, side, 0), to_x).wait_recv()
            for cond, cp in hops(d, side, s):
                when(cond, cp.start)
            for cp in spread(d, side, s):
                cp.start()

        when(ok, fn)

    def do_pass(step, which):
        d, side, s, ok = step

        def fn():
            for arrive, go in which(d, side, s):
                arrive.wait_recv()
                for cp in go:
                    cp.start()

        when(ok, fn)

    groups = [[st for st in steps if st[0] == d] for d in range(nz)]

    def phase(t):
        if t < nz:
            for st in groups[t]:
                do_line(st)
        if 0 <= t - 1 < nz:
            for st in groups[t - 1]:
                do_pass(st, passed)
        if 0 <= t - 2 < nz:
            for st in groups[t - 2]:
                do_pass(st, across)

    def last():
        for st in steps:
            d, side, s, ok = st

            def fn():
                for cp in partner(d, side, s):
                    cp.wait_recv()
                for cond, cp in hops(d, side, s):
                    when(cond, cp.wait_send)
                for cp in spread(d, side, s):
                    cp.wait_send()
                for which in (passed, across):
                    for _, go in which(d, side, s):
                        for cp in go:
                            cp.wait_send()

            when(ok, fn)

    return lambda: None, [functools.partial(phase, t) for t in range(nz + 2)], last


def gather_plane_first(axes, lo, rows, x_ref, o_ref, ssem, rsem):
    nz, ux, uy, uc = axes
    pc = Place(nz, ux, uy, uc)
    z, x, y, c = pc.z, pc.x, pc.y, pc.c
    half = rows // 2
    own = x_ref.at[pl.ds(lo, rows)]
    to_x, to_y, to_c = pc.dev(z, 1 - x, y, c), pc.dev(z, x, 1 - y, c), pc.dev(z, x, y, 1 - c)
    items = [(0, 0, x, y, (lo, rows))]
    if ux:
        items.append((1, 1, 1 - x, y, (lo, rows)))
    if uy:
        items.append((2, 1, x, 1 - y, (lo, rows)))
    if ux and uy:
        items.append((3, 2, 1 - x, 1 - y, (lo, half)))
        items.append((4, 2, 1 - x, 1 - y, (lo + half, half)))
    per = 5
    base = nz * 2 * per

    def iid(d, side, item):
        return (d * 2 + side) * per + item

    def copy(s, px, py, core, span, sidx, ridx, device, src=None):
        ref = o_ref.at[pc.blk(s, px, py, core), pl.ds(span[0], span[1])]
        return pltpu.make_async_remote_copy(
            src_ref=ref if src is None else src,
            dst_ref=ref,
            send_sem=ssem.at[sidx],
            recv_sem=rsem.at[ridx],
            device_id=device,
            device_id_type=MESH_ID,
        )

    def arrival(d, side, s, it):
        item, _, px, py, span = it
        return copy(s, px, py, c, span, 0, iid(d, side, item), to_x)

    def outgoing(d, side, s, it):
        item, _, px, py, span = it
        src = own if d == 0 and item == 0 else None
        out = []
        if d + 1 < nz:
            if d == 0 or side == 0:
                out.append(
                    (
                        z + 1 < nz,
                        copy(s, px, py, c, span, iid(d, 0, item), iid(d + 1, 0, item), pc.dev(z + 1, x, y, c), src),
                    )
                )
            if d == 0 or side == 1:
                out.append(
                    (
                        z >= 1,
                        copy(s, px, py, c, span, iid(d, 1, item), iid(d + 1, 1, item), pc.dev(z - 1, x, y, c), src),
                    )
                )
        if uc:
            at = base + iid(d, side, item)
            out.append((None, copy(s, px, py, c, span, at, at, to_c, src)))
        if d == 0:
            if item == 0 and ux:
                out.append((None, copy(s, px, py, c, span, 2 * base, iid(0, 0, 1), to_x, src)))
            if item == 0 and uy:
                out.append((None, copy(s, px, py, c, span, 2 * base + 1, iid(0, 0, 2), to_y, src)))
            if item == 1 and uy:
                out.append(
                    (None, copy(s, px, py, c, (lo, half), 2 * base + 2, iid(0, 0, 3), to_y))
                )
            if item == 2 and ux:
                out.append(
                    (None, copy(s, px, py, c, (lo + half, half), 2 * base + 3, iid(0, 0, 4), to_x))
                )
        return out

    steps = pc.line_steps()

    def phase(t):
        for d, side, s, ok in steps:
            for it in items:
                if d + it[1] != t:
                    continue

                if d > 0 or it[0] > 0:
                    when(ok, arrival(d, side, s, it).wait_recv)
                for cond, cp in outgoing(d, side, s, it):
                    when(both(ok, cond), cp.start)

    def last():
        for d, side, s, ok in steps:

            for it in items:
                if uc:
                    item, _, px, py, span = it
                    there = copy(s, px, py, 1 - c, span, 0, base + iid(d, side, item), to_c)
                    when(ok, there.wait_recv)
                for cond, cp in outgoing(d, side, s, it):
                    when(both(ok, cond), cp.wait_send)

    return lambda: None, [functools.partial(phase, t) for t in range(nz + 2)], last


WSH_AXES = (1, False, True, True)
CTX_AXES = (4, True, False, False)
ALL_AXES = (4, True, True, True)


def spans_of(axes, rows):
    if axes[0] == 1 or rows % 128:
        return rows, 0
    second = rows // 4 if axes[3] else rows // 8
    return rows - second, second


def run_jobs(axes_list, jobs):
    Place(
        max(a[0] for a in axes_list),
        any(a[1] for a in axes_list),
        any(a[2] for a in axes_list),
        any(a[3] for a in axes_list),
    ).greet()
    for begin, _, _ in jobs:
        begin()
    for t in range(max(len(phases) for _, phases, _ in jobs)):
        for _, phases, _ in jobs:
            if t < len(phases):
                phases[t]()
    for _, _, last in jobs:
        last()


def group_of(axes):
    return (axes[0] * 2 if axes[1] else 1) * (4 if axes[3] else 1)


GATHER_REFS, SCATTER_REFS = 5, 20


def gather_scratch(axes):
    dma = pltpu.SemaphoreType.DMA
    nz = axes[0]
    return [dma((nz * 20,)), dma((nz * 20,)), dma((nz * 20 + 4,)), dma((nz * 20,)), dma]


def gather_jobs(axes, x_ref, o_ref, s1, r1, s2, r2, lsem):
    pc = Place(*axes)
    rows = x_ref.shape[0]
    main, rest = spans_of(axes, rows)
    own = pltpu.make_async_copy(x_ref, o_ref.at[pc.blk(pc.z, pc.x, pc.y, pc.c)], lsem)
    _, phases, last = gather_line_first(axes, 0, main, x_ref, o_ref, s1, r1)

    def end():
        last()
        own.wait()

    jobs = [(own.start, phases, end)]
    if rest:
        jobs.append(gather_plane_first(axes, main, rest, x_ref, o_ref, s2, r2))
    return jobs


def scatter_scratch(axes, shape, dt):
    rows, cols = shape
    nz, ux, uy, uc = axes
    dma = pltpu.SemaphoreType.DMA
    out = []
    for second, n in enumerate(spans_of(axes, rows)):
        few = lambda use, k, r: pltpu.VMEM((k, r, cols) if use and n else (1, 16, cols), dt)
        lines = 1 if second else nz
        out += [
            few(True, nz * 4, n),
            few(uc, nz * 4, n),
            few(ux, lines, n),
            few(uy, lines, n),
            few(ux and uy, lines, n // 2),
            few(ux and uy, lines, n // 2),
            few(nz > 1, (nz + 1) * (4 if second else 1), n),
            dma((nz * (14 if second else 12),)),
            dma((nz * (18 if second else 12),)),
            dma((nz * 4,)),
        ]
    return out


def scatter_jobs(axes, p_ref, o_ref, *refs):
    rows = o_ref.shape[0]
    main, rest = spans_of(axes, rows)
    jobs = [scatter_line_last(axes, 0, main, p_ref, o_ref, *refs[:10])]
    if rest:
        jobs.append(scatter_line_first(axes, main, rest, p_ref, o_ref, *refs[10:]))
    return jobs


def transfer_kernel(kinds, axes_list, *refs):
    n = len(kinds)
    at = 2 * n
    jobs = []
    for i, (kind, axes) in enumerate(zip(kinds, axes_list)):
        many = GATHER_REFS if kind == "gather" else SCATTER_REFS
        make = gather_jobs if kind == "gather" else scatter_jobs
        jobs += make(axes, refs[i], refs[n + i], *refs[at : at + many])
        at += many
    run_jobs(axes_list, jobs)


def transfer(kinds, values, axes_list, collective_id):
    shapes, specs, scratch = [], [], []
    for kind, value, axes in zip(kinds, values, axes_list):
        if kind == "gather":
            shapes.append(jax.ShapeDtypeStruct((group_of(axes),) + value.shape, value.dtype))
            specs.append(pl.BlockSpec(memory_space=pl.ANY))
            scratch += gather_scratch(axes)
        else:
            shapes.append(jax.ShapeDtypeStruct(value.shape[1:], jnp.float32))
            specs.append(pl.BlockSpec(memory_space=pltpu.VMEM))
            scratch += scatter_scratch(axes, value.shape[1:], value.dtype)
    return pl.pallas_call(
        functools.partial(transfer_kernel, kinds, axes_list),
        out_shape=shapes,
        in_specs=[pl.BlockSpec(memory_space=pl.ANY)] * len(values),
        out_specs=specs,
        scratch_shapes=scratch,
        compiler_params=pltpu.CompilerParams(
            collective_id=collective_id, has_side_effects=True, vmem_limit_bytes=61 * 1024 * 1024
        ),
    )(*values)


def scatter_line_last(axes, lo, rows, p_ref, o_ref, acc, rc, rx, ry, ra, rb, rz, ssem, rsem, lsem):
    nz, ux, uy, uc = axes
    pc = Place(nz, ux, uy, uc)
    z, x, y, c = pc.z, pc.x, pc.y, pc.c
    half = rows // 2
    chunk = math.gcd(half, 32)
    f32 = jnp.float32
    to_x, to_y, to_c = pc.dev(z, 1 - x, y, c), pc.dev(z, x, 1 - y, c), pc.dev(z, x, y, 1 - c)
    rels = [(0, x, y)]
    if ux:
        rels.append((1, 1 - x, y))
    if uy:
        rels.append((2, x, 1 - y))
    if ux and uy:
        rels.append((3, 1 - x, 1 - y))
    KINDS = 12

    def slot(s):
        return s if nz > 1 else 0

    def sid(s, kind):
        return slot(s) * KINDS + kind

    def hf(ref, h):
        return ref.at[pl.ds(h * half, half)]

    def rcopy(src, dst, s, kind, device):
        return pltpu.make_async_remote_copy(
            src_ref=src,
            dst_ref=dst,
            send_sem=ssem.at[sid(s, kind)],
            recv_sem=rsem.at[sid(s, kind)],
            device_id=device,
            device_id_type=MESH_ID,
        )

    def load(s, rel, px, py):
        return pltpu.make_async_copy(
            p_ref.at[pc.blk(s, px, py, c), pl.ds(lo, rows)], acc.at[slot(s) * 4 + rel], lsem.at[slot(s) * 4 + rel]
        )

    def give(s, rel, px, py):
        return rcopy(
            p_ref.at[pc.blk(s, px, py, 1 - c), pl.ds(lo, rows)], rc.at[slot(s) * 4 + rel], s, rel, to_c
        )

    def fold(dst, lo, n, srcs):
        def body(i, _):
            r = pl.multiple_of(i * chunk, chunk)
            total = dst[pl.ds(lo + r, chunk), :].astype(f32)
            for ref, at in srcs:
                total = total + ref[pl.ds(at + r, chunk), :].astype(f32)
            dst[pl.ds(lo + r, chunk), :] = total.astype(dst.dtype)
            return 0

        lax.fori_loop(0, n // chunk, body, 0)

    def over_a(s):
        return rcopy(hf(acc.at[slot(s) * 4 + 3], 0), ra.at[slot(s)], s, 4, to_y)

    def over_b(s):
        return rcopy(hf(acc.at[slot(s) * 4 + 3], 1), rb.at[slot(s)], s, 5, to_x)

    def x_half(s, h):
        return rcopy(hf(acc.at[slot(s) * 4 + 1], h), hf(rx.at[slot(s)], h), s, 6 + h, to_x)

    def y_half(s, h):
        return rcopy(hf(acc.at[slot(s) * 4 + 2], h), hf(ry.at[slot(s)], h), s, 8 + h, to_y)

    def z_send(s, up):
        return rcopy(
            acc.at[slot(s) * 4],
            rz.at[slot(s)],
            s,
            10,
            pc.dev(z + (1 if up else -1), x, y, c),
        )

    def z_last(s, up):
        return pltpu.make_async_remote_copy(
            src_ref=acc.at[slot(s) * 4],
            dst_ref=rz.at[slot(s)] if up else rz.at[nz],
            send_sem=ssem.at[sid(s, 10)],
            recv_sem=rsem.at[sid(s, 10)] if up else rsem.at[sid(s, 11)],
            device_id=pc.dev(z + (1 if up else -1), x, y, c),
            device_id_type=MESH_ID,
        )

    steps = list(reversed(pc.line_steps()))

    def begin():
        for d, side, s, ok in steps:

            def fn():
                for rel, px, py in reversed(rels):
                    load(s, rel, px, py).start()
                    if uc:
                        give(s, rel, px, py).start()

            when(ok, fn)

    def first(step):
        _, _, s, ok = step

        def fn():
            for rel, px, py in reversed(rels):
                load(s, rel, px, py).wait()
                if uc:
                    give(s, rel, px, py).wait_recv()
                    fold(acc.at[slot(s) * 4 + rel], 0, rows, [(rc.at[slot(s) * 4 + rel], 0)])
                if rel == 3:
                    over_a(s).start()
                    over_b(s).start()
                if rel == 2:
                    y_half(s, 0).start()
                    if not ux:
                        y_half(s, 1).start()
                if rel == 1:
                    x_half(s, 1).start()
                    if not uy:
                        x_half(s, 0).start()

        when(ok, fn)

    def second(step):
        _, _, s, ok = step

        def fn():
            if ux and uy:
                over_a(s).wait_recv()
                fold(acc.at[slot(s) * 4 + 1], 0, half, [(ra.at[slot(s)], 0)])
                x_half(s, 0).start()
                over_b(s).wait_recv()
                fold(acc.at[slot(s) * 4 + 2], half, half, [(rb.at[slot(s)], 0)])
                y_half(s, 1).start()

        when(ok, fn)

    def third(step):
        d, side, s, ok = step

        def fn():
            srcs = []
            if ux:
                x_half(s, 0).wait_recv()
                x_half(s, 1).wait_recv()
                srcs.append((rx.at[slot(s)], 0))
            if uy:
                y_half(s, 0).wait_recv()
                y_half(s, 1).wait_recv()
                srcs.append((ry.at[slot(s)], 0))
            if d > 0:
                more = (z + 1 < nz) if side == 0 else (z >= 1)

                @pl.when(more)
                def _():
                    z_send(s, side == 1).wait_recv()
                    fold(acc.at[slot(s) * 4], 0, rows, srcs + [(rz.at[slot(s)], 0)])

                if srcs:

                    @pl.when(jnp.logical_not(more))
                    def _():
                        fold(acc.at[slot(s) * 4], 0, rows, srcs)

                if d == 1:
                    z_last(s, side == 1).start()
                else:
                    z_send(s, side == 1).start()
            else:

                def body(use_lo, use_hi):
                    terms = list(srcs)
                    if use_lo:
                        z_last(s, True).wait_recv()
                        terms.append((rz.at[slot(s)], 0))
                    if use_hi:
                        z_last(s, False).wait_recv()
                        terms.append((rz.at[nz], 0))

                    def step_(i, _):
                        r = pl.multiple_of(i * chunk, chunk)
                        total = acc[slot(s) * 4, pl.ds(r, chunk), :].astype(f32)
                        for ref, at in terms:
                            total = total + ref[pl.ds(at + r, chunk), :].astype(f32)
                        o_ref[pl.ds(pl.multiple_of(lo + i * chunk, chunk), chunk), :] = total.astype(
                            o_ref.dtype
                        )
                        return 0

                    lax.fori_loop(0, rows // chunk, step_, 0)

                if nz == 1:
                    body(False, False)
                else:
                    pl.when(jnp.logical_and(z >= 1, z + 1 < nz))(lambda: body(True, True))
                    pl.when(z == nz - 1)(lambda: body(True, False))
                    pl.when(z == 0)(lambda: body(False, True))

        when(ok, fn)

    groups = [[st for st in steps if st[0] == d] for d in reversed(range(nz))]

    def phase(t):
        if t < nz:
            for st in groups[t]:
                first(st)
        if 0 <= t - 1 < nz:
            for st in groups[t - 1]:
                second(st)
        if 0 <= t - 2 < nz:
            for st in groups[t - 2]:
                third(st)

    def last():
        for d, side, s, ok in steps:

            def fn():
                for rel, px, py in rels:
                    if uc:
                        give(s, rel, px, py).wait_send()
                if ux and uy:
                    over_a(s).wait_send()
                    over_b(s).wait_send()
                if ux:
                    x_half(s, 0).wait_send()
                    x_half(s, 1).wait_send()
                if uy:
                    y_half(s, 0).wait_send()
                    y_half(s, 1).wait_send()
                if d > 0:
                    z_send(s, side == 1).wait_send()

            when(ok, fn)

    return begin, [functools.partial(phase, t) for t in range(nz + 2)], last


def scatter_line_first(axes, lo, rows, p_ref, o_ref, acc, rc, rx, ry, ra, rb, rz, ssem, rsem, lsem):
    nz, ux, uy, uc = axes
    pc = Place(nz, ux, uy, uc)
    z, x, y, c = pc.z, pc.x, pc.y, pc.c
    half = rows // 2
    chunk = math.gcd(half, 32)
    f32 = jnp.float32
    to_x, to_y, to_c = pc.dev(z, 1 - x, y, c), pc.dev(z, x, 1 - y, c), pc.dev(z, x, y, 1 - c)
    rels = [(0, x, y)]
    if ux:
        rels.append((1, 1 - x, y))
    if uy:
        rels.append((2, x, 1 - y))
    if ux and uy:
        rels.append((3, 1 - x, 1 - y))
    plane = nz * 4 * 3

    def hf(ref, h):
        return ref.at[pl.ds(h * half, half)]

    def rcopy(src, dst, sidx, ridx, device):
        return pltpu.make_async_remote_copy(
            src_ref=src,
            dst_ref=dst,
            send_sem=ssem.at[sidx],
            recv_sem=rsem.at[ridx],
            device_id=device,
            device_id_type=MESH_ID,
        )

    def load(s, rel, px, py):
        return pltpu.make_async_copy(
            p_ref.at[pc.blk(s, px, py, c), pl.ds(lo, rows)], acc.at[s * 4 + rel], lsem.at[s * 4 + rel]
        )

    def give(s, rel, px, py):
        at = s * 4 + rel
        return rcopy(p_ref.at[pc.blk(s, px, py, 1 - c), pl.ds(lo, rows)], rc.at[at], at, at, to_c)

    def hop(s, rel, up, final):
        extra = final and not up
        return rcopy(
            acc.at[s * 4 + rel],
            rz.at[nz * 4 + rel] if extra else rz.at[s * 4 + rel],
            nz * 4 + s * 4 + rel,
            (nz * 8 + s * 4 + rel) if extra else (nz * 4 + s * 4 + rel),
            pc.dev(z + (1 if up else -1), x, y, c),
        )

    def fold(dst, at, n, srcs):
        def body(i, _):
            r = pl.multiple_of(i * chunk, chunk)
            total = dst[pl.ds(pl.multiple_of(at + r, chunk), chunk), :].astype(f32)
            for ref, first in srcs:
                total = total + ref[pl.ds(pl.multiple_of(first + r, chunk), chunk), :].astype(f32)
            dst[pl.ds(pl.multiple_of(at + r, chunk), chunk), :] = total.astype(dst.dtype)
            return 0

        lax.fori_loop(0, n // chunk, body, 0)

    def mine(rel):
        return acc.at[z * 4 + rel]

    def over_a():
        return rcopy(hf(mine(3), 0), ra.at[0], nz * 8, plane, to_y)

    def over_b():
        return rcopy(hf(mine(3), 1), rb.at[0], nz * 8 + 1, plane + 1, to_x)

    def x_half(h):
        return rcopy(hf(mine(1), h), hf(rx.at[0], h), nz * 8 + 2 + h, plane + 2 + h, to_x)

    def y_half(h):
        return rcopy(hf(mine(2), h), hf(ry.at[0], h), nz * 8 + 4 + h, plane + 4 + h, to_y)

    steps = list(reversed(pc.line_steps()))

    def begin():
        for d, side, s, ok in steps:

            def fn():
                for rel, px, py in reversed(rels):
                    load(s, rel, px, py).start()
                    if uc:
                        give(s, rel, px, py).start()

            when(ok, fn)

    def line(step):
        d, side, s, ok = step

        def fn():
            more = (z + 1 < nz) if side == 0 else (z >= 1)
            for rel, px, py in reversed(rels):
                load(s, rel, px, py).wait()
                srcs = []
                if uc:
                    give(s, rel, px, py).wait_recv()
                    srcs = [(rc.at[s * 4 + rel], 0)]
                target = acc.at[s * 4 + rel]
                if d > 0:

                    @pl.when(more)
                    def _():
                        hop(s, rel, side == 1, False).wait_recv()
                        fold(target, 0, rows, srcs + [(rz.at[s * 4 + rel], 0)])

                    if srcs:

                        @pl.when(jnp.logical_not(more))
                        def _():
                            fold(target, 0, rows, srcs)

                    hop(s, rel, side == 1, d == 1).start()
                else:
                    lower, upper = (rz.at[s * 4 + rel], 0), (rz.at[nz * 4 + rel], 0)

                    @pl.when(z >= 1)
                    def _():
                        hop(s, rel, True, True).wait_recv()

                    @pl.when(z + 1 < nz)
                    def _():
                        hop(s, rel, False, True).wait_recv()

                    both = jnp.logical_and(z >= 1, z + 1 < nz)
                    pl.when(both)(lambda: fold(target, 0, rows, srcs + [lower, upper]))
                    pl.when(z == 0)(lambda: fold(target, 0, rows, srcs + [upper]))
                    pl.when(z == nz - 1)(lambda: fold(target, 0, rows, srcs + [lower]))
                    if rel == 3:
                        over_a().start()
                        over_b().start()
                    if rel == 2:
                        y_half(0).start()
                        if not ux:
                            y_half(1).start()
                    if rel == 1:
                        x_half(1).start()
                        if not uy:
                            x_half(0).start()

        when(ok, fn)

    def cross():
        if ux and uy:
            over_a().wait_recv()
            fold(mine(1), 0, half, [(ra.at[0], 0)])
            x_half(0).start()
            over_b().wait_recv()
            fold(mine(2), half, half, [(rb.at[0], 0)])
            y_half(1).start()

    def total():
        srcs = []
        if ux:
            x_half(0).wait_recv()
            x_half(1).wait_recv()
            srcs.append(rx)
        if uy:
            y_half(0).wait_recv()
            y_half(1).wait_recv()
            srcs.append(ry)

        def body(i, _):
            r = pl.multiple_of(i * chunk, chunk)
            value = acc[z * 4, pl.ds(r, chunk), :].astype(f32)
            for ref in srcs:
                value = value + ref[0, pl.ds(r, chunk), :].astype(f32)
            o_ref[pl.ds(pl.multiple_of(lo + i * chunk, chunk), chunk), :] = value.astype(o_ref.dtype)
            return 0

        lax.fori_loop(0, rows // chunk, body, 0)

    groups = [[st for st in steps if st[0] == d] for d in reversed(range(nz))]

    def phase(t):
        if t < nz:
            for st in groups[t]:
                line(st)
        elif t == nz:
            cross()
        else:
            total()

    def last():
        for d, side, s, ok in steps:

            def fn():
                for rel, px, py in rels:
                    if uc:
                        give(s, rel, px, py).wait_send()
                    if d > 0:
                        hop(s, rel, side == 1, d == 1).wait_send()

            when(ok, fn)
        if ux and uy:
            over_a().wait_send()
            over_b().wait_send()
        if ux:
            x_half(0).wait_send()
            x_half(1).wait_send()
        if uy:
            y_half(0).wait_send()
            y_half(1).wait_send()

    return begin, [functools.partial(phase, t) for t in range(nz + 2)], last


LOG2E = 1.4426950408889634


def lane_swap(tensor):
    return pltpu.roll(tensor, tensor.shape[-1] // 2, tensor.ndim - 1)


def head_norm(tensor, gain, cos2, sin2):
    inverse = lax.rsqrt(jnp.mean(tensor * tensor, axis=-1, keepdims=True) + EPSILON)
    scaled = tensor * inverse * gain
    return scaled * cos2 + lane_swap(scaled) * sin2


def head_norm_back(tensor, gain, cos2, sin2, gradient):
    inverse = lax.rsqrt(jnp.mean(tensor * tensor, axis=-1, keepdims=True) + EPSILON)
    turned = gradient * cos2 - lane_swap(gradient) * sin2
    weighted = turned * gain
    inner = jnp.mean(weighted * tensor, axis=-1, keepdims=True)
    return (
        inverse * weighted - tensor * (inverse * inverse * inverse) * inner,
        turned * tensor * inverse,
    )


def token_rows(piece, seq, seq_count, rows_dev):
    return (piece * seq_count + seq) * rows_dev


def kv_prep_kernel(pieces, seqs, proj_ref, gain_ref, cos_ref, sin_ref, o_ref):
    hd = gain_ref.shape[-1]
    rows = proj_ref.shape[0] // (pieces * seqs)
    for piece in range(pieces):
        cos2 = cos_ref[piece * rows : (piece + 1) * rows, :]
        sin2 = sin_ref[piece * rows : (piece + 1) * rows, :]
        for seq in range(seqs):
            at = token_rows(piece, seq, seqs, rows)
            raw = proj_ref[at : at + rows, :hd]
            o_ref[at : at + rows, :hd] = head_norm(raw, gain_ref[...], cos2, sin2).astype(
                o_ref.dtype
            )
            o_ref[at : at + rows, hd:] = proj_ref[at : at + rows, hd:].astype(o_ref.dtype)


def kv_prep(projected, key_gain, cos2, sin2, heads, pieces, seqs):
    rows, _ = projected.shape
    hd = key_gain.shape[0]
    whole = lambda *shape: pl.BlockSpec(shape, lambda i: (0,) * len(shape))
    return pl.pallas_call(
        functools.partial(kv_prep_kernel, pieces, seqs),
        grid=(1,),
        out_shape=jax.ShapeDtypeStruct((rows, 2 * hd), jnp.bfloat16),
        in_specs=[
            pl.BlockSpec((rows, 2 * hd), lambda i: (0, heads // 2)),
            whole(1, hd),
            whole(*cos2.shape),
            whole(*sin2.shape),
        ],
        out_specs=whole(rows, 2 * hd),
        name="kv_prep",
    )(projected, key_gain.reshape(1, hd), cos2, sin2)


def kv_back_kernel(pieces, seqs, proj_ref, cot_ref, gain_ref, cos_ref, sin_ref, _, low_ref, gg_ref):
    hd = gain_ref.shape[-1]
    rows = proj_ref.shape[0] // (pieces * seqs)
    total = jnp.zeros((1, hd), jnp.float32)
    for piece in range(pieces):
        cos2 = cos_ref[piece * rows : (piece + 1) * rows, :]
        sin2 = sin_ref[piece * rows : (piece + 1) * rows, :]
        for seq in range(seqs):
            at = token_rows(piece, seq, seqs, rows)
            grad, terms = head_norm_back(
                proj_ref[at : at + rows, :hd],
                gain_ref[...],
                cos2,
                sin2,
                cot_ref[at : at + rows, :hd],
            )
            low_ref[at : at + rows, :hd] = grad.astype(low_ref.dtype)
            low_ref[at : at + rows, hd:] = cot_ref[at : at + rows, hd:].astype(low_ref.dtype)
            total = total + jnp.sum(terms, axis=0, keepdims=True)
    gg_ref[...] = total


def kv_back(projected, kv_cot, key_gain, cos2, sin2, low, heads, pieces, seqs):
    rows, _ = projected.shape
    hd = key_gain.shape[0]
    whole = lambda *shape: pl.BlockSpec(shape, lambda i: (0,) * len(shape))
    return pl.pallas_call(
        functools.partial(kv_back_kernel, pieces, seqs),
        grid=(1,),
        out_shape=(
            jax.ShapeDtypeStruct(low.shape, low.dtype),
            jax.ShapeDtypeStruct((1, hd), jnp.float32),
        ),
        in_specs=[
            pl.BlockSpec((rows, 2 * hd), lambda i: (0, heads // 2)),
            whole(rows, 2 * hd),
            whole(1, hd),
            whole(*cos2.shape),
            whole(*sin2.shape),
            pl.BlockSpec(memory_space=pl.ANY),
        ],
        out_specs=(pl.BlockSpec((rows, 2 * hd), lambda i: (0, heads // 2)), whole(1, hd)),
        input_output_aliases={5: 0},
        name="kv_back",
    )(projected, kv_cot, key_gain.reshape(1, hd), cos2, sin2, low)


def sort_blocks(loc_ref, kv_ref, dst, seqs, rows, pieces, hd, lo, blocks):
    per_half = pieces // 2

    def body(b, _):
        loc = loc_ref[b]
        chunk, half = loc // 2, loc % 2
        for seq in range(seqs):
            for i in range(per_half):
                at = ((half * per_half + i) * seqs + seq) * rows
                dst[seq, pl.ds(b * (per_half * rows) + i * rows, rows), :] = kv_ref[
                    chunk, pl.ds(at, rows), lo : lo + hd
                ]
        return 0

    lax.fori_loop(0, blocks, body, 0)


def attend_kernel(
    heads, pieces, seqs, scale, loc_ref, own_ref, proj_ref, kv_ref, gain_ref, cos_ref, sin_ref,
    attn_ref, lse_ref, qs_ref, ks, vs, acc, tot,
):
    f32, bf16 = jnp.float32, jnp.bfloat16
    hd = gain_ref.shape[-1]
    rows = proj_ref.shape[0] // (pieces * seqs)
    per_half = pieces // 2
    block = per_half * rows
    blocks = 2 * kv_ref.shape[0]
    pair = 2 * block
    tile = 2 * block
    sort_blocks(loc_ref, kv_ref, ks, seqs, rows, pieces, hd, 0, blocks)
    sort_blocks(loc_ref, kv_ref, vs, seqs, rows, pieces, hd, hd, blocks)
    for seq in range(seqs):
        for half in range(2):
            unit = seq * 2 + half
            for h in range(heads):
                for i in range(per_half):
                    piece = half * per_half + i
                    at = token_rows(piece, seq, seqs, rows)
                    turned = head_norm(
                        proj_ref[at : at + rows, h * hd : (h + 1) * hd],
                        gain_ref[...],
                        cos_ref[piece * rows : (piece + 1) * rows, :],
                        sin_ref[piece * rows : (piece + 1) * rows, :],
                    )
                    qs_ref[unit, h * block + i * rows : h * block + (i + 1) * rows, :] = (
                        turned.astype(bf16)
                    )
            acc[...] = jnp.zeros_like(acc)
            tot[...] = jnp.zeros_like(tot)
            mine = own_ref[half]

            def step(j, masked):
                keys = ks[seq, pl.ds(j * pair, pair), :]
                values = vs[seq, pl.ds(j * pair, pair), :]
                for t in range(heads * block // tile):
                    cols = slice(t * tile, (t + 1) * tile)
                    scores = lax.dot_general(
                        keys,
                        qs_ref[unit, cols, :],
                        (((1,), (1,)), ((), ())),
                        preferred_element_type=f32,
                    )
                    expo = jnp.exp2(scores * (scale * LOG2E))
                    if masked:
                        key_pos = j * pair + lax.broadcasted_iota(jnp.int32, expo.shape, 0)
                        query_pos = mine * block + (
                            lax.broadcasted_iota(jnp.int32, expo.shape, 1) % block
                        )
                        expo = jnp.where(key_pos <= query_pos, expo, 0.0)
                    tot[:, cols] += jnp.sum(expo.reshape(pair // 8, 8, tile), axis=0)
                    acc[:, cols] += lax.dot_general(
                        values,
                        expo.astype(bf16),
                        (((0,), (0,)), ((), ())),
                        preferred_element_type=f32,
                    )

            def body(j, _):
                step(j, False)
                return 0

            lax.fori_loop(0, mine // 2, body, 0)
            step(mine // 2, True)
            total = jnp.sum(tot[...], axis=0, keepdims=True)
            lse_ref[unit, :, :] = jnp.log(total)
            share = 1.0 / total
            for h in range(heads):
                cols = slice(h * block, (h + 1) * block)
                out = jnp.transpose(acc[:, cols] * share[:, cols]).astype(bf16)
                for i in range(per_half):
                    at = token_rows(half * per_half + i, seq, seqs, rows)
                    attn_ref[at : at + rows, h * hd : (h + 1) * hd] = out[
                        i * rows : (i + 1) * rows, :
                    ]


def attend(projected, kv_all, query_gain, cos2, sin2, loc, own, heads, pieces, seqs):
    rows = projected.shape[0]
    hd = query_gain.shape[0]
    units = 2 * seqs
    block = rows // units
    keys = kv_all.shape[0] * kv_all.shape[1] // seqs
    whole = lambda *shape: pl.BlockSpec(shape, lambda i, *_: (0,) * len(shape))
    f32, bf16 = jnp.float32, jnp.bfloat16
    return pl.pallas_call(
        functools.partial(attend_kernel, heads, pieces, seqs, hd**-0.5),
        grid_spec=pltpu.PrefetchScalarGridSpec(
            num_scalar_prefetch=2,
            grid=(1,),
            in_specs=[
                pl.BlockSpec((rows, heads * hd), lambda i, *_: (0, 0)),
                whole(*kv_all.shape),
                whole(1, hd),
                whole(*cos2.shape),
                whole(*sin2.shape),
            ],
            out_specs=[
                whole(rows, heads * hd),
                whole(units, 1, heads * block),
                whole(units, heads * block, hd),
            ],
            scratch_shapes=[
                pltpu.VMEM((seqs, keys, hd), bf16),
                pltpu.VMEM((seqs, keys, hd), bf16),
                pltpu.VMEM((hd, heads * block), f32),
                pltpu.VMEM((8, heads * block), f32),
            ],
        ),
        out_shape=(
            jax.ShapeDtypeStruct((rows, heads * hd), bf16),
            jax.ShapeDtypeStruct((units, 1, heads * block), f32),
            jax.ShapeDtypeStruct((units, heads * block, hd), bf16),
        ),
        compiler_params=pltpu.CompilerParams(vmem_limit_bytes=56 * 1024 * 1024),
        name="attend",
    )(loc, own, projected, kv_all, query_gain.reshape(1, hd), cos2, sin2)


def attend_back_kernel(
    heads, pieces, seqs, scale, loc_ref, own_ref, proj_ref, kv_ref, qs_ref, attn_ref, cot_ref,
    lse_ref, gain_ref, cos_ref, sin_ref, low_ref, dkv_ref, gg_ref, ks, vs, dk, dv, dq, cs, dl,
):
    f32, bf16 = jnp.float32, jnp.bfloat16
    hd = gain_ref.shape[-1]
    rows = proj_ref.shape[0] // (pieces * seqs)
    per_half = pieces // 2
    block = per_half * rows
    blocks = 2 * kv_ref.shape[0]
    pair = 2 * block
    tile = 2 * block
    sort_blocks(loc_ref, kv_ref, ks, seqs, rows, pieces, hd, 0, blocks)
    sort_blocks(loc_ref, kv_ref, vs, seqs, rows, pieces, hd, hd, blocks)
    dk[...] = jnp.zeros_like(dk)
    dv[...] = jnp.zeros_like(dv)
    gain_total = jnp.zeros((1, hd), f32)
    ones = jnp.ones((8, hd), bf16)
    nt = (((1,), (1,)), ((), ()))
    for seq in range(seqs):
        for half in range(2):
            unit = seq * 2 + half
            for h in range(heads):
                for i in range(per_half):
                    at = token_rows(half * per_half + i, seq, seqs, rows)
                    to = slice(h * block + i * rows, h * block + (i + 1) * rows)
                    part = cot_ref[at : at + rows, h * hd : (h + 1) * hd]
                    cs[to, :] = part
                    prod = part.astype(f32) * attn_ref[
                        at : at + rows, h * hd : (h + 1) * hd
                    ].astype(f32)
                    dq[to, :] = prod
            for t in range(heads * block // tile):
                cols = slice(t * tile, (t + 1) * tile)
                prod = dq[cols, :]
                high = prod.astype(bf16)
                rest = (prod - high.astype(f32)).astype(bf16)
                dl[:, cols] = lax.dot_general(
                    ones, high, nt, preferred_element_type=f32
                ) + lax.dot_general(ones, rest, nt, preferred_element_type=f32)
            dq[...] = jnp.zeros_like(dq)
            mine = own_ref[half]

            def step(j, masked):
                at = pl.ds(j * pair, pair)
                keys = ks[seq, at, :]
                values = vs[seq, at, :]
                key_sum = jnp.zeros((pair, hd), f32)
                value_sum = jnp.zeros((pair, hd), f32)
                for t in range(heads * block // tile):
                    cols = slice(t * tile, (t + 1) * tile)
                    query = qs_ref[unit, cols, :]
                    cot = cs[cols, :]
                    scores = lax.dot_general(keys, query, nt, preferred_element_type=f32)
                    weights = jnp.exp2(
                        scores * (scale * LOG2E) - lse_ref[unit, :, cols] * LOG2E
                    )
                    if masked:
                        key_pos = j * pair + lax.broadcasted_iota(jnp.int32, weights.shape, 0)
                        query_pos = mine * block + (
                            lax.broadcasted_iota(jnp.int32, weights.shape, 1) % block
                        )
                        weights = jnp.where(key_pos <= query_pos, weights, 0.0)
                    prob_cot = lax.dot_general(values, cot, nt, preferred_element_type=f32)
                    low = (weights * (prob_cot - dl[0:1, cols])).astype(bf16)
                    value_sum = value_sum + jnp.dot(
                        weights.astype(bf16), cot, preferred_element_type=f32
                    )
                    key_sum = key_sum + jnp.dot(low, query, preferred_element_type=f32)
                    dq[cols, :] += lax.dot_general(
                        low, keys, (((0,), (0,)), ((), ())), preferred_element_type=f32
                    )
                dk[seq, at, :] += key_sum
                dv[seq, at, :] += value_sum

            def body(j, _):
                step(j, False)
                return 0

            lax.fori_loop(0, mine // 2, body, 0)
            step(mine // 2, True)
            for h in range(heads):
                for i in range(per_half):
                    piece = half * per_half + i
                    at = token_rows(piece, seq, seqs, rows)
                    grad, terms = head_norm_back(
                        proj_ref[at : at + rows, h * hd : (h + 1) * hd],
                        gain_ref[...],
                        cos_ref[piece * rows : (piece + 1) * rows, :],
                        sin_ref[piece * rows : (piece + 1) * rows, :],
                        dq[h * block + i * rows : h * block + (i + 1) * rows, :] * scale,
                    )
                    low_ref[at : at + rows, h * hd : (h + 1) * hd] = grad.astype(bf16)
                    gain_total = gain_total + jnp.sum(terms, axis=0, keepdims=True)
    gg_ref[...] = gain_total

    def unsort(b, _):
        loc = loc_ref[b]
        chunk, half = loc // 2, loc % 2
        for seq in range(seqs):
            for i in range(per_half):
                at = pl.ds(((half * per_half + i) * seqs + seq) * rows, rows)
                here = pl.ds(b * block + i * rows, rows)
                dkv_ref[chunk, at, 0:hd] = (dk[seq, here, :] * scale).astype(bf16)
                dkv_ref[chunk, at, hd : 2 * hd] = dv[seq, here, :].astype(bf16)
        return 0

    lax.fori_loop(0, blocks, unsort, 0)


def attend_back(
    projected, kv_all, rotated, attention, attention_cot, log_total, query_gain, cos2, sin2, loc,
    own, heads, pieces, seqs,
):
    rows, all_cols = projected.shape
    hd = query_gain.shape[0]
    units = 2 * seqs
    block = rows // units
    keys = kv_all.shape[0] * kv_all.shape[1] // seqs
    whole = lambda *shape: pl.BlockSpec(shape, lambda i, *_: (0,) * len(shape))
    f32, bf16 = jnp.float32, jnp.bfloat16
    return pl.pallas_call(
        functools.partial(attend_back_kernel, heads, pieces, seqs, hd**-0.5),
        grid_spec=pltpu.PrefetchScalarGridSpec(
            num_scalar_prefetch=2,
            grid=(1,),
            in_specs=[
                pl.BlockSpec((rows, heads * hd), lambda i, *_: (0, 0)),
                whole(*kv_all.shape),
                whole(*rotated.shape),
                whole(rows, heads * hd),
                whole(rows, heads * hd),
                whole(*log_total.shape),
                whole(1, hd),
                whole(*cos2.shape),
                whole(*sin2.shape),
            ],
            out_specs=[
                pl.BlockSpec((rows, heads * hd), lambda i, *_: (0, 0)),
                whole(*kv_all.shape),
                whole(1, hd),
            ],
            scratch_shapes=[
                pltpu.VMEM((seqs, keys, hd), bf16),
                pltpu.VMEM((seqs, keys, hd), bf16),
                pltpu.VMEM((seqs, keys, hd), f32),
                pltpu.VMEM((seqs, keys, hd), f32),
                pltpu.VMEM((heads * block, hd), f32),
                pltpu.VMEM((heads * block, hd), bf16),
                pltpu.VMEM((8, heads * block), f32),
            ],
        ),
        out_shape=(
            jax.ShapeDtypeStruct((rows, all_cols), bf16),
            jax.ShapeDtypeStruct(kv_all.shape, bf16),
            jax.ShapeDtypeStruct((1, hd), f32),
        ),
        compiler_params=pltpu.CompilerParams(vmem_limit_bytes=60 * 1024 * 1024),
        name="attend_back",
    )(
        loc, own, projected, kv_all, rotated, attention, attention_cot, log_total,
        query_gain.reshape(1, hd), cos2, sin2,
    )


def picks_of(slots, capacity):
    return lax.broadcasted_iota(jnp.int32, (capacity, slots.shape[1]), 0) == slots


def expert_forward_kernel(
    capacity, slot_ref, weight_ref, x_ref, c_ref, gate_ref, up_ref, down_ref,
    rows_ref, cot_ref, gate_out, up_out, parts_ref, wc_ref, w_sc, cot_sc,
):
    f32, bf16 = jnp.float32, jnp.bfloat16
    devices = x_ref.shape[0]
    for d in range(devices):
        pick = picks_of(slot_ref[d : d + 1, :], capacity)
        low = pick.astype(bf16)
        at = slice(d * capacity, (d + 1) * capacity)
        rows_ref[at, :] = jnp.dot(low, x_ref[d], preferred_element_type=f32).astype(bf16)
        cot_sc[at, :] = jnp.dot(low, c_ref[d], preferred_element_type=f32).astype(bf16)
        w_sc[at, :] = jnp.sum(
            jnp.where(pick, weight_ref[d : d + 1, :], 0.0), axis=1, keepdims=True
        )
    rows = rows_ref[...]
    gate = jnp.dot(rows, gate_ref[...], preferred_element_type=f32)
    gate_out[...] = gate
    up = jnp.dot(rows, up_ref[...], preferred_element_type=f32)
    up_out[...] = up
    activation = (gate * jax.nn.sigmoid(gate) * up).astype(bf16)
    produced = jnp.dot(activation, down_ref[...], preferred_element_type=f32).astype(bf16)
    for d in range(devices):
        pick = picks_of(slot_ref[d : d + 1, :], capacity)
        at = slice(d * capacity, (d + 1) * capacity)
        cot = cot_sc[at, :].astype(f32)
        made = produced[at, :].astype(f32)
        weight = w_sc[at, :]
        share = jnp.sum(cot * made, axis=1, keepdims=True)
        wc_ref[d : d + 1, :] = jnp.sum(jnp.where(pick, share, 0.0), axis=0, keepdims=True)
        cot_ref[at, :] = (weight * cot).astype(bf16)
        parts_ref[d] = lax.dot_general(
            pick.astype(bf16),
            (weight * made).astype(bf16),
            (((0,), (0,)), ((), ())),
            preferred_element_type=f32,
        ).astype(bf16)


def expert_forward(slots, weights, tokens_all, cot_all, gate_w, up_w, down_w, capacity, per_step):
    f32, bf16 = jnp.float32, jnp.bfloat16
    devices, tokens, width = tokens_all.shape
    hidden = gate_w.shape[1]
    rows = per_step * capacity
    lead = lambda *shape: pl.BlockSpec(shape, lambda i: (i,) + (0,) * (len(shape) - 1))
    fixed = lambda a: pl.BlockSpec(a.shape, lambda i: (0, 0), pipeline_mode=pl.Buffered(1))
    total = devices * capacity
    return pl.pallas_call(
        functools.partial(expert_forward_kernel, capacity),
        grid=(devices // per_step,),
        in_specs=[
            lead(per_step, tokens),
            lead(per_step, tokens),
            lead(per_step, tokens, width),
            lead(per_step, tokens, width),
            fixed(gate_w),
            fixed(up_w),
            fixed(down_w),
        ],
        out_specs=[
            lead(rows, width),
            lead(rows, width),
            lead(rows, hidden),
            lead(rows, hidden),
            lead(per_step, tokens, width),
            lead(per_step, tokens),
        ],
        out_shape=[
            jax.ShapeDtypeStruct((total, width), bf16),
            jax.ShapeDtypeStruct((total, width), bf16),
            jax.ShapeDtypeStruct((total, hidden), f32),
            jax.ShapeDtypeStruct((total, hidden), f32),
            jax.ShapeDtypeStruct((devices, tokens, width), bf16),
            jax.ShapeDtypeStruct((devices, tokens), f32),
        ],
        scratch_shapes=[pltpu.VMEM((rows, 1), f32), pltpu.VMEM((rows, width), bf16)],
        compiler_params=pltpu.CompilerParams(vmem_limit_bytes=62 * 1024 * 1024),
        name="expert_forward",
    )(slots, weights, tokens_all, cot_all, gate_w, up_w, down_w)


def expert_back_kernel(
    capacity, slot_ref, cot_ref, gate_pre, up_pre, gate_ref, up_ref, down_ref,
    act_ref, gate_cot, up_cot, parts_ref,
):
    f32, bf16 = jnp.float32, jnp.bfloat16
    devices = parts_ref.shape[0]
    nt = (((1,), (1,)), ((), ()))
    act_cot = lax.dot_general(cot_ref[...], down_ref[...], nt, preferred_element_type=f32)
    gate, up = gate_pre[...], up_pre[...]
    sigmoid = jax.nn.sigmoid(gate)
    swish = gate * sigmoid
    act_ref[...] = (swish * up).astype(bf16)
    low_gate = (act_cot * up * sigmoid * (1.0 + gate * (1.0 - sigmoid))).astype(bf16)
    low_up = (act_cot * swish).astype(bf16)
    gate_cot[...] = low_gate
    up_cot[...] = low_up
    row_cot = lax.dot_general(low_gate, gate_ref[...], nt, preferred_element_type=f32)
    row_cot = row_cot + lax.dot_general(low_up, up_ref[...], nt, preferred_element_type=f32)
    row_cot = row_cot.astype(bf16)
    for d in range(devices):
        pick = picks_of(slot_ref[d : d + 1, :], capacity)
        parts_ref[d] = lax.dot_general(
            pick.astype(bf16),
            row_cot[d * capacity : (d + 1) * capacity, :],
            (((0,), (0,)), ((), ())),
            preferred_element_type=f32,
        ).astype(bf16)


def expert_back(slots, route_cot, gate_pre, up_pre, gate_w, up_w, down_w, capacity, per_step):
    bf16 = jnp.bfloat16
    devices, tokens = slots.shape
    width, hidden = gate_w.shape
    rows = per_step * capacity
    lead = lambda *shape: pl.BlockSpec(shape, lambda i: (i,) + (0,) * (len(shape) - 1))
    fixed = lambda a: pl.BlockSpec(a.shape, lambda i: (0, 0), pipeline_mode=pl.Buffered(1))
    total = devices * capacity
    return pl.pallas_call(
        functools.partial(expert_back_kernel, capacity),
        grid=(devices // per_step,),
        in_specs=[
            lead(per_step, tokens),
            lead(rows, width),
            lead(rows, hidden),
            lead(rows, hidden),
            fixed(gate_w),
            fixed(up_w),
            fixed(down_w),
        ],
        out_specs=[
            lead(rows, hidden),
            lead(rows, hidden),
            lead(rows, hidden),
            lead(per_step, tokens, width),
        ],
        out_shape=[
            jax.ShapeDtypeStruct((total, hidden), bf16),
            jax.ShapeDtypeStruct((total, hidden), bf16),
            jax.ShapeDtypeStruct((total, hidden), bf16),
            jax.ShapeDtypeStruct((devices, tokens, width), bf16),
        ],
        compiler_params=pltpu.CompilerParams(vmem_limit_bytes=60 * 1024 * 1024),
        name="expert_back",
    )(slots, route_cot, gate_pre, up_pre, gate_w, up_w, down_w)


def product_kernel(a_ref, *refs):
    n = len(refs) // 2
    for b_ref, o_ref in zip(refs[:n], refs[n:]):
        o_ref[0] = lax.dot_general(
            a_ref[...], b_ref[...], (((0,), (0,)), ((), ())), preferred_element_type=jnp.float32
        )


def column_products(a, others, block):
    rows, k = a.shape
    return pl.pallas_call(
        product_kernel,
        grid=(k // block,),
        in_specs=[pl.BlockSpec((rows, block), lambda i: (0, i))]
        + [
            pl.BlockSpec(b.shape, lambda i: (0, 0), pipeline_mode=pl.Buffered(1)) for b in others
        ],
        out_specs=[pl.BlockSpec((1, block, b.shape[1]), lambda i: (0, i, 0)) for b in others],
        out_shape=[jax.ShapeDtypeStruct((1, k, b.shape[1]), jnp.float32) for b in others],
        compiler_params=pltpu.CompilerParams(vmem_limit_bytes=60 * 1024 * 1024),
    )(a, *others)


def own_kernels():
    return lax.axis_size("ctx") == 8 and lax.axis_size("wsh") == 4


AXIS_NAMES = {WSH_AXES: "wsh", CTX_AXES: "ctx", ALL_AXES: ("ctx", "wsh")}


def gather(shards, axes_list, ident):
    if own_kernels():
        return transfer(["gather"] * len(shards), shards, axes_list, ident)
    return [lax.all_gather(x, AXIS_NAMES[axes], axis=0) for x, axes in zip(shards, axes_list)]


def scatter(parts, axes_list, ident):
    if own_kernels():
        return transfer(["scatter"] * len(parts), parts, axes_list, ident)
    return [
        lax.psum_scatter(x, AXIS_NAMES[axes], scatter_dimension=0, tiled=False).astype(jnp.float32)
        for x, axes in zip(parts, axes_list)
    ]


def exchange(pieces):
    return lax.all_to_all(pieces, ("ctx", "wsh"), split_axis=0, concat_axis=0, tiled=True)


def to_everyone(value, device_count):
    return exchange(jnp.broadcast_to(value[None], (device_count,) + value.shape))


def experts_plain(
    slot_mine, weight_mine, moe_all, cot_all, gate_w, up_w, down_w, capacity
):
    f32, bf16 = jnp.float32, jnp.bfloat16
    device_count, _, width = moe_all.shape
    picks = slot_mine[:, None, :] == jnp.arange(capacity, dtype=jnp.int32)[None, :, None]
    picks_low = picks.astype(bf16)
    slot_weight = jnp.sum(jnp.where(picks, weight_mine[:, None, :], 0.0), axis=-1)

    def take(everyone):
        return (
            jnp.einsum("dct,dtw->dcw", picks_low, everyone, preferred_element_type=f32)
            .astype(bf16)
            .reshape(device_count * capacity, width)
        )

    def put(rows):
        return jnp.einsum(
            "dct,dcw->dtw",
            picks_low,
            rows.reshape(device_count, capacity, width),
            preferred_element_type=f32,
        ).astype(bf16)

    rows_in = take(moe_all)
    cot_rows = take(cot_all).astype(f32)
    weight_rows = slot_weight.reshape(device_count * capacity, 1)
    route_cot = (weight_rows * cot_rows).astype(bf16)
    gate_pre = jnp.dot(rows_in, gate_w, preferred_element_type=f32)
    up_pre = jnp.dot(rows_in, up_w, preferred_element_type=f32)
    sigmoid = jax.nn.sigmoid(gate_pre)
    swish = gate_pre * sigmoid
    activation = (swish * up_pre).astype(bf16)
    produced = jnp.dot(activation, down_w, preferred_element_type=f32).astype(bf16).astype(f32)
    out_parts = put((weight_rows * produced).astype(bf16))
    slot_cot = jnp.sum(cot_rows * produced, axis=-1).reshape(device_count, capacity)
    cot_mine = jnp.sum(jnp.where(picks, slot_cot[:, :, None], 0.0), axis=1)
    down_grad = jnp.einsum("rf,rd->fd", activation, route_cot, preferred_element_type=f32)
    act_cot = jnp.einsum("rd,fd->rf", route_cot, down_w, preferred_element_type=f32)
    gate_cot = (act_cot * up_pre * sigmoid * (1.0 + gate_pre * (1.0 - sigmoid))).astype(bf16)
    up_cot = (act_cot * swish).astype(bf16)
    gate_grad = jnp.einsum("rd,rf->df", rows_in, gate_cot, preferred_element_type=f32)
    up_grad = jnp.einsum("rd,rf->df", rows_in, up_cot, preferred_element_type=f32)
    row_cot = jnp.einsum("rf,df->rd", gate_cot, gate_w, preferred_element_type=f32)
    row_cot = row_cot + jnp.einsum("rf,df->rd", up_cot, up_w, preferred_element_type=f32)
    return (
        out_parts,
        cot_mine,
        put(row_cot.astype(bf16)),
        gate_grad[None],
        up_grad[None],
        down_grad[None],
    )


def local(
    inputs,
    pair_map,
    norm_gain,
    query_weight,
    key_weight,
    value_weight,
    query_gain,
    key_gain,
    out_weight,
    moe_gain,
    router,
    expert_gate,
    expert_up,
    expert_down,
    expert_ids,
    dispatch_slot,
    cotangent,
):
    f32, bf16 = jnp.float32, jnp.bfloat16
    rows_dev, seq_count, width = inputs.shape
    ctx_count = lax.axis_size("ctx")
    wsh_count = lax.axis_size("wsh")
    device_count = ctx_count * wsh_count
    head_dim = query_gain.shape[0]
    group_rows = rows_dev * wsh_count
    block_len = group_rows // 2
    seq_len = group_rows * ctx_count
    tokens = rows_dev * seq_count
    group_tokens = tokens * wsh_count
    top_count = expert_ids.shape[-1]
    expert_count = router.shape[1]
    capacity = max(2, 3 * top_count * block_len // (2 * device_count))
    positions = positions_of(pair_map, seq_len, block_len, pair_map.shape[0])
    me_ctx = lax.axis_index("ctx")
    query_pos = lax.dynamic_slice_in_dim(positions, me_ctx * group_rows, group_rows, 0)
    cosine, sine_table = rope_tables(query_pos, head_dim)
    cos2 = jnp.concatenate([cosine, cosine], axis=1)
    sin2 = jnp.concatenate([-sine_table, sine_table], axis=1)
    block_ids = jnp.arange(2 * ctx_count, dtype=jnp.int32)
    blocks_by_loc = jnp.stack([pair_map, 2 * ctx_count - 1 - pair_map], axis=1).reshape(-1)
    loc = jnp.sum(
        jnp.where(blocks_by_loc[None, :] == block_ids[:, None], block_ids[None, :], 0), axis=1
    ).astype(jnp.int32)
    own_blocks = lax.dynamic_slice_in_dim(blocks_by_loc, 2 * me_ctx, 2, 0)

    inputs_f = inputs.transpose(1, 0, 2).reshape(tokens, width).astype(f32)
    cot_flat = cotangent.transpose(1, 0, 2).reshape(tokens, width)
    normed_f, inverse_one = rms_forward(inputs_f, norm_gain)
    q_cols, kv_cols = query_weight.shape[1], key_weight.shape[1]
    heads_loc = q_cols // head_dim
    qkv_shard = jnp.concatenate([query_weight, key_weight, value_weight], axis=1)
    normed_flat, qkv_full = gather([normed_f.astype(bf16), qkv_shard], [WSH_AXES, CTX_AXES], 1)
    normed_flat = normed_flat.reshape(group_tokens, width)
    qkv_full = qkv_full.reshape(width, q_cols + 2 * kv_cols)
    out_shard, qkv_full = lax.optimization_barrier((out_weight.T, qkv_full))
    out_full = lax.all_gather(out_shard, "ctx", axis=0, tiled=True)
    projected = jnp.dot(normed_flat, qkv_full, preferred_element_type=f32)
    kv_own = kv_prep(projected, key_gain, cos2, sin2, heads_loc, wsh_count, seq_count)
    (kv_all,) = gather([kv_own], [CTX_AXES], 3)
    cot_low, kv_all = lax.optimization_barrier((cot_flat.astype(bf16), kv_all))
    cot_all = lax.all_gather(cot_low, ("ctx", "wsh"), axis=0)

    attention, log_total, rotated = attend(
        projected, kv_all, query_gain, cos2, sin2, loc, own_blocks, heads_loc, wsh_count, seq_count
    )
    mixed = jnp.einsum("tc,dc->td", attention, out_full, preferred_element_type=f32)
    (mixed,) = scatter([mixed.astype(bf16).reshape(wsh_count, tokens, width)], [WSH_AXES], 4)
    residual = inputs_f + mixed

    def rows_first(value):
        return value.reshape(seq_count, rows_dev, width).transpose(1, 0, 2)

    moe_normed_f, inverse_two = rms_forward(residual, moe_gain)
    moe_flat = moe_normed_f.astype(bf16)
    (moe_all,) = gather([moe_flat], [ALL_AXES], 5)
    logits = jnp.dot(moe_flat, router, preferred_element_type=f32)
    route_ids = expert_ids.transpose(1, 0, 2).reshape(tokens, top_count)
    slots = dispatch_slot.transpose(1, 0, 2).reshape(tokens, top_count)
    expert_onehot = (
        route_ids[:, :, None] == jnp.arange(expert_count, dtype=jnp.int32)[None, None, :]
    )
    named = jnp.any(expert_onehot, axis=1)
    slot_dense = jnp.sum(jnp.where(expert_onehot, slots[:, :, None] + 1, 0), axis=1) - 1
    chosen_top = jnp.max(jnp.where(named, logits, MASKED), axis=-1, keepdims=True)
    chosen_exp = jnp.where(named, jnp.exp(jnp.where(named, logits - chosen_top, 0.0)), 0.0)
    weight_dense = chosen_exp / jnp.sum(chosen_exp, axis=-1, keepdims=True)
    routing = exchange(jnp.stack([slot_dense.astype(f32).T, weight_dense.T], axis=1))
    slot_mine = routing[:, 0, :].astype(jnp.int32)
    weight_mine = routing[:, 1, :]
    gate_w, up_w, down_w = (expert_gate[0], expert_up[0], expert_down[0])
    if capacity % 16 == 0:
        per_step = 8
        rows_in, route_cot, gate_pre, up_pre, out_parts, cot_mine = expert_forward(
            slot_mine, weight_mine, moe_all, cot_all, gate_w, up_w, down_w, capacity, per_step
        )
        activation, gate_cot, up_cot, row_parts = expert_back(
            slot_mine, route_cot, gate_pre, up_pre, gate_w, up_w, down_w, capacity, per_step
        )
        gate_grad, up_grad = column_products(rows_in, [gate_cot, up_cot], 256)
        (down_grad,) = column_products(activation, [route_cot], 256)
    else:
        out_parts, cot_mine, row_parts, gate_grad, up_grad, down_grad = experts_plain(
            slot_mine, weight_mine, moe_all, cot_all, gate_w, up_w, down_w, capacity
        )
    weight_cot = exchange(cot_mine).T

    chosen_cot = weight_dense * (
        weight_cot - jnp.sum(weight_dense * weight_cot, axis=-1, keepdims=True)
    )
    logit_cot = chosen_cot.astype(bf16)
    router_part = jnp.einsum("te,td->ed", logit_cot, moe_flat, preferred_element_type=f32)
    if own_kernels():
        row_sum, moe_sum, router_sum = scatter(
            [row_parts, out_parts, router_part.reshape(device_count, -1, 128)],
            [ALL_AXES, ALL_AXES, ALL_AXES],
            6,
        )
    else:
        row_sum, moe_sum = scatter([row_parts, out_parts], [ALL_AXES, ALL_AXES], 6)
        router_grad = lax.psum(router_part, ("ctx", "wsh")).T
    outputs = rows_first((residual + moe_sum).astype(bf16))
    normed_two_cot = (
        jnp.einsum("te,de->td", logit_cot, router, preferred_element_type=f32) + row_sum
    )
    residual_norm_cot, moe_gain_grad = rms_backward(
        residual, inverse_two, moe_gain, normed_two_cot
    )
    residual_cot = cot_flat + residual_norm_cot
    residual_low = residual_cot.astype(bf16)
    (residual_flat,) = gather([residual_low], [WSH_AXES], 8)
    residual_flat = residual_flat.reshape(group_tokens, width)

    out_grad = jnp.einsum("td,tc->dc", residual_flat, attention, preferred_element_type=f32).astype(
        bf16
    )
    out_weight_grad = lax.psum_scatter(out_grad, "ctx", scatter_dimension=0, tiled=True)
    out_weight_grad = out_weight_grad.astype(f32).T
    residual_flat, _ = lax.optimization_barrier((residual_flat, out_grad))
    attention_cot = jnp.einsum(
        "td,dc->tc", residual_flat, out_full, preferred_element_type=f32
    ).astype(bf16)
    low, kv_sums, query_gain_grad = attend_back(
        projected,
        kv_all,
        rotated,
        attention,
        attention_cot,
        log_total,
        query_gain,
        cos2,
        sin2,
        loc,
        own_blocks,
        heads_loc,
        wsh_count,
        seq_count,
    )
    kv_sums, gate_grad, up_grad, down_grad = lax.optimization_barrier(
        (kv_sums, gate_grad, up_grad, down_grad)
    )
    (kv_cot,) = scatter([kv_sums], [CTX_AXES], 9)
    low, key_gain_grad = kv_back(
        projected, kv_cot, key_gain, cos2, sin2, low, heads_loc, wsh_count, seq_count
    )
    summed = jnp.einsum("tq,cq->tc", low, qkv_full, preferred_element_type=f32)
    qkv_grad = jnp.einsum("tc,tq->cq", normed_flat, low, preferred_element_type=f32).astype(bf16)
    last_parts = [
        summed.astype(bf16).reshape(wsh_count, tokens, width),
        qkv_grad.reshape(ctx_count, width // ctx_count, q_cols + 2 * kv_cols),
    ]
    if own_kernels():
        normed_cot, qkv_grad, router_all = transfer(
            ["scatter", "scatter", "gather"],
            last_parts + [router_sum],
            [WSH_AXES, CTX_AXES, ALL_AXES],
            10,
        )
        router_grad = router_all.reshape(expert_count, width).T
    else:
        normed_cot, qkv_grad = scatter(last_parts, [WSH_AXES, CTX_AXES], 10)
    input_norm_cot, norm_gain_grad = rms_backward(inputs_f, inverse_one, norm_gain, normed_cot)
    input_grad = rows_first(residual_cot + input_norm_cot)
    query_gain_grad = query_gain_grad.reshape(head_dim)
    key_gain_grad = key_gain_grad.reshape(head_dim)
    gains = jnp.concatenate([norm_gain_grad, moe_gain_grad, query_gain_grad, key_gain_grad])
    gains = jnp.sum(to_everyone(gains, device_count), axis=0)
    return (
        outputs,
        input_grad,
        gains[:width],
        qkv_grad[:, :q_cols],
        qkv_grad[:, q_cols : q_cols + kv_cols],
        qkv_grad[:, q_cols + kv_cols :],
        gains[2 * width : 2 * width + head_dim],
        gains[2 * width + head_dim :],
        out_weight_grad,
        gains[width : 2 * width],
        router_grad,
        gate_grad,
        up_grad,
        down_grad,
    )


def solution(mesh):
    return jax.shard_map(
        local,
        mesh=mesh,
        in_specs=(
            P(("ctx", "wsh"), None, None),
            P(),
            P(),
            P("ctx", "wsh"),
            P("ctx", "wsh"),
            P("ctx", "wsh"),
            P(),
            P(),
            P("wsh", "ctx"),
            P(),
            P(),
            P(("ctx", "wsh"), None, None),
            P(("ctx", "wsh"), None, None),
            P(("ctx", "wsh"), None, None),
            P(("ctx", "wsh"), None, None),
            P(("ctx", "wsh"), None, None),
            P(("ctx", "wsh"), None, None),
        ),
        out_specs=(
            P(("ctx", "wsh"), None, None),
            P(("ctx", "wsh"), None, None),
            P(),
            P("ctx", "wsh"),
            P("ctx", "wsh"),
            P("ctx", "wsh"),
            P(),
            P(),
            P("wsh", "ctx"),
            P(),
            P(),
            P(("ctx", "wsh"), None, None),
            P(("ctx", "wsh"), None, None),
            P(("ctx", "wsh"), None, None),
        ),
        check_vma=False,
    )
```

```python
import functools
import math

import jax
import jax.numpy as jnp
from jax import lax
from jax.experimental import pallas as pl
from jax.experimental.pallas import tpu as pltpu
from jax.sharding import PartitionSpec as P


EPSILON = 1e-06
ROPE_BASE = 1000000.0
MASKED = -1e30


def positions_of(pair_map, seq_len, block_len, group_count):
    row_index = jnp.arange(seq_len, dtype=jnp.int32)
    owner_group = row_index // (2 * block_len)
    inner_row = row_index % (2 * block_len)
    group_table = jnp.arange(group_count, dtype=jnp.int32)
    pair_index = jnp.sum(
        jnp.where(owner_group[:, None] == group_table[None, :], pair_map[None, :], 0), axis=1
    )
    block_index = jnp.where(inner_row < block_len, pair_index, 2 * group_count - 1 - pair_index)
    return block_index * block_len + inner_row % block_len


def rope_tables(positions, head_dim):
    half_dim = head_dim // 2
    frequency = ROPE_BASE ** (-(jnp.arange(half_dim, dtype=jnp.float32) * 2.0) / head_dim)
    angles = positions.astype(jnp.float32)[:, None] * frequency[None, :]
    return (jnp.cos(angles), jnp.sin(angles))


def rms_forward(tensor, gain_vector):
    inverse = lax.rsqrt(jnp.mean(tensor * tensor, axis=-1, keepdims=True) + EPSILON)
    return (tensor * inverse * gain_vector, inverse)


def rms_backward(tensor, inverse, gain_vector, gradient):
    weighted = gradient * gain_vector
    inner_mean = jnp.mean(weighted * tensor, axis=-1, keepdims=True)
    tensor_grad = inverse * weighted - tensor * inverse**3 * inner_mean
    gain_grad = jnp.sum((gradient * tensor * inverse).reshape(-1, tensor.shape[-1]), axis=0)
    return (tensor_grad, gain_grad)


MESH_ID = pl.DeviceIdType.MESH


class Place:
    def __init__(self, nz, ux, uy, uc):
        ci, wi = lax.axis_index("ctx"), lax.axis_index("wsh")
        self.nz, self.ux, self.uy, self.uc = nz, ux, uy, uc
        self.z, self.x, self.y, self.c = ci // 2, ci % 2, wi // 2, wi % 2

    def dev(self, z, x, y, c):
        return (z * 2 + x, y * 2 + c)

    def blk(self, z, x, y, c):
        if self.ux and self.uc:
            return (z * 2 + x) * 4 + y * 2 + c
        if self.ux:
            return z * 2 + x
        return y * 2 + c

    def greet(self):
        z, x, y, c, nz = self.z, self.x, self.y, self.c, self.nz
        barrier = pltpu.get_barrier_semaphore()
        count = 0
        if nz > 1:
            for step in (-1, 1):
                ok = jnp.logical_and(z + step >= 0, z + step < nz)

                @pl.when(ok)
                def _():
                    pl.semaphore_signal(
                        barrier, inc=1, device_id=self.dev(z + step, x, y, c), device_id_type=MESH_ID
                    )

                count = count + ok.astype(jnp.int32)
        for use, place in (
            (self.ux, (z, 1 - x, y, c)),
            (self.uy, (z, x, 1 - y, c)),
            (self.uc, (z, x, y, 1 - c)),
        ):
            if use:
                pl.semaphore_signal(
                    barrier, inc=1, device_id=self.dev(*place), device_id_type=MESH_ID
                )
                count = count + 1
        pl.semaphore_wait(barrier, count)

    def line_steps(self):
        steps = [(0, 0, self.z, None)]
        for d in range(1, self.nz):
            steps.append((d, 0, self.z - d, self.z - d >= 0))
            steps.append((d, 1, self.z + d, self.z + d < self.nz))
        return steps


def both(a, b):
    if a is None or b is None:
        return a if b is None else b
    return a.astype(jnp.int32) * b.astype(jnp.int32) > 0


def when(cond, fn):
    if cond is None:
        fn()
    else:
        pl.when(cond)(fn)


def gather_line_first(axes, lo, rows, x_ref, o_ref, ssem, rsem):
    nz, ux, uy, uc = axes
    pc = Place(nz, ux, uy, uc)
    z, x, y, c = pc.z, pc.x, pc.y, pc.c
    half = rows // 2
    x_ref = x_ref.at[pl.ds(lo, rows)]
    to_x, to_y, to_c = pc.dev(z, 1 - x, y, c), pc.dev(z, x, 1 - y, c), pc.dev(z, x, y, 1 - c)

    def part(b, p):
        if p == 0:
            return o_ref.at[b, pl.ds(lo, rows)]
        return o_ref.at[b, pl.ds(lo + (p - 1) * half, half)]

    def sid(d, side, kind):
        return (d * 2 + side) * 10 + kind

    def copy(b, p, sidx, ridx, device, src=None):
        return pltpu.make_async_remote_copy(
            src_ref=part(b, p) if src is None else src,
            dst_ref=part(b, p),
            send_sem=ssem.at[sidx],
            recv_sem=rsem.at[ridx],
            device_id=device,
            device_id_type=MESH_ID,
        )

    def hops(d, side, s):
        out = []
        if nz > 1:
            b = pc.blk(s, x, y, c)
            src = x_ref if d == 0 else None
            if d == 0 or side == 0:
                if d + 1 < nz:
                    out.append(
                        (z + 1 < nz, copy(b, 0, sid(d, 0, 0), sid(d + 1, 0, 0), pc.dev(z + 1, x, y, c), src))
                    )
            if d == 0 or side == 1:
                if d + 1 < nz:
                    out.append(
                        (z >= 1, copy(b, 0, sid(d, 1, 0), sid(d + 1, 1, 0), pc.dev(z - 1, x, y, c), src))
                    )
        return out

    def spread(d, side, s):
        b = pc.blk(s, x, y, c)
        src = x_ref if d == 0 else None
        out = []
        if ux:
            out.append(copy(b, 0, sid(d, side, 1), sid(d, side, 1), to_x, src))
        if uy:
            out.append(copy(b, 0, sid(d, side, 2), sid(d, side, 2), to_y, src))
        if uc:
            out.append(copy(b, 0, sid(d, side, 5), sid(d, side, 5), to_c, src))
        return out

    def passed(d, side, s):
        out = []
        if ux:
            b = pc.blk(s, 1 - x, y, c)
            arrive = copy(b, 0, sid(d, side, 1), sid(d, side, 1), to_x)
            go = []
            if uy:
                go.append(copy(b, 1, sid(d, side, 3), sid(d, side, 3), to_y))
            if uc:
                go.append(copy(b, 0, sid(d, side, 6), sid(d, side, 6), to_c))
            out.append((arrive, go))
        if uy:
            b = pc.blk(s, x, 1 - y, c)
            arrive = copy(b, 0, sid(d, side, 2), sid(d, side, 2), to_y)
            go = []
            if ux:
                go.append(copy(b, 2, sid(d, side, 4), sid(d, side, 4), to_x))
            if uc:
                go.append(copy(b, 0, sid(d, side, 7), sid(d, side, 7), to_c))
            out.append((arrive, go))
        return out

    def across(d, side, s):
        out = []
        if ux and uy:
            b = pc.blk(s, 1 - x, 1 - y, c)
            arrive = copy(b, 1, sid(d, side, 3), sid(d, side, 3), to_y)
            go = [copy(b, 1, sid(d, side, 8), sid(d, side, 8), to_c)] if uc else []
            out.append((arrive, go))
            arrive = copy(b, 2, sid(d, side, 4), sid(d, side, 4), to_x)
            go = [copy(b, 2, sid(d, side, 9), sid(d, side, 9), to_c)] if uc else []
            out.append((arrive, go))
        return out

    def partner(d, side, s):
        out = []
        if uc:
            out.append(copy(pc.blk(s, x, y, 1 - c), 0, 0, sid(d, side, 5), to_c))
            if ux:
                out.append(copy(pc.blk(s, 1 - x, y, 1 - c), 0, 0, sid(d, side, 6), to_c))
            if uy:
                out.append(copy(pc.blk(s, x, 1 - y, 1 - c), 0, 0, sid(d, side, 7), to_c))
            if ux and uy:
                b = pc.blk(s, 1 - x, 1 - y, 1 - c)
                out.append(copy(b, 1, 0, sid(d, side, 8), to_c))
                out.append(copy(b, 2, 0, sid(d, side, 9), to_c))
        return out

    steps = pc.line_steps()

    def do_line(step):
        d, side, s, ok = step

        def fn():
            if d > 0:
                copy(pc.blk(s, x, y, c), 0, 0, sid(d, side, 0), to_x).wait_recv()
            for cond, cp in hops(d, side, s):
                when(cond, cp.start)
            for cp in spread(d, side, s):
                cp.start()

        when(ok, fn)

    def do_pass(step, which):
        d, side, s, ok = step

        def fn():
            for arrive, go in which(d, side, s):
                arrive.wait_recv()
                for cp in go:
                    cp.start()

        when(ok, fn)

    groups = [[st for st in steps if st[0] == d] for d in range(nz)]

    def phase(t):
        if t < nz:
            for st in groups[t]:
                do_line(st)
        if 0 <= t - 1 < nz:
            for st in groups[t - 1]:
                do_pass(st, passed)
        if 0 <= t - 2 < nz:
            for st in groups[t - 2]:
                do_pass(st, across)

    def last():
        for st in steps:
            d, side, s, ok = st

            def fn():
                for cp in partner(d, side, s):
                    cp.wait_recv()
                for cond, cp in hops(d, side, s):
                    when(cond, cp.wait_send)
                for cp in spread(d, side, s):
                    cp.wait_send()
                for which in (passed, across):
                    for _, go in which(d, side, s):
                        for cp in go:
                            cp.wait_send()

            when(ok, fn)

    return lambda: None, [functools.partial(phase, t) for t in range(nz + 2)], last


def gather_plane_first(axes, lo, rows, x_ref, o_ref, ssem, rsem):
    nz, ux, uy, uc = axes
    pc = Place(nz, ux, uy, uc)
    z, x, y, c = pc.z, pc.x, pc.y, pc.c
    half = rows // 2
    own = x_ref.at[pl.ds(lo, rows)]
    to_x, to_y, to_c = pc.dev(z, 1 - x, y, c), pc.dev(z, x, 1 - y, c), pc.dev(z, x, y, 1 - c)
    items = [(0, 0, x, y, (lo, rows))]
    if ux:
        items.append((1, 1, 1 - x, y, (lo, rows)))
    if uy:
        items.append((2, 1, x, 1 - y, (lo, rows)))
    if ux and uy:
        items.append((3, 2, 1 - x, 1 - y, (lo, half)))
        items.append((4, 2, 1 - x, 1 - y, (lo + half, half)))
    per = 5
    base = nz * 2 * per

    def iid(d, side, item):
        return (d * 2 + side) * per + item

    def copy(s, px, py, core, span, sidx, ridx, device, src=None):
        ref = o_ref.at[pc.blk(s, px, py, core), pl.ds(span[0], span[1])]
        return pltpu.make_async_remote_copy(
            src_ref=ref if src is None else src,
            dst_ref=ref,
            send_sem=ssem.at[sidx],
            recv_sem=rsem.at[ridx],
            device_id=device,
            device_id_type=MESH_ID,
        )

    def arrival(d, side, s, it):
        item, _, px, py, span = it
        return copy(s, px, py, c, span, 0, iid(d, side, item), to_x)

    def outgoing(d, side, s, it):
        item, _, px, py, span = it
        src = own if d == 0 and item == 0 else None
        out = []
        if d + 1 < nz:
            if d == 0 or side == 0:
                out.append(
                    (
                        z + 1 < nz,
                        copy(s, px, py, c, span, iid(d, 0, item), iid(d + 1, 0, item), pc.dev(z + 1, x, y, c), src),
                    )
                )
            if d == 0 or side == 1:
                out.append(
                    (
                        z >= 1,
                        copy(s, px, py, c, span, iid(d, 1, item), iid(d + 1, 1, item), pc.dev(z - 1, x, y, c), src),
                    )
                )
        if uc:
            at = base + iid(d, side, item)
            out.append((None, copy(s, px, py, c, span, at, at, to_c, src)))
        if d == 0:
            if item == 0 and ux:
                out.append((None, copy(s, px, py, c, span, 2 * base, iid(0, 0, 1), to_x, src)))
            if item == 0 and uy:
                out.append((None, copy(s, px, py, c, span, 2 * base + 1, iid(0, 0, 2), to_y, src)))
            if item == 1 and uy:
                out.append(
                    (None, copy(s, px, py, c, (lo, half), 2 * base + 2, iid(0, 0, 3), to_y))
                )
            if item == 2 and ux:
                out.append(
                    (None, copy(s, px, py, c, (lo + half, half), 2 * base + 3, iid(0, 0, 4), to_x))
                )
        return out

    steps = pc.line_steps()

    def phase(t):
        for d, side, s, ok in steps:
            for it in items:
                if d + it[1] != t:
                    continue

                if d > 0 or it[0] > 0:
                    when(ok, arrival(d, side, s, it).wait_recv)
                for cond, cp in outgoing(d, side, s, it):
                    when(both(ok, cond), cp.start)

    def last():
        for d, side, s, ok in steps:

            for it in items:
                if uc:
                    item, _, px, py, span = it
                    there = copy(s, px, py, 1 - c, span, 0, base + iid(d, side, item), to_c)
                    when(ok, there.wait_recv)
                for cond, cp in outgoing(d, side, s, it):
                    when(both(ok, cond), cp.wait_send)

    return lambda: None, [functools.partial(phase, t) for t in range(nz + 2)], last


WSH_AXES = (1, False, True, True)
CTX_AXES = (4, True, False, False)
ALL_AXES = (4, True, True, True)


def spans_of(axes, rows):
    if axes[0] == 1 or rows % 128:
        return rows, 0
    second = rows // 4 if axes[3] else rows // 8
    return rows - second, second


def run_jobs(axes_list, jobs):
    Place(
        max(a[0] for a in axes_list),
        any(a[1] for a in axes_list),
        any(a[2] for a in axes_list),
        any(a[3] for a in axes_list),
    ).greet()
    for begin, _, _ in jobs:
        begin()
    for t in range(max(len(phases) for _, phases, _ in jobs)):
        for _, phases, _ in jobs:
            if t < len(phases):
                phases[t]()
    for _, _, last in jobs:
        last()


def group_of(axes):
    return (axes[0] * 2 if axes[1] else 1) * (4 if axes[3] else 1)


GATHER_REFS, SCATTER_REFS = 5, 20


def gather_scratch(axes):
    dma = pltpu.SemaphoreType.DMA
    nz = axes[0]
    return [dma((nz * 20,)), dma((nz * 20,)), dma((nz * 20 + 4,)), dma((nz * 20,)), dma]


def gather_jobs(axes, x_ref, o_ref, s1, r1, s2, r2, lsem):
    pc = Place(*axes)
    rows = x_ref.shape[0]
    main, rest = spans_of(axes, rows)
    own = pltpu.make_async_copy(x_ref, o_ref.at[pc.blk(pc.z, pc.x, pc.y, pc.c)], lsem)
    _, phases, last = gather_line_first(axes, 0, main, x_ref, o_ref, s1, r1)

    def end():
        last()
        own.wait()

    jobs = [(own.start, phases, end)]
    if rest:
        jobs.append(gather_plane_first(axes, main, rest, x_ref, o_ref, s2, r2))
    return jobs


def scatter_scratch(axes, shape, dt):
    rows, cols = shape
    nz, ux, uy, uc = axes
    dma = pltpu.SemaphoreType.DMA
    out = []
    for second, n in enumerate(spans_of(axes, rows)):
        few = lambda use, k, r: pltpu.VMEM((k, r, cols) if use and n else (1, 16, cols), dt)
        lines = 1 if second else nz
        out += [
            few(True, nz * 4, n),
            few(uc, nz * 4, n),
            few(ux, lines, n),
            few(uy, lines, n),
            few(ux and uy, lines, n // 2),
            few(ux and uy, lines, n // 2),
            few(nz > 1, (nz + 1) * (4 if second else 1), n),
            dma((nz * (14 if second else 12),)),
            dma((nz * (18 if second else 12),)),
            dma((nz * 4,)),
        ]
    return out


def scatter_jobs(axes, p_ref, o_ref, *refs):
    rows = o_ref.shape[0]
    main, rest = spans_of(axes, rows)
    jobs = [scatter_line_last(axes, 0, main, p_ref, o_ref, *refs[:10])]
    if rest:
        jobs.append(scatter_line_first(axes, main, rest, p_ref, o_ref, *refs[10:]))
    return jobs


def transfer_kernel(kinds, axes_list, *refs):
    n = len(kinds)
    at = 2 * n
    jobs = []
    for i, (kind, axes) in enumerate(zip(kinds, axes_list)):
        many = GATHER_REFS if kind == "gather" else SCATTER_REFS
        make = gather_jobs if kind == "gather" else scatter_jobs
        jobs += make(axes, refs[i], refs[n + i], *refs[at : at + many])
        at += many
    run_jobs(axes_list, jobs)


def transfer(kinds, values, axes_list, collective_id):
    shapes, specs, scratch = [], [], []
    for kind, value, axes in zip(kinds, values, axes_list):
        if kind == "gather":
            shapes.append(jax.ShapeDtypeStruct((group_of(axes),) + value.shape, value.dtype))
            specs.append(pl.BlockSpec(memory_space=pl.ANY))
            scratch += gather_scratch(axes)
        else:
            shapes.append(jax.ShapeDtypeStruct(value.shape[1:], jnp.float32))
            specs.append(pl.BlockSpec(memory_space=pltpu.VMEM))
            scratch += scatter_scratch(axes, value.shape[1:], value.dtype)
    return pl.pallas_call(
        functools.partial(transfer_kernel, kinds, axes_list),
        out_shape=shapes,
        in_specs=[pl.BlockSpec(memory_space=pl.ANY)] * len(values),
        out_specs=specs,
        scratch_shapes=scratch,
        compiler_params=pltpu.CompilerParams(
            collective_id=collective_id, has_side_effects=True, vmem_limit_bytes=61 * 1024 * 1024
        ),
    )(*values)


def scatter_line_last(axes, lo, rows, p_ref, o_ref, acc, rc, rx, ry, ra, rb, rz, ssem, rsem, lsem):
    nz, ux, uy, uc = axes
    pc = Place(nz, ux, uy, uc)
    z, x, y, c = pc.z, pc.x, pc.y, pc.c
    half = rows // 2
    chunk = math.gcd(half, 32)
    f32 = jnp.float32
    to_x, to_y, to_c = pc.dev(z, 1 - x, y, c), pc.dev(z, x, 1 - y, c), pc.dev(z, x, y, 1 - c)
    rels = [(0, x, y)]
    if ux:
        rels.append((1, 1 - x, y))
    if uy:
        rels.append((2, x, 1 - y))
    if ux and uy:
        rels.append((3, 1 - x, 1 - y))
    KINDS = 12

    def slot(s):
        return s if nz > 1 else 0

    def sid(s, kind):
        return slot(s) * KINDS + kind

    def hf(ref, h):
        return ref.at[pl.ds(h * half, half)]

    def rcopy(src, dst, s, kind, device):
        return pltpu.make_async_remote_copy(
            src_ref=src,
            dst_ref=dst,
            send_sem=ssem.at[sid(s, kind)],
            recv_sem=rsem.at[sid(s, kind)],
            device_id=device,
            device_id_type=MESH_ID,
        )

    def load(s, rel, px, py):
        return pltpu.make_async_copy(
            p_ref.at[pc.blk(s, px, py, c), pl.ds(lo, rows)], acc.at[slot(s) * 4 + rel], lsem.at[slot(s) * 4 + rel]
        )

    def give(s, rel, px, py):
        return rcopy(
            p_ref.at[pc.blk(s, px, py, 1 - c), pl.ds(lo, rows)], rc.at[slot(s) * 4 + rel], s, rel, to_c
        )

    def fold(dst, lo, n, srcs):
        def body(i, _):
            r = pl.multiple_of(i * chunk, chunk)
            total = dst[pl.ds(lo + r, chunk), :].astype(f32)
            for ref, at in srcs:
                total = total + ref[pl.ds(at + r, chunk), :].astype(f32)
            dst[pl.ds(lo + r, chunk), :] = total.astype(dst.dtype)
            return 0

        lax.fori_loop(0, n // chunk, body, 0)

    def over_a(s):
        return rcopy(hf(acc.at[slot(s) * 4 + 3], 0), ra.at[slot(s)], s, 4, to_y)

    def over_b(s):
        return rcopy(hf(acc.at[slot(s) * 4 + 3], 1), rb.at[slot(s)], s, 5, to_x)

    def x_half(s, h):
        return rcopy(hf(acc.at[slot(s) * 4 + 1], h), hf(rx.at[slot(s)], h), s, 6 + h, to_x)

    def y_half(s, h):
        return rcopy(hf(acc.at[slot(s) * 4 + 2], h), hf(ry.at[slot(s)], h), s, 8 + h, to_y)

    def z_send(s, up):
        return rcopy(
            acc.at[slot(s) * 4],
            rz.at[slot(s)],
            s,
            10,
            pc.dev(z + (1 if up else -1), x, y, c),
        )

    def z_last(s, up):
        return pltpu.make_async_remote_copy(
            src_ref=acc.at[slot(s) * 4],
            dst_ref=rz.at[slot(s)] if up else rz.at[nz],
            send_sem=ssem.at[sid(s, 10)],
            recv_sem=rsem.at[sid(s, 10)] if up else rsem.at[sid(s, 11)],
            device_id=pc.dev(z + (1 if up else -1), x, y, c),
            device_id_type=MESH_ID,
        )

    steps = list(reversed(pc.line_steps()))

    def begin():
        for d, side, s, ok in steps:

            def fn():
                for rel, px, py in reversed(rels):
                    load(s, rel, px, py).start()
                    if uc:
                        give(s, rel, px, py).start()

            when(ok, fn)

    def first(step):
        _, _, s, ok = step

        def fn():
            for rel, px, py in reversed(rels):
                load(s, rel, px, py).wait()
                if uc:
                    give(s, rel, px, py).wait_recv()
                    fold(acc.at[slot(s) * 4 + rel], 0, rows, [(rc.at[slot(s) * 4 + rel], 0)])
                if rel == 3:
                    over_a(s).start()
                    over_b(s).start()
                if rel == 2:
                    y_half(s, 0).start()
                    if not ux:
                        y_half(s, 1).start()
                if rel == 1:
                    x_half(s, 1).start()
                    if not uy:
                        x_half(s, 0).start()

        when(ok, fn)

    def second(step):
        _, _, s, ok = step

        def fn():
            if ux and uy:
                over_a(s).wait_recv()
                fold(acc.at[slot(s) * 4 + 1], 0, half, [(ra.at[slot(s)], 0)])
                x_half(s, 0).start()
                over_b(s).wait_recv()
                fold(acc.at[slot(s) * 4 + 2], half, half, [(rb.at[slot(s)], 0)])
                y_half(s, 1).start()

        when(ok, fn)

    def third(step):
        d, side, s, ok = step

        def fn():
            srcs = []
            if ux:
                x_half(s, 0).wait_recv()
                x_half(s, 1).wait_recv()
                srcs.append((rx.at[slot(s)], 0))
            if uy:
                y_half(s, 0).wait_recv()
                y_half(s, 1).wait_recv()
                srcs.append((ry.at[slot(s)], 0))
            if d > 0:
                more = (z + 1 < nz) if side == 0 else (z >= 1)

                @pl.when(more)
                def _():
                    z_send(s, side == 1).wait_recv()
                    fold(acc.at[slot(s) * 4], 0, rows, srcs + [(rz.at[slot(s)], 0)])

                if srcs:

                    @pl.when(jnp.logical_not(more))
                    def _():
                        fold(acc.at[slot(s) * 4], 0, rows, srcs)

                if d == 1:
                    z_last(s, side == 1).start()
                else:
                    z_send(s, side == 1).start()
            else:

                def body(use_lo, use_hi):
                    terms = list(srcs)
                    if use_lo:
                        z_last(s, True).wait_recv()
                        terms.append((rz.at[slot(s)], 0))
                    if use_hi:
                        z_last(s, False).wait_recv()
                        terms.append((rz.at[nz], 0))

                    def step_(i, _):
                        r = pl.multiple_of(i * chunk, chunk)
                        total = acc[slot(s) * 4, pl.ds(r, chunk), :].astype(f32)
                        for ref, at in terms:
                            total = total + ref[pl.ds(at + r, chunk), :].astype(f32)
                        o_ref[pl.ds(pl.multiple_of(lo + i * chunk, chunk), chunk), :] = total.astype(
                            o_ref.dtype
                        )
                        return 0

                    lax.fori_loop(0, rows // chunk, step_, 0)

                if nz == 1:
                    body(False, False)
                else:
                    pl.when(jnp.logical_and(z >= 1, z + 1 < nz))(lambda: body(True, True))
                    pl.when(z == nz - 1)(lambda: body(True, False))
                    pl.when(z == 0)(lambda: body(False, True))

        when(ok, fn)

    groups = [[st for st in steps if st[0] == d] for d in reversed(range(nz))]

    def phase(t):
        if t < nz:
            for st in groups[t]:
                first(st)
        if 0 <= t - 1 < nz:
            for st in groups[t - 1]:
                second(st)
        if 0 <= t - 2 < nz:
            for st in groups[t - 2]:
                third(st)

    def last():
        for d, side, s, ok in steps:

            def fn():
                for rel, px, py in rels:
                    if uc:
                        give(s, rel, px, py).wait_send()
                if ux and uy:
                    over_a(s).wait_send()
                    over_b(s).wait_send()
                if ux:
                    x_half(s, 0).wait_send()
                    x_half(s, 1).wait_send()
                if uy:
                    y_half(s, 0).wait_send()
                    y_half(s, 1).wait_send()
                if d > 0:
                    z_send(s, side == 1).wait_send()

            when(ok, fn)

    return begin, [functools.partial(phase, t) for t in range(nz + 2)], last


def scatter_line_first(axes, lo, rows, p_ref, o_ref, acc, rc, rx, ry, ra, rb, rz, ssem, rsem, lsem):
    nz, ux, uy, uc = axes
    pc = Place(nz, ux, uy, uc)
    z, x, y, c = pc.z, pc.x, pc.y, pc.c
    half = rows // 2
    chunk = math.gcd(half, 32)
    f32 = jnp.float32
    to_x, to_y, to_c = pc.dev(z, 1 - x, y, c), pc.dev(z, x, 1 - y, c), pc.dev(z, x, y, 1 - c)
    rels = [(0, x, y)]
    if ux:
        rels.append((1, 1 - x, y))
    if uy:
        rels.append((2, x, 1 - y))
    if ux and uy:
        rels.append((3, 1 - x, 1 - y))
    plane = nz * 4 * 3

    def hf(ref, h):
        return ref.at[pl.ds(h * half, half)]

    def rcopy(src, dst, sidx, ridx, device):
        return pltpu.make_async_remote_copy(
            src_ref=src,
            dst_ref=dst,
            send_sem=ssem.at[sidx],
            recv_sem=rsem.at[ridx],
            device_id=device,
            device_id_type=MESH_ID,
        )

    def load(s, rel, px, py):
        return pltpu.make_async_copy(
            p_ref.at[pc.blk(s, px, py, c), pl.ds(lo, rows)], acc.at[s * 4 + rel], lsem.at[s * 4 + rel]
        )

    def give(s, rel, px, py):
        at = s * 4 + rel
        return rcopy(p_ref.at[pc.blk(s, px, py, 1 - c), pl.ds(lo, rows)], rc.at[at], at, at, to_c)

    def hop(s, rel, up, final):
        extra = final and not up
        return rcopy(
            acc.at[s * 4 + rel],
            rz.at[nz * 4 + rel] if extra else rz.at[s * 4 + rel],
            nz * 4 + s * 4 + rel,
            (nz * 8 + s * 4 + rel) if extra else (nz * 4 + s * 4 + rel),
            pc.dev(z + (1 if up else -1), x, y, c),
        )

    def fold(dst, at, n, srcs):
        def body(i, _):
            r = pl.multiple_of(i * chunk, chunk)
            total = dst[pl.ds(pl.multiple_of(at + r, chunk), chunk), :].astype(f32)
            for ref, first in srcs:
                total = total + ref[pl.ds(pl.multiple_of(first + r, chunk), chunk), :].astype(f32)
            dst[pl.ds(pl.multiple_of(at + r, chunk), chunk), :] = total.astype(dst.dtype)
            return 0

        lax.fori_loop(0, n // chunk, body, 0)

    def mine(rel):
        return acc.at[z * 4 + rel]

    def over_a():
        return rcopy(hf(mine(3), 0), ra.at[0], nz * 8, plane, to_y)

    def over_b():
        return rcopy(hf(mine(3), 1), rb.at[0], nz * 8 + 1, plane + 1, to_x)

    def x_half(h):
        return rcopy(hf(mine(1), h), hf(rx.at[0], h), nz * 8 + 2 + h, plane + 2 + h, to_x)

    def y_half(h):
        return rcopy(hf(mine(2), h), hf(ry.at[0], h), nz * 8 + 4 + h, plane + 4 + h, to_y)

    steps = list(reversed(pc.line_steps()))

    def begin():
        for d, side, s, ok in steps:

            def fn():
                for rel, px, py in reversed(rels):
                    load(s, rel, px, py).start()
                    if uc:
                        give(s, rel, px, py).start()

            when(ok, fn)

    def line(step):
        d, side, s, ok = step

        def fn():
            more = (z + 1 < nz) if side == 0 else (z >= 1)
            for rel, px, py in reversed(rels):
                load(s, rel, px, py).wait()
                srcs = []
                if uc:
                    give(s, rel, px, py).wait_recv()
                    srcs = [(rc.at[s * 4 + rel], 0)]
                target = acc.at[s * 4 + rel]
                if d > 0:

                    @pl.when(more)
                    def _():
                        hop(s, rel, side == 1, False).wait_recv()
                        fold(target, 0, rows, srcs + [(rz.at[s * 4 + rel], 0)])

                    if srcs:

                        @pl.when(jnp.logical_not(more))
                        def _():
                            fold(target, 0, rows, srcs)

                    hop(s, rel, side == 1, d == 1).start()
                else:
                    lower, upper = (rz.at[s * 4 + rel], 0), (rz.at[nz * 4 + rel], 0)

                    @pl.when(z >= 1)
                    def _():
                        hop(s, rel, True, True).wait_recv()

                    @pl.when(z + 1 < nz)
                    def _():
                        hop(s, rel, False, True).wait_recv()

                    both = jnp.logical_and(z >= 1, z + 1 < nz)
                    pl.when(both)(lambda: fold(target, 0, rows, srcs + [lower, upper]))
                    pl.when(z == 0)(lambda: fold(target, 0, rows, srcs + [upper]))
                    pl.when(z == nz - 1)(lambda: fold(target, 0, rows, srcs + [lower]))
                    if rel == 3:
                        over_a().start()
                        over_b().start()
                    if rel == 2:
                        y_half(0).start()
                        if not ux:
                            y_half(1).start()
                    if rel == 1:
                        x_half(1).start()
                        if not uy:
                            x_half(0).start()

        when(ok, fn)

    def cross():
        if ux and uy:
            over_a().wait_recv()
            fold(mine(1), 0, half, [(ra.at[0], 0)])
            x_half(0).start()
            over_b().wait_recv()
            fold(mine(2), half, half, [(rb.at[0], 0)])
            y_half(1).start()

    def total():
        srcs = []
        if ux:
            x_half(0).wait_recv()
            x_half(1).wait_recv()
            srcs.append(rx)
        if uy:
            y_half(0).wait_recv()
            y_half(1).wait_recv()
            srcs.append(ry)

        def body(i, _):
            r = pl.multiple_of(i * chunk, chunk)
            value = acc[z * 4, pl.ds(r, chunk), :].astype(f32)
            for ref in srcs:
                value = value + ref[0, pl.ds(r, chunk), :].astype(f32)
            o_ref[pl.ds(pl.multiple_of(lo + i * chunk, chunk), chunk), :] = value.astype(o_ref.dtype)
            return 0

        lax.fori_loop(0, rows // chunk, body, 0)

    groups = [[st for st in steps if st[0] == d] for d in reversed(range(nz))]

    def phase(t):
        if t < nz:
            for st in groups[t]:
                line(st)
        elif t == nz:
            cross()
        else:
            total()

    def last():
        for d, side, s, ok in steps:

            def fn():
                for rel, px, py in rels:
                    if uc:
                        give(s, rel, px, py).wait_send()
                    if d > 0:
                        hop(s, rel, side == 1, d == 1).wait_send()

            when(ok, fn)
        if ux and uy:
            over_a().wait_send()
            over_b().wait_send()
        if ux:
            x_half(0).wait_send()
            x_half(1).wait_send()
        if uy:
            y_half(0).wait_send()
            y_half(1).wait_send()

    return begin, [functools.partial(phase, t) for t in range(nz + 2)], last


LOG2E = 1.4426950408889634


def lane_swap(tensor):
    return pltpu.roll(tensor, tensor.shape[-1] // 2, tensor.ndim - 1)


def head_norm(tensor, gain, cos2, sin2):
    inverse = lax.rsqrt(jnp.mean(tensor * tensor, axis=-1, keepdims=True) + EPSILON)
    scaled = tensor * inverse * gain
    return scaled * cos2 + lane_swap(scaled) * sin2


def head_norm_back(tensor, gain, cos2, sin2, gradient):
    inverse = lax.rsqrt(jnp.mean(tensor * tensor, axis=-1, keepdims=True) + EPSILON)
    turned = gradient * cos2 - lane_swap(gradient) * sin2
    weighted = turned * gain
    inner = jnp.mean(weighted * tensor, axis=-1, keepdims=True)
    return (
        inverse * weighted - tensor * (inverse * inverse * inverse) * inner,
        turned * tensor * inverse,
    )


def token_rows(piece, seq, seq_count, rows_dev):
    return (piece * seq_count + seq) * rows_dev


def kv_prep_kernel(pieces, seqs, proj_ref, gain_ref, cos_ref, sin_ref, o_ref):
    hd = gain_ref.shape[-1]
    rows = proj_ref.shape[0] // (pieces * seqs)
    for piece in range(pieces):
        cos2 = cos_ref[piece * rows : (piece + 1) * rows, :]
        sin2 = sin_ref[piece * rows : (piece + 1) * rows, :]
        for seq in range(seqs):
            at = token_rows(piece, seq, seqs, rows)
            raw = proj_ref[at : at + rows, :hd]
            o_ref[at : at + rows, :hd] = head_norm(raw, gain_ref[...], cos2, sin2).astype(
                o_ref.dtype
            )
            o_ref[at : at + rows, hd:] = proj_ref[at : at + rows, hd:].astype(o_ref.dtype)


def kv_prep(projected, key_gain, cos2, sin2, heads, pieces, seqs):
    rows, _ = projected.shape
    hd = key_gain.shape[0]
    whole = lambda *shape: pl.BlockSpec(shape, lambda i: (0,) * len(shape))
    return pl.pallas_call(
        functools.partial(kv_prep_kernel, pieces, seqs),
        grid=(1,),
        out_shape=jax.ShapeDtypeStruct((rows, 2 * hd), jnp.bfloat16),
        in_specs=[
            pl.BlockSpec((rows, 2 * hd), lambda i: (0, heads // 2)),
            whole(1, hd),
            whole(*cos2.shape),
            whole(*sin2.shape),
        ],
        out_specs=whole(rows, 2 * hd),
        name="kv_prep",
    )(projected, key_gain.reshape(1, hd), cos2, sin2)


def kv_back_kernel(pieces, seqs, proj_ref, cot_ref, gain_ref, cos_ref, sin_ref, _, low_ref, gg_ref):
    hd = gain_ref.shape[-1]
    rows = proj_ref.shape[0] // (pieces * seqs)
    total = jnp.zeros((1, hd), jnp.float32)
    for piece in range(pieces):
        cos2 = cos_ref[piece * rows : (piece + 1) * rows, :]
        sin2 = sin_ref[piece * rows : (piece + 1) * rows, :]
        for seq in range(seqs):
            at = token_rows(piece, seq, seqs, rows)
            grad, terms = head_norm_back(
                proj_ref[at : at + rows, :hd],
                gain_ref[...],
                cos2,
                sin2,
                cot_ref[at : at + rows, :hd],
            )
            low_ref[at : at + rows, :hd] = grad.astype(low_ref.dtype)
            low_ref[at : at + rows, hd:] = cot_ref[at : at + rows, hd:].astype(low_ref.dtype)
            total = total + jnp.sum(terms, axis=0, keepdims=True)
    gg_ref[...] = total


def kv_back(projected, kv_cot, key_gain, cos2, sin2, low, heads, pieces, seqs):
    rows, _ = projected.shape
    hd = key_gain.shape[0]
    whole = lambda *shape: pl.BlockSpec(shape, lambda i: (0,) * len(shape))
    return pl.pallas_call(
        functools.partial(kv_back_kernel, pieces, seqs),
        grid=(1,),
        out_shape=(
            jax.ShapeDtypeStruct(low.shape, low.dtype),
            jax.ShapeDtypeStruct((1, hd), jnp.float32),
        ),
        in_specs=[
            pl.BlockSpec((rows, 2 * hd), lambda i: (0, heads // 2)),
            whole(rows, 2 * hd),
            whole(1, hd),
            whole(*cos2.shape),
            whole(*sin2.shape),
            pl.BlockSpec(memory_space=pl.ANY),
        ],
        out_specs=(pl.BlockSpec((rows, 2 * hd), lambda i: (0, heads // 2)), whole(1, hd)),
        input_output_aliases={5: 0},
        name="kv_back",
    )(projected, kv_cot, key_gain.reshape(1, hd), cos2, sin2, low)


def sort_blocks(loc_ref, kv_ref, dst, seqs, rows, pieces, hd, lo, blocks):
    per_half = pieces // 2

    def body(b, _):
        loc = loc_ref[b]
        chunk, half = loc // 2, loc % 2
        for seq in range(seqs):
            for i in range(per_half):
                at = ((half * per_half + i) * seqs + seq) * rows
                dst[seq, pl.ds(b * (per_half * rows) + i * rows, rows), :] = kv_ref[
                    chunk, pl.ds(at, rows), lo : lo + hd
                ]
        return 0

    lax.fori_loop(0, blocks, body, 0)


def attend_kernel(
    heads, pieces, seqs, scale, loc_ref, own_ref, proj_ref, kv_ref, gain_ref, cos_ref, sin_ref,
    attn_ref, lse_ref, qs_ref, ks, vs, acc, tot,
):
    f32, bf16 = jnp.float32, jnp.bfloat16
    hd = gain_ref.shape[-1]
    rows = proj_ref.shape[0] // (pieces * seqs)
    per_half = pieces // 2
    block = per_half * rows
    blocks = 2 * kv_ref.shape[0]
    pair = 2 * block
    tile = heads * block
    sort_blocks(loc_ref, kv_ref, ks, seqs, rows, pieces, hd, 0, blocks)
    sort_blocks(loc_ref, kv_ref, vs, seqs, rows, pieces, hd, hd, blocks)
    for seq in range(seqs):
        for half in range(2):
            unit = seq * 2 + half
            for h in range(heads):
                for i in range(per_half):
                    piece = half * per_half + i
                    at = token_rows(piece, seq, seqs, rows)
                    turned = head_norm(
                        proj_ref[at : at + rows, h * hd : (h + 1) * hd],
                        gain_ref[...],
                        cos_ref[piece * rows : (piece + 1) * rows, :],
                        sin_ref[piece * rows : (piece + 1) * rows, :],
                    )
                    qs_ref[unit, h * block + i * rows : h * block + (i + 1) * rows, :] = (
                        turned.astype(bf16)
                    )
            acc[...] = jnp.zeros_like(acc)
            tot[...] = jnp.zeros_like(tot)
            mine = own_ref[half]

            def step(j, masked):
                keys = ks[seq, pl.ds(j * pair, pair), :]
                values = vs[seq, pl.ds(j * pair, pair), :]
                for t in range(heads * block // tile):
                    cols = slice(t * tile, (t + 1) * tile)
                    scores = lax.dot_general(
                        keys,
                        qs_ref[unit, cols, :],
                        (((1,), (1,)), ((), ())),
                        preferred_element_type=f32,
                    )
                    expo = jnp.exp2(scores * (scale * LOG2E))
                    if masked:
                        key_pos = j * pair + lax.broadcasted_iota(jnp.int32, expo.shape, 0)
                        query_pos = mine * block + (
                            lax.broadcasted_iota(jnp.int32, expo.shape, 1) % block
                        )
                        expo = jnp.where(key_pos <= query_pos, expo, 0.0)
                    tot[:, cols] += jnp.sum(expo.reshape(pair // 8, 8, tile), axis=0)
                    acc[:, cols] += lax.dot_general(
                        values,
                        expo.astype(bf16),
                        (((0,), (0,)), ((), ())),
                        preferred_element_type=f32,
                    )

            def body(j, _):
                step(j, False)
                return 0

            lax.fori_loop(0, mine // 2, body, 0)
            step(mine // 2, True)
            total = jnp.sum(tot[...], axis=0, keepdims=True)
            lse_ref[unit, :, :] = jnp.log(total)
            share = 1.0 / total
            for h in range(heads):
                cols = slice(h * block, (h + 1) * block)
                out = jnp.transpose(acc[:, cols] * share[:, cols]).astype(bf16)
                for i in range(per_half):
                    at = token_rows(half * per_half + i, seq, seqs, rows)
                    attn_ref[at : at + rows, h * hd : (h + 1) * hd] = out[
                        i * rows : (i + 1) * rows, :
                    ]


def attend(projected, kv_all, query_gain, cos2, sin2, loc, own, heads, pieces, seqs):
    rows = projected.shape[0]
    hd = query_gain.shape[0]
    units = 2 * seqs
    block = rows // units
    keys = kv_all.shape[0] * kv_all.shape[1] // seqs
    whole = lambda *shape: pl.BlockSpec(shape, lambda i, *_: (0,) * len(shape))
    f32, bf16 = jnp.float32, jnp.bfloat16
    return pl.pallas_call(
        functools.partial(attend_kernel, heads, pieces, seqs, hd**-0.5),
        grid_spec=pltpu.PrefetchScalarGridSpec(
            num_scalar_prefetch=2,
            grid=(1,),
            in_specs=[
                pl.BlockSpec((rows, heads * hd), lambda i, *_: (0, 0)),
                whole(*kv_all.shape),
                whole(1, hd),
                whole(*cos2.shape),
                whole(*sin2.shape),
            ],
            out_specs=[
                whole(rows, heads * hd),
                whole(units, 1, heads * block),
                whole(units, heads * block, hd),
            ],
            scratch_shapes=[
                pltpu.VMEM((seqs, keys, hd), bf16),
                pltpu.VMEM((seqs, keys, hd), bf16),
                pltpu.VMEM((hd, heads * block), f32),
                pltpu.VMEM((8, heads * block), f32),
            ],
        ),
        out_shape=(
            jax.ShapeDtypeStruct((rows, heads * hd), bf16),
            jax.ShapeDtypeStruct((units, 1, heads * block), f32),
            jax.ShapeDtypeStruct((units, heads * block, hd), bf16),
        ),
        compiler_params=pltpu.CompilerParams(vmem_limit_bytes=56 * 1024 * 1024),
        name="attend",
    )(loc, own, projected, kv_all, query_gain.reshape(1, hd), cos2, sin2)


def attend_back_kernel(
    heads, pieces, seqs, scale, loc_ref, own_ref, proj_ref, kv_ref, qs_ref, attn_ref, cot_ref,
    lse_ref, gain_ref, cos_ref, sin_ref, low_ref, dkv_ref, gg_ref, ks, vs, dk, dv, dq, cs, dl,
):
    f32, bf16 = jnp.float32, jnp.bfloat16
    hd = gain_ref.shape[-1]
    rows = proj_ref.shape[0] // (pieces * seqs)
    per_half = pieces // 2
    block = per_half * rows
    blocks = 2 * kv_ref.shape[0]
    pair = 2 * block
    tile = heads * block
    sort_blocks(loc_ref, kv_ref, ks, seqs, rows, pieces, hd, 0, blocks)
    sort_blocks(loc_ref, kv_ref, vs, seqs, rows, pieces, hd, hd, blocks)
    dk[...] = jnp.zeros_like(dk)
    dv[...] = jnp.zeros_like(dv)
    gain_total = jnp.zeros((1, hd), f32)
    ones = jnp.ones((8, hd), bf16)
    nt = (((1,), (1,)), ((), ()))
    for seq in range(seqs):
        for half in range(2):
            unit = seq * 2 + half
            for h in range(heads):
                for i in range(per_half):
                    at = token_rows(half * per_half + i, seq, seqs, rows)
                    to = slice(h * block + i * rows, h * block + (i + 1) * rows)
                    part = cot_ref[at : at + rows, h * hd : (h + 1) * hd]
                    cs[to, :] = part
                    prod = part.astype(f32) * attn_ref[
                        at : at + rows, h * hd : (h + 1) * hd
                    ].astype(f32)
                    dq[to, :] = prod
            for t in range(heads * block // tile):
                cols = slice(t * tile, (t + 1) * tile)
                prod = dq[cols, :]
                high = prod.astype(bf16)
                rest = (prod - high.astype(f32)).astype(bf16)
                dl[:, cols] = lax.dot_general(
                    ones, high, nt, preferred_element_type=f32
                ) + lax.dot_general(ones, rest, nt, preferred_element_type=f32)
            dq[...] = jnp.zeros_like(dq)
            mine = own_ref[half]

            def step(j, masked):
                at = pl.ds(j * pair, pair)
                keys = ks[seq, at, :]
                values = vs[seq, at, :]
                key_sum = jnp.zeros((pair, hd), f32)
                value_sum = jnp.zeros((pair, hd), f32)
                for t in range(heads * block // tile):
                    cols = slice(t * tile, (t + 1) * tile)
                    query = qs_ref[unit, cols, :]
                    cot = cs[cols, :]
                    scores = lax.dot_general(keys, query, nt, preferred_element_type=f32)
                    weights = jnp.exp2(
                        scores * (scale * LOG2E) - lse_ref[unit, :, cols] * LOG2E
                    )
                    if masked:
                        key_pos = j * pair + lax.broadcasted_iota(jnp.int32, weights.shape, 0)
                        query_pos = mine * block + (
                            lax.broadcasted_iota(jnp.int32, weights.shape, 1) % block
                        )
                        weights = jnp.where(key_pos <= query_pos, weights, 0.0)
                    prob_cot = lax.dot_general(values, cot, nt, preferred_element_type=f32)
                    low = (weights * (prob_cot - dl[0:1, cols])).astype(bf16)
                    value_sum = value_sum + jnp.dot(
                        weights.astype(bf16), cot, preferred_element_type=f32
                    )
                    key_sum = key_sum + jnp.dot(low, query, preferred_element_type=f32)
                    dq[cols, :] += lax.dot_general(
                        low, keys, (((0,), (0,)), ((), ())), preferred_element_type=f32
                    )
                dk[seq, at, :] += key_sum
                dv[seq, at, :] += value_sum

            def body(j, _):
                step(j, False)
                return 0

            lax.fori_loop(0, mine // 2, body, 0)
            step(mine // 2, True)
            for h in range(heads):
                for i in range(per_half):
                    piece = half * per_half + i
                    at = token_rows(piece, seq, seqs, rows)
                    grad, terms = head_norm_back(
                        proj_ref[at : at + rows, h * hd : (h + 1) * hd],
                        gain_ref[...],
                        cos_ref[piece * rows : (piece + 1) * rows, :],
                        sin_ref[piece * rows : (piece + 1) * rows, :],
                        dq[h * block + i * rows : h * block + (i + 1) * rows, :] * scale,
                    )
                    low_ref[at : at + rows, h * hd : (h + 1) * hd] = grad.astype(bf16)
                    gain_total = gain_total + jnp.sum(terms, axis=0, keepdims=True)
    gg_ref[...] = gain_total

    def unsort(b, _):
        loc = loc_ref[b]
        chunk, half = loc // 2, loc % 2
        for seq in range(seqs):
            for i in range(per_half):
                at = pl.ds(((half * per_half + i) * seqs + seq) * rows, rows)
                here = pl.ds(b * block + i * rows, rows)
                dkv_ref[chunk, at, 0:hd] = (dk[seq, here, :] * scale).astype(bf16)
                dkv_ref[chunk, at, hd : 2 * hd] = dv[seq, here, :].astype(bf16)
        return 0

    lax.fori_loop(0, blocks, unsort, 0)


def attend_back(
    projected, kv_all, rotated, attention, attention_cot, log_total, query_gain, cos2, sin2, loc,
    own, heads, pieces, seqs,
):
    rows, all_cols = projected.shape
    hd = query_gain.shape[0]
    units = 2 * seqs
    block = rows // units
    keys = kv_all.shape[0] * kv_all.shape[1] // seqs
    whole = lambda *shape: pl.BlockSpec(shape, lambda i, *_: (0,) * len(shape))
    f32, bf16 = jnp.float32, jnp.bfloat16
    return pl.pallas_call(
        functools.partial(attend_back_kernel, heads, pieces, seqs, hd**-0.5),
        grid_spec=pltpu.PrefetchScalarGridSpec(
            num_scalar_prefetch=2,
            grid=(1,),
            in_specs=[
                pl.BlockSpec((rows, heads * hd), lambda i, *_: (0, 0)),
                whole(*kv_all.shape),
                whole(*rotated.shape),
                whole(rows, heads * hd),
                whole(rows, heads * hd),
                whole(*log_total.shape),
                whole(1, hd),
                whole(*cos2.shape),
                whole(*sin2.shape),
            ],
            out_specs=[
                pl.BlockSpec((rows, heads * hd), lambda i, *_: (0, 0)),
                whole(*kv_all.shape),
                whole(1, hd),
            ],
            scratch_shapes=[
                pltpu.VMEM((seqs, keys, hd), bf16),
                pltpu.VMEM((seqs, keys, hd), bf16),
                pltpu.VMEM((seqs, keys, hd), f32),
                pltpu.VMEM((seqs, keys, hd), f32),
                pltpu.VMEM((heads * block, hd), f32),
                pltpu.VMEM((heads * block, hd), bf16),
                pltpu.VMEM((8, heads * block), f32),
            ],
        ),
        out_shape=(
            jax.ShapeDtypeStruct((rows, all_cols), bf16),
            jax.ShapeDtypeStruct(kv_all.shape, bf16),
            jax.ShapeDtypeStruct((1, hd), f32),
        ),
        compiler_params=pltpu.CompilerParams(vmem_limit_bytes=60 * 1024 * 1024),
        name="attend_back",
    )(
        loc, own, projected, kv_all, rotated, attention, attention_cot, log_total,
        query_gain.reshape(1, hd), cos2, sin2,
    )


def picks_of(slots, capacity):
    return lax.broadcasted_iota(jnp.int32, (capacity, slots.shape[1]), 0) == slots


def expert_kernel(
    capacity, slot_ref, weight_ref, x_ref, c_ref, gate_ref, up_ref, down_ref,
    rows_ref, cot_ref, act_ref, gate_cot, up_cot, out_parts, row_parts, wc_ref, w_sc, cot_sc,
):
    f32, bf16 = jnp.float32, jnp.bfloat16
    nt = (((1,), (1,)), ((), ()))
    tn = (((0,), (0,)), ((), ()))
    devices = x_ref.shape[0]
    picks = [picks_of(slot_ref[d], capacity) for d in range(devices)]
    spans = [slice(d * capacity, (d + 1) * capacity) for d in range(devices)]
    for d in range(devices):
        low = picks[d].astype(bf16)
        rows_ref[spans[d], :] = jnp.dot(low, x_ref[d], preferred_element_type=f32).astype(bf16)
        cot_sc[spans[d], :] = jnp.dot(low, c_ref[d], preferred_element_type=f32).astype(bf16)
        w_sc[spans[d], :] = jnp.sum(
            jnp.where(picks[d], weight_ref[d], 0.0), axis=1, keepdims=True
        )
    rows = rows_ref[...]
    gate = jnp.dot(rows, gate_ref[...], preferred_element_type=f32)
    up = jnp.dot(rows, up_ref[...], preferred_element_type=f32)
    sigmoid = jax.nn.sigmoid(gate)
    swish = gate * sigmoid
    activation = (swish * up).astype(bf16)
    act_ref[...] = activation
    cot_ref[...] = (w_sc[...] * cot_sc[...].astype(f32)).astype(bf16)
    act_cot = lax.dot_general(cot_ref[...], down_ref[...], nt, preferred_element_type=f32)
    low_gate = (act_cot * up * sigmoid * (1.0 + gate * (1.0 - sigmoid))).astype(bf16)
    low_up = (act_cot * swish).astype(bf16)
    gate_cot[...] = low_gate
    up_cot[...] = low_up
    produced = jnp.dot(activation, down_ref[...], preferred_element_type=f32).astype(bf16)
    for d in range(devices):
        made = produced[spans[d], :].astype(f32)
        share = jnp.sum(cot_sc[spans[d], :].astype(f32) * made, axis=1, keepdims=True)
        wc_ref[d] = jnp.sum(jnp.where(picks[d], share, 0.0), axis=0, keepdims=True)
        out_parts[d] = lax.dot_general(
            picks[d].astype(bf16),
            (w_sc[spans[d], :] * made).astype(bf16),
            tn,
            preferred_element_type=f32,
        ).astype(bf16)
    row_cot = lax.dot_general(low_gate, gate_ref[...], nt, preferred_element_type=f32)
    row_cot = row_cot + lax.dot_general(low_up, up_ref[...], nt, preferred_element_type=f32)
    row_cot = row_cot.astype(bf16)
    for d in range(devices):
        row_parts[d] = lax.dot_general(
            picks[d].astype(bf16), row_cot[spans[d], :], tn, preferred_element_type=f32
        ).astype(bf16)


def expert_pass(slots, weights, tokens_all, cot_all, gate_w, up_w, down_w, capacity, per_step):
    f32, bf16 = jnp.float32, jnp.bfloat16
    devices, tokens, width = tokens_all.shape
    hidden = gate_w.shape[1]
    rows = per_step * capacity
    total = devices * capacity
    lead = lambda *shape: pl.BlockSpec(shape, lambda i: (i,) + (0,) * (len(shape) - 1))
    fixed = lambda a: pl.BlockSpec(a.shape, lambda i: (0, 0), pipeline_mode=pl.Buffered(1))
    return pl.pallas_call(
        functools.partial(expert_kernel, capacity),
        grid=(devices // per_step,),
        in_specs=[
            lead(per_step, 1, tokens),
            lead(per_step, 1, tokens),
            lead(per_step, tokens, width),
            lead(per_step, tokens, width),
            fixed(gate_w),
            fixed(up_w),
            fixed(down_w),
        ],
        out_specs=[
            lead(rows, width),
            lead(rows, width),
            lead(rows, hidden),
            lead(rows, hidden),
            lead(rows, hidden),
            lead(per_step, tokens, width),
            lead(per_step, tokens, width),
            lead(per_step, 1, tokens),
        ],
        out_shape=[
            jax.ShapeDtypeStruct((total, width), bf16),
            jax.ShapeDtypeStruct((total, width), bf16),
            jax.ShapeDtypeStruct((total, hidden), bf16),
            jax.ShapeDtypeStruct((total, hidden), bf16),
            jax.ShapeDtypeStruct((total, hidden), bf16),
            jax.ShapeDtypeStruct((devices, tokens, width), bf16),
            jax.ShapeDtypeStruct((devices, tokens, width), bf16),
            jax.ShapeDtypeStruct((devices, 1, tokens), f32),
        ],
        scratch_shapes=[pltpu.VMEM((rows, 1), f32), pltpu.VMEM((rows, width), bf16)],
        compiler_params=pltpu.CompilerParams(vmem_limit_bytes=62 * 1024 * 1024),
        name="expert_pass",
    )(slots, weights, tokens_all, cot_all, gate_w, up_w, down_w)


def product_kernel(a_ref, *refs):
    n = len(refs) // 2
    for b_ref, o_ref in zip(refs[:n], refs[n:]):
        o_ref[0] = lax.dot_general(
            a_ref[...], b_ref[...], (((0,), (0,)), ((), ())), preferred_element_type=jnp.float32
        )


def column_products(a, others, block):
    rows, k = a.shape
    return pl.pallas_call(
        product_kernel,
        grid=(k // block,),
        in_specs=[pl.BlockSpec((rows, block), lambda i: (0, i))]
        + [
            pl.BlockSpec(b.shape, lambda i: (0, 0), pipeline_mode=pl.Buffered(1)) for b in others
        ],
        out_specs=[pl.BlockSpec((1, block, b.shape[1]), lambda i: (0, i, 0)) for b in others],
        out_shape=[jax.ShapeDtypeStruct((1, k, b.shape[1]), jnp.float32) for b in others],
        compiler_params=pltpu.CompilerParams(vmem_limit_bytes=60 * 1024 * 1024),
    )(a, *others)


def own_kernels():
    return lax.axis_size("ctx") == 8 and lax.axis_size("wsh") == 4


AXIS_NAMES = {WSH_AXES: "wsh", CTX_AXES: "ctx", ALL_AXES: ("ctx", "wsh")}


def gather(shards, axes_list, ident):
    if own_kernels():
        return transfer(["gather"] * len(shards), shards, axes_list, ident)
    return [lax.all_gather(x, AXIS_NAMES[axes], axis=0) for x, axes in zip(shards, axes_list)]


def scatter(parts, axes_list, ident):
    if own_kernels():
        return transfer(["scatter"] * len(parts), parts, axes_list, ident)
    return [
        lax.psum_scatter(x, AXIS_NAMES[axes], scatter_dimension=0, tiled=False).astype(jnp.float32)
        for x, axes in zip(parts, axes_list)
    ]


def exchange(pieces):
    return lax.all_to_all(pieces, ("ctx", "wsh"), split_axis=0, concat_axis=0, tiled=True)


def to_everyone(value, device_count):
    return exchange(jnp.broadcast_to(value[None], (device_count,) + value.shape))


def experts_plain(
    slot_mine, weight_mine, moe_all, cot_all, gate_w, up_w, down_w, capacity
):
    f32, bf16 = jnp.float32, jnp.bfloat16
    device_count, _, width = moe_all.shape
    picks = slot_mine[:, None, :] == jnp.arange(capacity, dtype=jnp.int32)[None, :, None]
    picks_low = picks.astype(bf16)
    slot_weight = jnp.sum(jnp.where(picks, weight_mine[:, None, :], 0.0), axis=-1)

    def take(everyone):
        return (
            jnp.einsum("dct,dtw->dcw", picks_low, everyone, preferred_element_type=f32)
            .astype(bf16)
            .reshape(device_count * capacity, width)
        )

    def put(rows):
        return jnp.einsum(
            "dct,dcw->dtw",
            picks_low,
            rows.reshape(device_count, capacity, width),
            preferred_element_type=f32,
        ).astype(bf16)

    rows_in = take(moe_all)
    cot_rows = take(cot_all).astype(f32)
    weight_rows = slot_weight.reshape(device_count * capacity, 1)
    route_cot = (weight_rows * cot_rows).astype(bf16)
    gate_pre = jnp.dot(rows_in, gate_w, preferred_element_type=f32)
    up_pre = jnp.dot(rows_in, up_w, preferred_element_type=f32)
    sigmoid = jax.nn.sigmoid(gate_pre)
    swish = gate_pre * sigmoid
    activation = (swish * up_pre).astype(bf16)
    produced = jnp.dot(activation, down_w, preferred_element_type=f32).astype(bf16).astype(f32)
    out_parts = put((weight_rows * produced).astype(bf16))
    slot_cot = jnp.sum(cot_rows * produced, axis=-1).reshape(device_count, capacity)
    cot_mine = jnp.sum(jnp.where(picks, slot_cot[:, :, None], 0.0), axis=1)
    down_grad = jnp.einsum("rf,rd->fd", activation, route_cot, preferred_element_type=f32)
    act_cot = jnp.einsum("rd,fd->rf", route_cot, down_w, preferred_element_type=f32)
    gate_cot = (act_cot * up_pre * sigmoid * (1.0 + gate_pre * (1.0 - sigmoid))).astype(bf16)
    up_cot = (act_cot * swish).astype(bf16)
    gate_grad = jnp.einsum("rd,rf->df", rows_in, gate_cot, preferred_element_type=f32)
    up_grad = jnp.einsum("rd,rf->df", rows_in, up_cot, preferred_element_type=f32)
    row_cot = jnp.einsum("rf,df->rd", gate_cot, gate_w, preferred_element_type=f32)
    row_cot = row_cot + jnp.einsum("rf,df->rd", up_cot, up_w, preferred_element_type=f32)
    return (
        out_parts,
        cot_mine,
        put(row_cot.astype(bf16)),
        gate_grad[None],
        up_grad[None],
        down_grad[None],
    )


def local(
    inputs,
    pair_map,
    norm_gain,
    query_weight,
    key_weight,
    value_weight,
    query_gain,
    key_gain,
    out_weight,
    moe_gain,
    router,
    expert_gate,
    expert_up,
    expert_down,
    expert_ids,
    dispatch_slot,
    cotangent,
):
    f32, bf16 = jnp.float32, jnp.bfloat16
    rows_dev, seq_count, width = inputs.shape
    ctx_count = lax.axis_size("ctx")
    wsh_count = lax.axis_size("wsh")
    device_count = ctx_count * wsh_count
    head_dim = query_gain.shape[0]
    group_rows = rows_dev * wsh_count
    block_len = group_rows // 2
    seq_len = group_rows * ctx_count
    tokens = rows_dev * seq_count
    group_tokens = tokens * wsh_count
    top_count = expert_ids.shape[-1]
    expert_count = router.shape[1]
    capacity = max(2, 3 * top_count * block_len // (2 * device_count))
    positions = positions_of(pair_map, seq_len, block_len, pair_map.shape[0])
    me_ctx = lax.axis_index("ctx")
    query_pos = lax.dynamic_slice_in_dim(positions, me_ctx * group_rows, group_rows, 0)
    cosine, sine_table = rope_tables(query_pos, head_dim)
    cos2 = jnp.concatenate([cosine, cosine], axis=1)
    sin2 = jnp.concatenate([-sine_table, sine_table], axis=1)
    block_ids = jnp.arange(2 * ctx_count, dtype=jnp.int32)
    blocks_by_loc = jnp.stack([pair_map, 2 * ctx_count - 1 - pair_map], axis=1).reshape(-1)
    loc = jnp.sum(
        jnp.where(blocks_by_loc[None, :] == block_ids[:, None], block_ids[None, :], 0), axis=1
    ).astype(jnp.int32)
    own_blocks = lax.dynamic_slice_in_dim(blocks_by_loc, 2 * me_ctx, 2, 0)

    inputs_f = inputs.transpose(1, 0, 2).reshape(tokens, width).astype(f32)
    cot_flat = cotangent.transpose(1, 0, 2).reshape(tokens, width)
    normed_f, inverse_one = rms_forward(inputs_f, norm_gain)
    q_cols, kv_cols = query_weight.shape[1], key_weight.shape[1]
    heads_loc = q_cols // head_dim
    qkv_shard = jnp.concatenate([query_weight, key_weight, value_weight], axis=1)
    normed_flat, qkv_full = gather([normed_f.astype(bf16), qkv_shard], [WSH_AXES, CTX_AXES], 1)
    normed_flat = normed_flat.reshape(group_tokens, width)
    qkv_full = qkv_full.reshape(width, q_cols + 2 * kv_cols)
    out_full = lax.all_gather(out_weight.T, "ctx", axis=0, tiled=True)
    cot_low, qkv_full = lax.optimization_barrier((cot_flat.astype(bf16), qkv_full))
    cot_all = lax.all_gather(cot_low, ("ctx", "wsh"), axis=0)
    projected = jnp.dot(normed_flat, qkv_full, preferred_element_type=f32)
    kv_own = kv_prep(projected, key_gain, cos2, sin2, heads_loc, wsh_count, seq_count)
    (kv_all,) = gather([kv_own], [CTX_AXES], 3)

    attention, log_total, rotated = attend(
        projected, kv_all, query_gain, cos2, sin2, loc, own_blocks, heads_loc, wsh_count, seq_count
    )
    mixed = jnp.einsum("tc,dc->td", attention, out_full, preferred_element_type=f32)
    (mixed,) = scatter([mixed.astype(bf16).reshape(wsh_count, tokens, width)], [WSH_AXES], 4)
    residual = inputs_f + mixed

    def rows_first(value):
        return value.reshape(seq_count, rows_dev, width).transpose(1, 0, 2)

    moe_normed_f, inverse_two = rms_forward(residual, moe_gain)
    moe_flat = moe_normed_f.astype(bf16)
    (moe_all,) = gather([moe_flat], [ALL_AXES], 5)
    logits = jnp.dot(moe_flat, router, preferred_element_type=f32)
    route_ids = expert_ids.transpose(1, 0, 2).reshape(tokens, top_count)
    slots = dispatch_slot.transpose(1, 0, 2).reshape(tokens, top_count)
    expert_onehot = (
        route_ids[:, :, None] == jnp.arange(expert_count, dtype=jnp.int32)[None, None, :]
    )
    named = jnp.any(expert_onehot, axis=1)
    slot_dense = jnp.sum(jnp.where(expert_onehot, slots[:, :, None] + 1, 0), axis=1) - 1
    chosen_top = jnp.max(jnp.where(named, logits, MASKED), axis=-1, keepdims=True)
    chosen_exp = jnp.where(named, jnp.exp(jnp.where(named, logits - chosen_top, 0.0)), 0.0)
    weight_dense = chosen_exp / jnp.sum(chosen_exp, axis=-1, keepdims=True)
    routing = exchange(jnp.stack([slot_dense.astype(f32).T, weight_dense.T], axis=1))
    slot_mine = routing[:, 0, :].astype(jnp.int32)
    weight_mine = routing[:, 1, :]
    gate_w, up_w, down_w = (expert_gate[0], expert_up[0], expert_down[0])
    if capacity % 16 == 0:
        rows_in, route_cot, activation, gate_cot, up_cot, out_parts, row_parts, cot_mine = (
            expert_pass(
                slot_mine[:, None],
                weight_mine[:, None],
                moe_all,
                cot_all,
                gate_w,
                up_w,
                down_w,
                capacity,
                8,
            )
        )
        cot_mine = cot_mine[:, 0]
        gate_grad, up_grad = column_products(rows_in, [gate_cot, up_cot], 256)
        (down_grad,) = column_products(activation, [route_cot], 256)
    else:
        out_parts, cot_mine, row_parts, gate_grad, up_grad, down_grad = experts_plain(
            slot_mine, weight_mine, moe_all, cot_all, gate_w, up_w, down_w, capacity
        )
    weight_cot = exchange(cot_mine).T

    chosen_cot = weight_dense * (
        weight_cot - jnp.sum(weight_dense * weight_cot, axis=-1, keepdims=True)
    )
    out_parts, gate_grad, up_grad = lax.optimization_barrier((out_parts, gate_grad, up_grad))
    logit_cot = chosen_cot.astype(bf16)
    router_part = jnp.einsum("te,td->ed", logit_cot, moe_flat, preferred_element_type=f32)
    if own_kernels():
        row_sum, moe_sum, router_sum = scatter(
            [row_parts, out_parts, router_part.reshape(device_count, -1, 128)],
            [ALL_AXES, ALL_AXES, ALL_AXES],
            6,
        )
    else:
        row_sum, moe_sum = scatter([row_parts, out_parts], [ALL_AXES, ALL_AXES], 6)
        router_grad = lax.psum(router_part, ("ctx", "wsh")).T
    outputs = rows_first((residual + moe_sum).astype(bf16))
    normed_two_cot = (
        jnp.einsum("te,de->td", logit_cot, router, preferred_element_type=f32) + row_sum
    )
    residual_norm_cot, moe_gain_grad = rms_backward(
        residual, inverse_two, moe_gain, normed_two_cot
    )
    residual_cot = cot_flat + residual_norm_cot
    residual_low = residual_cot.astype(bf16)
    (residual_flat,) = gather([residual_low], [WSH_AXES], 8)
    residual_flat = residual_flat.reshape(group_tokens, width)

    out_grad = jnp.einsum("td,tc->dc", residual_flat, attention, preferred_element_type=f32).astype(
        bf16
    )
    out_weight_grad = lax.psum_scatter(out_grad, "ctx", scatter_dimension=0, tiled=True)
    out_weight_grad = out_weight_grad.astype(f32).T
    residual_flat, _ = lax.optimization_barrier((residual_flat, out_grad))
    attention_cot = jnp.einsum(
        "td,dc->tc", residual_flat, out_full, preferred_element_type=f32
    ).astype(bf16)
    low, kv_sums, query_gain_grad = attend_back(
        projected,
        kv_all,
        rotated,
        attention,
        attention_cot,
        log_total,
        query_gain,
        cos2,
        sin2,
        loc,
        own_blocks,
        heads_loc,
        wsh_count,
        seq_count,
    )
    kv_sums, down_grad = lax.optimization_barrier((kv_sums, down_grad))
    (kv_cot,) = scatter([kv_sums], [CTX_AXES], 9)
    low, key_gain_grad = kv_back(
        projected, kv_cot, key_gain, cos2, sin2, low, heads_loc, wsh_count, seq_count
    )
    summed = jnp.einsum("tq,cq->tc", low, qkv_full, preferred_element_type=f32)
    qkv_grad = jnp.einsum("tc,tq->cq", normed_flat, low, preferred_element_type=f32).astype(bf16)
    last_parts = [
        summed.astype(bf16).reshape(wsh_count, tokens, width),
        qkv_grad.reshape(ctx_count, width // ctx_count, q_cols + 2 * kv_cols),
    ]
    if own_kernels():
        normed_cot, qkv_grad, router_all = transfer(
            ["scatter", "scatter", "gather"],
            last_parts + [router_sum],
            [WSH_AXES, CTX_AXES, ALL_AXES],
            10,
        )
        router_grad = router_all.reshape(expert_count, width).T
    else:
        normed_cot, qkv_grad = scatter(last_parts, [WSH_AXES, CTX_AXES], 10)
    input_norm_cot, norm_gain_grad = rms_backward(inputs_f, inverse_one, norm_gain, normed_cot)
    input_grad = rows_first(residual_cot + input_norm_cot)
    query_gain_grad = query_gain_grad.reshape(head_dim)
    key_gain_grad = key_gain_grad.reshape(head_dim)
    gains = jnp.concatenate([norm_gain_grad, moe_gain_grad, query_gain_grad, key_gain_grad])
    gains = jnp.sum(to_everyone(gains, device_count), axis=0)
    return (
        outputs,
        input_grad,
        gains[:width],
        qkv_grad[:, :q_cols],
        qkv_grad[:, q_cols : q_cols + kv_cols],
        qkv_grad[:, q_cols + kv_cols :],
        gains[2 * width : 2 * width + head_dim],
        gains[2 * width + head_dim :],
        out_weight_grad,
        gains[width : 2 * width],
        router_grad,
        gate_grad,
        up_grad,
        down_grad,
    )


def solution(mesh):
    return jax.shard_map(
        local,
        mesh=mesh,
        in_specs=(
            P(("ctx", "wsh"), None, None),
            P(),
            P(),
            P("ctx", "wsh"),
            P("ctx", "wsh"),
            P("ctx", "wsh"),
            P(),
            P(),
            P("wsh", "ctx"),
            P(),
            P(),
            P(("ctx", "wsh"), None, None),
            P(("ctx", "wsh"), None, None),
            P(("ctx", "wsh"), None, None),
            P(("ctx", "wsh"), None, None),
            P(("ctx", "wsh"), None, None),
            P(("ctx", "wsh"), None, None),
        ),
        out_specs=(
            P(("ctx", "wsh"), None, None),
            P(("ctx", "wsh"), None, None),
            P(),
            P("ctx", "wsh"),
            P("ctx", "wsh"),
            P("ctx", "wsh"),
            P(),
            P(),
            P("wsh", "ctx"),
            P(),
            P(),
            P(("ctx", "wsh"), None, None),
            P(("ctx", "wsh"), None, None),
            P(("ctx", "wsh"), None, None),
        ),
        check_vma=False,
    )
```

```python
import functools
import math

import jax
import jax.numpy as jnp
from jax import lax
from jax.experimental import pallas as pl
from jax.experimental.pallas import tpu as pltpu
from jax.sharding import PartitionSpec as P


EPSILON = 1e-06
ROPE_BASE = 1000000.0
MASKED = -1e30


def positions_of(pair_map, seq_len, block_len, group_count):
    row_index = jnp.arange(seq_len, dtype=jnp.int32)
    owner_group = row_index // (2 * block_len)
    inner_row = row_index % (2 * block_len)
    group_table = jnp.arange(group_count, dtype=jnp.int32)
    pair_index = jnp.sum(
        jnp.where(owner_group[:, None] == group_table[None, :], pair_map[None, :], 0), axis=1
    )
    block_index = jnp.where(inner_row < block_len, pair_index, 2 * group_count - 1 - pair_index)
    return block_index * block_len + inner_row % block_len


def rope_tables(positions, head_dim):
    half_dim = head_dim // 2
    frequency = ROPE_BASE ** (-(jnp.arange(half_dim, dtype=jnp.float32) * 2.0) / head_dim)
    angles = positions.astype(jnp.float32)[:, None] * frequency[None, :]
    return (jnp.cos(angles), jnp.sin(angles))


def rms_forward(tensor, gain_vector):
    inverse = lax.rsqrt(jnp.mean(tensor * tensor, axis=-1, keepdims=True) + EPSILON)
    return (tensor * inverse * gain_vector, inverse)


def rms_backward(tensor, inverse, gain_vector, gradient):
    weighted = gradient * gain_vector
    inner_mean = jnp.mean(weighted * tensor, axis=-1, keepdims=True)
    tensor_grad = inverse * weighted - tensor * inverse**3 * inner_mean
    gain_grad = jnp.sum((gradient * tensor * inverse).reshape(-1, tensor.shape[-1]), axis=0)
    return (tensor_grad, gain_grad)


MESH_ID = pl.DeviceIdType.MESH


class Place:
    def __init__(self, nz, ux, uy, uc):
        ci, wi = lax.axis_index("ctx"), lax.axis_index("wsh")
        self.nz, self.ux, self.uy, self.uc = nz, ux, uy, uc
        self.z, self.x, self.y, self.c = ci // 2, ci % 2, wi // 2, wi % 2

    def dev(self, z, x, y, c):
        return (z * 2 + x, y * 2 + c)

    def blk(self, z, x, y, c):
        if self.ux and self.uc:
            return (z * 2 + x) * 4 + y * 2 + c
        if self.ux:
            return z * 2 + x
        return y * 2 + c

    def greet(self):
        z, x, y, c, nz = self.z, self.x, self.y, self.c, self.nz
        barrier = pltpu.get_barrier_semaphore()
        count = 0
        if nz > 1:
            for step in (-1, 1):
                ok = jnp.logical_and(z + step >= 0, z + step < nz)

                @pl.when(ok)
                def _():
                    pl.semaphore_signal(
                        barrier, inc=1, device_id=self.dev(z + step, x, y, c), device_id_type=MESH_ID
                    )

                count = count + ok.astype(jnp.int32)
        for use, place in (
            (self.ux, (z, 1 - x, y, c)),
            (self.uy, (z, x, 1 - y, c)),
            (self.uc, (z, x, y, 1 - c)),
        ):
            if use:
                pl.semaphore_signal(
                    barrier, inc=1, device_id=self.dev(*place), device_id_type=MESH_ID
                )
                count = count + 1
        pl.semaphore_wait(barrier, count)

    def line_steps(self):
        steps = [(0, 0, self.z, None)]
        for d in range(1, self.nz):
            steps.append((d, 0, self.z - d, self.z - d >= 0))
            steps.append((d, 1, self.z + d, self.z + d < self.nz))
        return steps


def both(a, b):
    if a is None or b is None:
        return a if b is None else b
    return a.astype(jnp.int32) * b.astype(jnp.int32) > 0


def when(cond, fn):
    if cond is None:
        fn()
    else:
        pl.when(cond)(fn)


def gather_line_first(axes, lo, rows, x_ref, o_ref, ssem, rsem):
    nz, ux, uy, uc = axes
    pc = Place(nz, ux, uy, uc)
    z, x, y, c = pc.z, pc.x, pc.y, pc.c
    half = rows // 2
    x_ref = x_ref.at[pl.ds(lo, rows)]
    to_x, to_y, to_c = pc.dev(z, 1 - x, y, c), pc.dev(z, x, 1 - y, c), pc.dev(z, x, y, 1 - c)

    def part(b, p):
        if p == 0:
            return o_ref.at[b, pl.ds(lo, rows)]
        return o_ref.at[b, pl.ds(lo + (p - 1) * half, half)]

    def sid(d, side, kind):
        return (d * 2 + side) * 10 + kind

    def copy(b, p, sidx, ridx, device, src=None):
        return pltpu.make_async_remote_copy(
            src_ref=part(b, p) if src is None else src,
            dst_ref=part(b, p),
            send_sem=ssem.at[sidx],
            recv_sem=rsem.at[ridx],
            device_id=device,
            device_id_type=MESH_ID,
        )

    def hops(d, side, s):
        out = []
        if nz > 1:
            b = pc.blk(s, x, y, c)
            src = x_ref if d == 0 else None
            if d == 0 or side == 0:
                if d + 1 < nz:
                    out.append(
                        (z + 1 < nz, copy(b, 0, sid(d, 0, 0), sid(d + 1, 0, 0), pc.dev(z + 1, x, y, c), src))
                    )
            if d == 0 or side == 1:
                if d + 1 < nz:
                    out.append(
                        (z >= 1, copy(b, 0, sid(d, 1, 0), sid(d + 1, 1, 0), pc.dev(z - 1, x, y, c), src))
                    )
        return out

    def spread(d, side, s):
        b = pc.blk(s, x, y, c)
        src = x_ref if d == 0 else None
        out = []
        if ux:
            out.append(copy(b, 0, sid(d, side, 1), sid(d, side, 1), to_x, src))
        if uy:
            out.append(copy(b, 0, sid(d, side, 2), sid(d, side, 2), to_y, src))
        if uc:
            out.append(copy(b, 0, sid(d, side, 5), sid(d, side, 5), to_c, src))
        return out

    def passed(d, side, s):
        out = []
        if ux:
            b = pc.blk(s, 1 - x, y, c)
            arrive = copy(b, 0, sid(d, side, 1), sid(d, side, 1), to_x)
            go = []
            if uy:
                go.append(copy(b, 1, sid(d, side, 3), sid(d, side, 3), to_y))
            if uc:
                go.append(copy(b, 0, sid(d, side, 6), sid(d, side, 6), to_c))
            out.append((arrive, go))
        if uy:
            b = pc.blk(s, x, 1 - y, c)
            arrive = copy(b, 0, sid(d, side, 2), sid(d, side, 2), to_y)
            go = []
            if ux:
                go.append(copy(b, 2, sid(d, side, 4), sid(d, side, 4), to_x))
            if uc:
                go.append(copy(b, 0, sid(d, side, 7), sid(d, side, 7), to_c))
            out.append((arrive, go))
        return out

    def across(d, side, s):
        out = []
        if ux and uy:
            b = pc.blk(s, 1 - x, 1 - y, c)
            arrive = copy(b, 1, sid(d, side, 3), sid(d, side, 3), to_y)
            go = [copy(b, 1, sid(d, side, 8), sid(d, side, 8), to_c)] if uc else []
            out.append((arrive, go))
            arrive = copy(b, 2, sid(d, side, 4), sid(d, side, 4), to_x)
            go = [copy(b, 2, sid(d, side, 9), sid(d, side, 9), to_c)] if uc else []
            out.append((arrive, go))
        return out

    def partner(d, side, s):
        out = []
        if uc:
            out.append(copy(pc.blk(s, x, y, 1 - c), 0, 0, sid(d, side, 5), to_c))
            if ux:
                out.append(copy(pc.blk(s, 1 - x, y, 1 - c), 0, 0, sid(d, side, 6), to_c))
            if uy:
                out.append(copy(pc.blk(s, x, 1 - y, 1 - c), 0, 0, sid(d, side, 7), to_c))
            if ux and uy:
                b = pc.blk(s, 1 - x, 1 - y, 1 - c)
                out.append(copy(b, 1, 0, sid(d, side, 8), to_c))
                out.append(copy(b, 2, 0, sid(d, side, 9), to_c))
        return out

    steps = pc.line_steps()

    def do_line(step):
        d, side, s, ok = step

        def fn():
            if d > 0:
                copy(pc.blk(s, x, y, c), 0, 0, sid(d, side, 0), to_x).wait_recv()
            for cond, cp in hops(d, side, s):
                when(cond, cp.start)
            for cp in spread(d, side, s):
                cp.start()

        when(ok, fn)

    def do_pass(step, which):
        d, side, s, ok = step

        def fn():
            for arrive, go in which(d, side, s):
                arrive.wait_recv()
                for cp in go:
                    cp.start()

        when(ok, fn)

    groups = [[st for st in steps if st[0] == d] for d in range(nz)]

    def phase(t):
        if t < nz:
            for st in groups[t]:
                do_line(st)
        if 0 <= t - 1 < nz:
            for st in groups[t - 1]:
                do_pass(st, passed)
        if 0 <= t - 2 < nz:
            for st in groups[t - 2]:
                do_pass(st, across)

    def last():
        for st in steps:
            d, side, s, ok = st

            def fn():
                for cp in partner(d, side, s):
                    cp.wait_recv()
                for cond, cp in hops(d, side, s):
                    when(cond, cp.wait_send)
                for cp in spread(d, side, s):
                    cp.wait_send()
                for which in (passed, across):
                    for _, go in which(d, side, s):
                        for cp in go:
                            cp.wait_send()

            when(ok, fn)

    return lambda: None, [functools.partial(phase, t) for t in range(nz + 2)], last


def gather_plane_first(axes, lo, rows, x_ref, o_ref, ssem, rsem):
    nz, ux, uy, uc = axes
    pc = Place(nz, ux, uy, uc)
    z, x, y, c = pc.z, pc.x, pc.y, pc.c
    half = rows // 2
    own = x_ref.at[pl.ds(lo, rows)]
    to_x, to_y, to_c = pc.dev(z, 1 - x, y, c), pc.dev(z, x, 1 - y, c), pc.dev(z, x, y, 1 - c)
    items = [(0, 0, x, y, (lo, rows))]
    if ux:
        items.append((1, 1, 1 - x, y, (lo, rows)))
    if uy:
        items.append((2, 1, x, 1 - y, (lo, rows)))
    if ux and uy:
        items.append((3, 2, 1 - x, 1 - y, (lo, half)))
        items.append((4, 2, 1 - x, 1 - y, (lo + half, half)))
    per = 5
    base = nz * 2 * per

    def iid(d, side, item):
        return (d * 2 + side) * per + item

    def copy(s, px, py, core, span, sidx, ridx, device, src=None):
        ref = o_ref.at[pc.blk(s, px, py, core), pl.ds(span[0], span[1])]
        return pltpu.make_async_remote_copy(
            src_ref=ref if src is None else src,
            dst_ref=ref,
            send_sem=ssem.at[sidx],
            recv_sem=rsem.at[ridx],
            device_id=device,
            device_id_type=MESH_ID,
        )

    def arrival(d, side, s, it):
        item, _, px, py, span = it
        return copy(s, px, py, c, span, 0, iid(d, side, item), to_x)

    def outgoing(d, side, s, it):
        item, _, px, py, span = it
        src = own if d == 0 and item == 0 else None
        out = []
        if d + 1 < nz:
            if d == 0 or side == 0:
                out.append(
                    (
                        z + 1 < nz,
                        copy(s, px, py, c, span, iid(d, 0, item), iid(d + 1, 0, item), pc.dev(z + 1, x, y, c), src),
                    )
                )
            if d == 0 or side == 1:
                out.append(
                    (
                        z >= 1,
                        copy(s, px, py, c, span, iid(d, 1, item), iid(d + 1, 1, item), pc.dev(z - 1, x, y, c), src),
                    )
                )
        if uc:
            at = base + iid(d, side, item)
            out.append((None, copy(s, px, py, c, span, at, at, to_c, src)))
        if d == 0:
            if item == 0 and ux:
                out.append((None, copy(s, px, py, c, span, 2 * base, iid(0, 0, 1), to_x, src)))
            if item == 0 and uy:
                out.append((None, copy(s, px, py, c, span, 2 * base + 1, iid(0, 0, 2), to_y, src)))
            if item == 1 and uy:
                out.append(
                    (None, copy(s, px, py, c, (lo, half), 2 * base + 2, iid(0, 0, 3), to_y))
                )
            if item == 2 and ux:
                out.append(
                    (None, copy(s, px, py, c, (lo + half, half), 2 * base + 3, iid(0, 0, 4), to_x))
                )
        return out

    steps = pc.line_steps()

    def phase(t):
        for d, side, s, ok in steps:
            for it in items:
                if d + it[1] != t:
                    continue

                if d > 0 or it[0] > 0:
                    when(ok, arrival(d, side, s, it).wait_recv)
                for cond, cp in outgoing(d, side, s, it):
                    when(both(ok, cond), cp.start)

    def last():
        for d, side, s, ok in steps:

            for it in items:
                if uc:
                    item, _, px, py, span = it
                    there = copy(s, px, py, 1 - c, span, 0, base + iid(d, side, item), to_c)
                    when(ok, there.wait_recv)
                for cond, cp in outgoing(d, side, s, it):
                    when(both(ok, cond), cp.wait_send)

    return lambda: None, [functools.partial(phase, t) for t in range(nz + 2)], last


WSH_AXES = (1, False, True, True)
CTX_AXES = (4, True, False, False)
ALL_AXES = (4, True, True, True)


def spans_of(axes, rows):
    if axes[0] == 1 or rows % 128:
        return rows, 0
    second = rows // 4 if axes[3] else rows // 8
    return rows - second, second


def run_jobs(axes_list, jobs):
    Place(
        max(a[0] for a in axes_list),
        any(a[1] for a in axes_list),
        any(a[2] for a in axes_list),
        any(a[3] for a in axes_list),
    ).greet()
    for begin, _, _ in jobs:
        begin()
    for t in range(max(len(phases) for _, phases, _ in jobs)):
        for _, phases, _ in jobs:
            if t < len(phases):
                phases[t]()
    for _, _, last in jobs:
        last()


def group_of(axes):
    return (axes[0] * 2 if axes[1] else 1) * (4 if axes[3] else 1)


GATHER_REFS, SCATTER_REFS = 5, 20


def gather_scratch(axes):
    dma = pltpu.SemaphoreType.DMA
    nz = axes[0]
    return [dma((nz * 20,)), dma((nz * 20,)), dma((nz * 20 + 4,)), dma((nz * 20,)), dma]


def gather_jobs(axes, x_ref, o_ref, s1, r1, s2, r2, lsem):
    pc = Place(*axes)
    rows = x_ref.shape[0]
    main, rest = spans_of(axes, rows)
    own = pltpu.make_async_copy(x_ref, o_ref.at[pc.blk(pc.z, pc.x, pc.y, pc.c)], lsem)
    _, phases, last = gather_line_first(axes, 0, main, x_ref, o_ref, s1, r1)

    def end():
        last()
        own.wait()

    jobs = [(own.start, phases, end)]
    if rest:
        jobs.append(gather_plane_first(axes, main, rest, x_ref, o_ref, s2, r2))
    return jobs


def scatter_scratch(axes, shape, dt):
    rows, cols = shape
    nz, ux, uy, uc = axes
    dma = pltpu.SemaphoreType.DMA
    out = []
    for second, n in enumerate(spans_of(axes, rows)):
        few = lambda use, k, r: pltpu.VMEM((k, r, cols) if use and n else (1, 16, cols), dt)
        lines = 1 if second else nz
        out += [
            few(True, nz * 4, n),
            few(uc, nz * 4, n),
            few(ux, lines, n),
            few(uy, lines, n),
            few(ux and uy, lines, n // 2),
            few(ux and uy, lines, n // 2),
            few(nz > 1, (nz + 1) * (4 if second else 1), n),
            dma((nz * (14 if second else 12),)),
            dma((nz * (18 if second else 12),)),
            dma((nz * 4,)),
        ]
    return out


def scatter_jobs(axes, p_ref, o_ref, *refs):
    rows = o_ref.shape[0]
    main, rest = spans_of(axes, rows)
    jobs = [scatter_line_last(axes, 0, main, p_ref, o_ref, *refs[:10])]
    if rest:
        jobs.append(scatter_line_first(axes, main, rest, p_ref, o_ref, *refs[10:]))
    return jobs


def transfer_kernel(kinds, axes_list, *refs):
    n = len(kinds)
    at = 2 * n
    jobs = []
    for i, (kind, axes) in enumerate(zip(kinds, axes_list)):
        many = GATHER_REFS if kind == "gather" else SCATTER_REFS
        make = gather_jobs if kind == "gather" else scatter_jobs
        jobs += make(axes, refs[i], refs[n + i], *refs[at : at + many])
        at += many
    run_jobs(axes_list, jobs)


def transfer(kinds, values, axes_list, collective_id):
    shapes, specs, scratch = [], [], []
    for kind, value, axes in zip(kinds, values, axes_list):
        if kind == "gather":
            shapes.append(jax.ShapeDtypeStruct((group_of(axes),) + value.shape, value.dtype))
            specs.append(pl.BlockSpec(memory_space=pl.ANY))
            scratch += gather_scratch(axes)
        else:
            shapes.append(jax.ShapeDtypeStruct(value.shape[1:], jnp.float32))
            specs.append(pl.BlockSpec(memory_space=pltpu.VMEM))
            scratch += scatter_scratch(axes, value.shape[1:], value.dtype)
    return pl.pallas_call(
        functools.partial(transfer_kernel, kinds, axes_list),
        out_shape=shapes,
        in_specs=[pl.BlockSpec(memory_space=pl.ANY)] * len(values),
        out_specs=specs,
        scratch_shapes=scratch,
        compiler_params=pltpu.CompilerParams(
            collective_id=collective_id, has_side_effects=True, vmem_limit_bytes=61 * 1024 * 1024
        ),
    )(*values)


def scatter_line_last(axes, lo, rows, p_ref, o_ref, acc, rc, rx, ry, ra, rb, rz, ssem, rsem, lsem):
    nz, ux, uy, uc = axes
    pc = Place(nz, ux, uy, uc)
    z, x, y, c = pc.z, pc.x, pc.y, pc.c
    half = rows // 2
    chunk = math.gcd(half, 32)
    f32 = jnp.float32
    to_x, to_y, to_c = pc.dev(z, 1 - x, y, c), pc.dev(z, x, 1 - y, c), pc.dev(z, x, y, 1 - c)
    rels = [(0, x, y)]
    if ux:
        rels.append((1, 1 - x, y))
    if uy:
        rels.append((2, x, 1 - y))
    if ux and uy:
        rels.append((3, 1 - x, 1 - y))
    KINDS = 12

    def slot(s):
        return s if nz > 1 else 0

    def sid(s, kind):
        return slot(s) * KINDS + kind

    def hf(ref, h):
        return ref.at[pl.ds(h * half, half)]

    def rcopy(src, dst, s, kind, device):
        return pltpu.make_async_remote_copy(
            src_ref=src,
            dst_ref=dst,
            send_sem=ssem.at[sid(s, kind)],
            recv_sem=rsem.at[sid(s, kind)],
            device_id=device,
            device_id_type=MESH_ID,
        )

    def load(s, rel, px, py):
        return pltpu.make_async_copy(
            p_ref.at[pc.blk(s, px, py, c), pl.ds(lo, rows)], acc.at[slot(s) * 4 + rel], lsem.at[slot(s) * 4 + rel]
        )

    def give(s, rel, px, py):
        return rcopy(
            p_ref.at[pc.blk(s, px, py, 1 - c), pl.ds(lo, rows)], rc.at[slot(s) * 4 + rel], s, rel, to_c
        )

    def fold(dst, lo, n, srcs):
        def body(i, _):
            r = pl.multiple_of(i * chunk, chunk)
            total = dst[pl.ds(lo + r, chunk), :].astype(f32)
            for ref, at in srcs:
                total = total + ref[pl.ds(at + r, chunk), :].astype(f32)
            dst[pl.ds(lo + r, chunk), :] = total.astype(dst.dtype)
            return 0

        lax.fori_loop(0, n // chunk, body, 0)

    def over_a(s):
        return rcopy(hf(acc.at[slot(s) * 4 + 3], 0), ra.at[slot(s)], s, 4, to_y)

    def over_b(s):
        return rcopy(hf(acc.at[slot(s) * 4 + 3], 1), rb.at[slot(s)], s, 5, to_x)

    def x_half(s, h):
        return rcopy(hf(acc.at[slot(s) * 4 + 1], h), hf(rx.at[slot(s)], h), s, 6 + h, to_x)

    def y_half(s, h):
        return rcopy(hf(acc.at[slot(s) * 4 + 2], h), hf(ry.at[slot(s)], h), s, 8 + h, to_y)

    def z_send(s, up):
        return rcopy(
            acc.at[slot(s) * 4],
            rz.at[slot(s)],
            s,
            10,
            pc.dev(z + (1 if up else -1), x, y, c),
        )

    def z_last(s, up):
        return pltpu.make_async_remote_copy(
            src_ref=acc.at[slot(s) * 4],
            dst_ref=rz.at[slot(s)] if up else rz.at[nz],
            send_sem=ssem.at[sid(s, 10)],
            recv_sem=rsem.at[sid(s, 10)] if up else rsem.at[sid(s, 11)],
            device_id=pc.dev(z + (1 if up else -1), x, y, c),
            device_id_type=MESH_ID,
        )

    steps = list(reversed(pc.line_steps()))

    def begin():
        for d, side, s, ok in steps:

            def fn():
                for rel, px, py in reversed(rels):
                    load(s, rel, px, py).start()
                    if uc:
                        give(s, rel, px, py).start()

            when(ok, fn)

    def first(step):
        _, _, s, ok = step

        def fn():
            for rel, px, py in reversed(rels):
                load(s, rel, px, py).wait()
                if uc:
                    give(s, rel, px, py).wait_recv()
                    fold(acc.at[slot(s) * 4 + rel], 0, rows, [(rc.at[slot(s) * 4 + rel], 0)])
                if rel == 3:
                    over_a(s).start()
                    over_b(s).start()
                if rel == 2:
                    y_half(s, 0).start()
                    if not ux:
                        y_half(s, 1).start()
                if rel == 1:
                    x_half(s, 1).start()
                    if not uy:
                        x_half(s, 0).start()

        when(ok, fn)

    def second(step):
        _, _, s, ok = step

        def fn():
            if ux and uy:
                over_a(s).wait_recv()
                fold(acc.at[slot(s) * 4 + 1], 0, half, [(ra.at[slot(s)], 0)])
                x_half(s, 0).start()
                over_b(s).wait_recv()
                fold(acc.at[slot(s) * 4 + 2], half, half, [(rb.at[slot(s)], 0)])
                y_half(s, 1).start()

        when(ok, fn)

    def third(step):
        d, side, s, ok = step

        def fn():
            srcs = []
            if ux:
                x_half(s, 0).wait_recv()
                x_half(s, 1).wait_recv()
                srcs.append((rx.at[slot(s)], 0))
            if uy:
                y_half(s, 0).wait_recv()
                y_half(s, 1).wait_recv()
                srcs.append((ry.at[slot(s)], 0))
            if d > 0:
                more = (z + 1 < nz) if side == 0 else (z >= 1)

                @pl.when(more)
                def _():
                    z_send(s, side == 1).wait_recv()
                    fold(acc.at[slot(s) * 4], 0, rows, srcs + [(rz.at[slot(s)], 0)])

                if srcs:

                    @pl.when(jnp.logical_not(more))
                    def _():
                        fold(acc.at[slot(s) * 4], 0, rows, srcs)

                if d == 1:
                    z_last(s, side == 1).start()
                else:
                    z_send(s, side == 1).start()
            else:

                def body(use_lo, use_hi):
                    terms = list(srcs)
                    if use_lo:
                        z_last(s, True).wait_recv()
                        terms.append((rz.at[slot(s)], 0))
                    if use_hi:
                        z_last(s, False).wait_recv()
                        terms.append((rz.at[nz], 0))

                    def step_(i, _):
                        r = pl.multiple_of(i * chunk, chunk)
                        total = acc[slot(s) * 4, pl.ds(r, chunk), :].astype(f32)
                        for ref, at in terms:
                            total = total + ref[pl.ds(at + r, chunk), :].astype(f32)
                        o_ref[pl.ds(pl.multiple_of(lo + i * chunk, chunk), chunk), :] = total.astype(
                            o_ref.dtype
                        )
                        return 0

                    lax.fori_loop(0, rows // chunk, step_, 0)

                if nz == 1:
                    body(False, False)
                else:
                    pl.when(jnp.logical_and(z >= 1, z + 1 < nz))(lambda: body(True, True))
                    pl.when(z == nz - 1)(lambda: body(True, False))
                    pl.when(z == 0)(lambda: body(False, True))

        when(ok, fn)

    groups = [[st for st in steps if st[0] == d] for d in reversed(range(nz))]

    def phase(t):
        if t < nz:
            for st in groups[t]:
                first(st)
        if 0 <= t - 1 < nz:
            for st in groups[t - 1]:
                second(st)
        if 0 <= t - 2 < nz:
            for st in groups[t - 2]:
                third(st)

    def last():
        for d, side, s, ok in steps:

            def fn():
                for rel, px, py in rels:
                    if uc:
                        give(s, rel, px, py).wait_send()
                if ux and uy:
                    over_a(s).wait_send()
                    over_b(s).wait_send()
                if ux:
                    x_half(s, 0).wait_send()
                    x_half(s, 1).wait_send()
                if uy:
                    y_half(s, 0).wait_send()
                    y_half(s, 1).wait_send()
                if d > 0:
                    z_send(s, side == 1).wait_send()

            when(ok, fn)

    return begin, [functools.partial(phase, t) for t in range(nz + 2)], last


def scatter_line_first(axes, lo, rows, p_ref, o_ref, acc, rc, rx, ry, ra, rb, rz, ssem, rsem, lsem):
    nz, ux, uy, uc = axes
    pc = Place(nz, ux, uy, uc)
    z, x, y, c = pc.z, pc.x, pc.y, pc.c
    half = rows // 2
    chunk = math.gcd(half, 32)
    f32 = jnp.float32
    to_x, to_y, to_c = pc.dev(z, 1 - x, y, c), pc.dev(z, x, 1 - y, c), pc.dev(z, x, y, 1 - c)
    rels = [(0, x, y)]
    if ux:
        rels.append((1, 1 - x, y))
    if uy:
        rels.append((2, x, 1 - y))
    if ux and uy:
        rels.append((3, 1 - x, 1 - y))
    plane = nz * 4 * 3

    def hf(ref, h):
        return ref.at[pl.ds(h * half, half)]

    def rcopy(src, dst, sidx, ridx, device):
        return pltpu.make_async_remote_copy(
            src_ref=src,
            dst_ref=dst,
            send_sem=ssem.at[sidx],
            recv_sem=rsem.at[ridx],
            device_id=device,
            device_id_type=MESH_ID,
        )

    def load(s, rel, px, py):
        return pltpu.make_async_copy(
            p_ref.at[pc.blk(s, px, py, c), pl.ds(lo, rows)], acc.at[s * 4 + rel], lsem.at[s * 4 + rel]
        )

    def give(s, rel, px, py):
        at = s * 4 + rel
        return rcopy(p_ref.at[pc.blk(s, px, py, 1 - c), pl.ds(lo, rows)], rc.at[at], at, at, to_c)

    def hop(s, rel, up, final):
        extra = final and not up
        return rcopy(
            acc.at[s * 4 + rel],
            rz.at[nz * 4 + rel] if extra else rz.at[s * 4 + rel],
            nz * 4 + s * 4 + rel,
            (nz * 8 + s * 4 + rel) if extra else (nz * 4 + s * 4 + rel),
            pc.dev(z + (1 if up else -1), x, y, c),
        )

    def fold(dst, at, n, srcs):
        def body(i, _):
            r = pl.multiple_of(i * chunk, chunk)
            total = dst[pl.ds(pl.multiple_of(at + r, chunk), chunk), :].astype(f32)
            for ref, first in srcs:
                total = total + ref[pl.ds(pl.multiple_of(first + r, chunk), chunk), :].astype(f32)
            dst[pl.ds(pl.multiple_of(at + r, chunk), chunk), :] = total.astype(dst.dtype)
            return 0

        lax.fori_loop(0, n // chunk, body, 0)

    def mine(rel):
        return acc.at[z * 4 + rel]

    def over_a():
        return rcopy(hf(mine(3), 0), ra.at[0], nz * 8, plane, to_y)

    def over_b():
        return rcopy(hf(mine(3), 1), rb.at[0], nz * 8 + 1, plane + 1, to_x)

    def x_half(h):
        return rcopy(hf(mine(1), h), hf(rx.at[0], h), nz * 8 + 2 + h, plane + 2 + h, to_x)

    def y_half(h):
        return rcopy(hf(mine(2), h), hf(ry.at[0], h), nz * 8 + 4 + h, plane + 4 + h, to_y)

    steps = list(reversed(pc.line_steps()))

    def begin():
        for d, side, s, ok in steps:

            def fn():
                for rel, px, py in reversed(rels):
                    load(s, rel, px, py).start()
                    if uc:
                        give(s, rel, px, py).start()

            when(ok, fn)

    def line(step):
        d, side, s, ok = step

        def fn():
            more = (z + 1 < nz) if side == 0 else (z >= 1)
            for rel, px, py in reversed(rels):
                load(s, rel, px, py).wait()
                srcs = []
                if uc:
                    give(s, rel, px, py).wait_recv()
                    srcs = [(rc.at[s * 4 + rel], 0)]
                target = acc.at[s * 4 + rel]
                if d > 0:

                    @pl.when(more)
                    def _():
                        hop(s, rel, side == 1, False).wait_recv()
                        fold(target, 0, rows, srcs + [(rz.at[s * 4 + rel], 0)])

                    if srcs:

                        @pl.when(jnp.logical_not(more))
                        def _():
                            fold(target, 0, rows, srcs)

                    hop(s, rel, side == 1, d == 1).start()
                else:
                    lower, upper = (rz.at[s * 4 + rel], 0), (rz.at[nz * 4 + rel], 0)

                    @pl.when(z >= 1)
                    def _():
                        hop(s, rel, True, True).wait_recv()

                    @pl.when(z + 1 < nz)
                    def _():
                        hop(s, rel, False, True).wait_recv()

                    both = jnp.logical_and(z >= 1, z + 1 < nz)
                    pl.when(both)(lambda: fold(target, 0, rows, srcs + [lower, upper]))
                    pl.when(z == 0)(lambda: fold(target, 0, rows, srcs + [upper]))
                    pl.when(z == nz - 1)(lambda: fold(target, 0, rows, srcs + [lower]))
                    if rel == 3:
                        over_a().start()
                        over_b().start()
                    if rel == 2:
                        y_half(0).start()
                        if not ux:
                            y_half(1).start()
                    if rel == 1:
                        x_half(1).start()
                        if not uy:
                            x_half(0).start()

        when(ok, fn)

    def cross():
        if ux and uy:
            over_a().wait_recv()
            fold(mine(1), 0, half, [(ra.at[0], 0)])
            x_half(0).start()
            over_b().wait_recv()
            fold(mine(2), half, half, [(rb.at[0], 0)])
            y_half(1).start()

    def total():
        srcs = []
        if ux:
            x_half(0).wait_recv()
            x_half(1).wait_recv()
            srcs.append(rx)
        if uy:
            y_half(0).wait_recv()
            y_half(1).wait_recv()
            srcs.append(ry)

        def body(i, _):
            r = pl.multiple_of(i * chunk, chunk)
            value = acc[z * 4, pl.ds(r, chunk), :].astype(f32)
            for ref in srcs:
                value = value + ref[0, pl.ds(r, chunk), :].astype(f32)
            o_ref[pl.ds(pl.multiple_of(lo + i * chunk, chunk), chunk), :] = value.astype(o_ref.dtype)
            return 0

        lax.fori_loop(0, rows // chunk, body, 0)

    groups = [[st for st in steps if st[0] == d] for d in reversed(range(nz))]

    def phase(t):
        if t < nz:
            for st in groups[t]:
                line(st)
        elif t == nz:
            cross()
        else:
            total()

    def last():
        for d, side, s, ok in steps:

            def fn():
                for rel, px, py in rels:
                    if uc:
                        give(s, rel, px, py).wait_send()
                    if d > 0:
                        hop(s, rel, side == 1, d == 1).wait_send()

            when(ok, fn)
        if ux and uy:
            over_a().wait_send()
            over_b().wait_send()
        if ux:
            x_half(0).wait_send()
            x_half(1).wait_send()
        if uy:
            y_half(0).wait_send()
            y_half(1).wait_send()

    return begin, [functools.partial(phase, t) for t in range(nz + 2)], last


LOG2E = 1.4426950408889634


def lane_swap(tensor):
    return pltpu.roll(tensor, tensor.shape[-1] // 2, tensor.ndim - 1)


def head_norm(tensor, gain, cos2, sin2):
    inverse = lax.rsqrt(jnp.mean(tensor * tensor, axis=-1, keepdims=True) + EPSILON)
    scaled = tensor * inverse * gain
    return scaled * cos2 + lane_swap(scaled) * sin2


def head_norm_back(tensor, gain, cos2, sin2, gradient):
    inverse = lax.rsqrt(jnp.mean(tensor * tensor, axis=-1, keepdims=True) + EPSILON)
    turned = gradient * cos2 - lane_swap(gradient) * sin2
    weighted = turned * gain
    inner = jnp.mean(weighted * tensor, axis=-1, keepdims=True)
    return (
        inverse * weighted - tensor * (inverse * inverse * inverse) * inner,
        turned * tensor * inverse,
    )


def token_rows(piece, seq, seq_count, rows_dev):
    return (piece * seq_count + seq) * rows_dev


def kv_prep_kernel(pieces, seqs, proj_ref, gain_ref, cos_ref, sin_ref, o_ref):
    hd = gain_ref.shape[-1]
    rows = proj_ref.shape[0] // (pieces * seqs)
    for piece in range(pieces):
        cos2 = cos_ref[piece * rows : (piece + 1) * rows, :]
        sin2 = sin_ref[piece * rows : (piece + 1) * rows, :]
        for seq in range(seqs):
            at = token_rows(piece, seq, seqs, rows)
            raw = proj_ref[at : at + rows, :hd]
            o_ref[at : at + rows, :hd] = head_norm(raw, gain_ref[...], cos2, sin2).astype(
                o_ref.dtype
            )
            o_ref[at : at + rows, hd:] = proj_ref[at : at + rows, hd:].astype(o_ref.dtype)


def kv_prep(projected, key_gain, cos2, sin2, heads, pieces, seqs):
    rows, _ = projected.shape
    hd = key_gain.shape[0]
    whole = lambda *shape: pl.BlockSpec(shape, lambda i: (0,) * len(shape))
    return pl.pallas_call(
        functools.partial(kv_prep_kernel, pieces, seqs),
        grid=(1,),
        out_shape=jax.ShapeDtypeStruct((rows, 2 * hd), jnp.bfloat16),
        in_specs=[
            pl.BlockSpec((rows, 2 * hd), lambda i: (0, heads // 2)),
            whole(1, hd),
            whole(*cos2.shape),
            whole(*sin2.shape),
        ],
        out_specs=whole(rows, 2 * hd),
        name="kv_prep",
    )(projected, key_gain.reshape(1, hd), cos2, sin2)


def kv_back_kernel(pieces, seqs, proj_ref, cot_ref, gain_ref, cos_ref, sin_ref, _, low_ref, gg_ref):
    hd = gain_ref.shape[-1]
    rows = proj_ref.shape[0] // (pieces * seqs)
    total = jnp.zeros((1, hd), jnp.float32)
    for piece in range(pieces):
        cos2 = cos_ref[piece * rows : (piece + 1) * rows, :]
        sin2 = sin_ref[piece * rows : (piece + 1) * rows, :]
        for seq in range(seqs):
            at = token_rows(piece, seq, seqs, rows)
            grad, terms = head_norm_back(
                proj_ref[at : at + rows, :hd],
                gain_ref[...],
                cos2,
                sin2,
                cot_ref[at : at + rows, :hd],
            )
            low_ref[at : at + rows, :hd] = grad.astype(low_ref.dtype)
            low_ref[at : at + rows, hd:] = cot_ref[at : at + rows, hd:].astype(low_ref.dtype)
            total = total + jnp.sum(terms, axis=0, keepdims=True)
    gg_ref[...] = total


def kv_back(projected, kv_cot, key_gain, cos2, sin2, low, heads, pieces, seqs):
    rows, _ = projected.shape
    hd = key_gain.shape[0]
    whole = lambda *shape: pl.BlockSpec(shape, lambda i: (0,) * len(shape))
    return pl.pallas_call(
        functools.partial(kv_back_kernel, pieces, seqs),
        grid=(1,),
        out_shape=(
            jax.ShapeDtypeStruct(low.shape, low.dtype),
            jax.ShapeDtypeStruct((1, hd), jnp.float32),
        ),
        in_specs=[
            pl.BlockSpec((rows, 2 * hd), lambda i: (0, heads // 2)),
            whole(rows, 2 * hd),
            whole(1, hd),
            whole(*cos2.shape),
            whole(*sin2.shape),
            pl.BlockSpec(memory_space=pl.ANY),
        ],
        out_specs=(pl.BlockSpec((rows, 2 * hd), lambda i: (0, heads // 2)), whole(1, hd)),
        input_output_aliases={5: 0},
        name="kv_back",
    )(projected, kv_cot, key_gain.reshape(1, hd), cos2, sin2, low)


def sort_blocks(loc_ref, kv_ref, dst, seqs, rows, pieces, hd, lo, blocks):
    per_half = pieces // 2

    def body(b, _):
        loc = loc_ref[b]
        chunk, half = loc // 2, loc % 2
        for seq in range(seqs):
            for i in range(per_half):
                at = ((half * per_half + i) * seqs + seq) * rows
                dst[seq, pl.ds(b * (per_half * rows) + i * rows, rows), :] = kv_ref[
                    chunk, pl.ds(at, rows), lo : lo + hd
                ]
        return 0

    lax.fori_loop(0, blocks, body, 0)


def attend_kernel(
    heads, pieces, seqs, scale, loc_ref, own_ref, proj_ref, kv_ref, gain_ref, cos_ref, sin_ref,
    attn_ref, lse_ref, qs_ref, ks, vs, acc, tot,
):
    f32, bf16 = jnp.float32, jnp.bfloat16
    hd = gain_ref.shape[-1]
    rows = proj_ref.shape[0] // (pieces * seqs)
    per_half = pieces // 2
    block = per_half * rows
    blocks = 2 * kv_ref.shape[0]
    pair = 2 * block
    tile = heads * block
    sort_blocks(loc_ref, kv_ref, ks, seqs, rows, pieces, hd, 0, blocks)
    sort_blocks(loc_ref, kv_ref, vs, seqs, rows, pieces, hd, hd, blocks)
    for seq in range(seqs):
        for half in range(2):
            unit = seq * 2 + half
            for h in range(heads):
                for i in range(per_half):
                    piece = half * per_half + i
                    at = token_rows(piece, seq, seqs, rows)
                    turned = head_norm(
                        proj_ref[at : at + rows, h * hd : (h + 1) * hd],
                        gain_ref[...],
                        cos_ref[piece * rows : (piece + 1) * rows, :],
                        sin_ref[piece * rows : (piece + 1) * rows, :],
                    )
                    qs_ref[unit, h * block + i * rows : h * block + (i + 1) * rows, :] = (
                        turned.astype(bf16)
                    )
            acc[...] = jnp.zeros_like(acc)
            tot[...] = jnp.zeros_like(tot)
            mine = own_ref[half]

            def step(j, masked):
                keys = ks[seq, pl.ds(j * pair, pair), :]
                values = vs[seq, pl.ds(j * pair, pair), :]
                for t in range(heads * block // tile):
                    cols = slice(t * tile, (t + 1) * tile)
                    scores = lax.dot_general(
                        keys,
                        qs_ref[unit, cols, :],
                        (((1,), (1,)), ((), ())),
                        preferred_element_type=f32,
                    )
                    expo = jnp.exp2(scores * (scale * LOG2E))
                    if masked:
                        key_pos = j * pair + lax.broadcasted_iota(jnp.int32, expo.shape, 0)
                        query_pos = mine * block + (
                            lax.broadcasted_iota(jnp.int32, expo.shape, 1) % block
                        )
                        expo = jnp.where(key_pos <= query_pos, expo, 0.0)
                    tot[:, cols] += jnp.sum(expo.reshape(pair // 8, 8, tile), axis=0)
                    acc[:, cols] += lax.dot_general(
                        values,
                        expo.astype(bf16),
                        (((0,), (0,)), ((), ())),
                        preferred_element_type=f32,
                    )

            def body(j, _):
                step(j, False)
                return 0

            lax.fori_loop(0, mine // 2, body, 0)
            step(mine // 2, True)
            total = jnp.sum(tot[...], axis=0, keepdims=True)
            lse_ref[unit, :, :] = jnp.log(total)
            share = 1.0 / total
            for h in range(heads):
                cols = slice(h * block, (h + 1) * block)
                out = jnp.transpose(acc[:, cols] * share[:, cols]).astype(bf16)
                for i in range(per_half):
                    at = token_rows(half * per_half + i, seq, seqs, rows)
                    attn_ref[at : at + rows, h * hd : (h + 1) * hd] = out[
                        i * rows : (i + 1) * rows, :
                    ]


def attend(projected, kv_all, query_gain, cos2, sin2, loc, own, heads, pieces, seqs):
    rows = projected.shape[0]
    hd = query_gain.shape[0]
    units = 2 * seqs
    block = rows // units
    keys = kv_all.shape[0] * kv_all.shape[1] // seqs
    whole = lambda *shape: pl.BlockSpec(shape, lambda i, *_: (0,) * len(shape))
    f32, bf16 = jnp.float32, jnp.bfloat16
    return pl.pallas_call(
        functools.partial(attend_kernel, heads, pieces, seqs, hd**-0.5),
        grid_spec=pltpu.PrefetchScalarGridSpec(
            num_scalar_prefetch=2,
            grid=(1,),
            in_specs=[
                pl.BlockSpec((rows, heads * hd), lambda i, *_: (0, 0)),
                whole(*kv_all.shape),
                whole(1, hd),
                whole(*cos2.shape),
                whole(*sin2.shape),
            ],
            out_specs=[
                whole(rows, heads * hd),
                whole(units, 1, heads * block),
                whole(units, heads * block, hd),
            ],
            scratch_shapes=[
                pltpu.VMEM((seqs, keys, hd), bf16),
                pltpu.VMEM((seqs, keys, hd), bf16),
                pltpu.VMEM((hd, heads * block), f32),
                pltpu.VMEM((8, heads * block), f32),
            ],
        ),
        out_shape=(
            jax.ShapeDtypeStruct((rows, heads * hd), bf16),
            jax.ShapeDtypeStruct((units, 1, heads * block), f32),
            jax.ShapeDtypeStruct((units, heads * block, hd), bf16),
        ),
        compiler_params=pltpu.CompilerParams(vmem_limit_bytes=56 * 1024 * 1024),
        name="attend",
    )(loc, own, projected, kv_all, query_gain.reshape(1, hd), cos2, sin2)


def attend_back_kernel(
    heads, pieces, seqs, scale, loc_ref, own_ref, proj_ref, kv_ref, qs_ref, attn_ref, cot_ref,
    lse_ref, gain_ref, cos_ref, sin_ref, low_ref, dkv_ref, gg_ref, ks, vs, dk, dv, dq, cs, dl,
):
    f32, bf16 = jnp.float32, jnp.bfloat16
    hd = gain_ref.shape[-1]
    rows = proj_ref.shape[0] // (pieces * seqs)
    per_half = pieces // 2
    block = per_half * rows
    blocks = 2 * kv_ref.shape[0]
    pair = 2 * block
    tile = heads * block
    sort_blocks(loc_ref, kv_ref, ks, seqs, rows, pieces, hd, 0, blocks)
    sort_blocks(loc_ref, kv_ref, vs, seqs, rows, pieces, hd, hd, blocks)
    dk[...] = jnp.zeros_like(dk)
    dv[...] = jnp.zeros_like(dv)
    gain_total = jnp.zeros((1, hd), f32)
    ones = jnp.ones((8, hd), bf16)
    nt = (((1,), (1,)), ((), ()))
    for seq in range(seqs):
        for half in range(2):
            unit = seq * 2 + half
            for h in range(heads):
                for i in range(per_half):
                    at = token_rows(half * per_half + i, seq, seqs, rows)
                    to = slice(h * block + i * rows, h * block + (i + 1) * rows)
                    part = cot_ref[at : at + rows, h * hd : (h + 1) * hd]
                    cs[to, :] = part
                    prod = part.astype(f32) * attn_ref[
                        at : at + rows, h * hd : (h + 1) * hd
                    ].astype(f32)
                    dq[to, :] = prod
            for t in range(heads * block // tile):
                cols = slice(t * tile, (t + 1) * tile)
                prod = dq[cols, :]
                high = prod.astype(bf16)
                rest = (prod - high.astype(f32)).astype(bf16)
                dl[:, cols] = lax.dot_general(
                    ones, high, nt, preferred_element_type=f32
                ) + lax.dot_general(ones, rest, nt, preferred_element_type=f32)
            dq[...] = jnp.zeros_like(dq)
            mine = own_ref[half]

            def step(j, masked):
                at = pl.ds(j * pair, pair)
                keys = ks[seq, at, :]
                values = vs[seq, at, :]
                key_sum = jnp.zeros((pair, hd), f32)
                value_sum = jnp.zeros((pair, hd), f32)
                for t in range(heads * block // tile):
                    cols = slice(t * tile, (t + 1) * tile)
                    query = qs_ref[unit, cols, :]
                    cot = cs[cols, :]
                    scores = lax.dot_general(keys, query, nt, preferred_element_type=f32)
                    weights = jnp.exp2(
                        scores * (scale * LOG2E) - lse_ref[unit, :, cols] * LOG2E
                    )
                    if masked:
                        key_pos = j * pair + lax.broadcasted_iota(jnp.int32, weights.shape, 0)
                        query_pos = mine * block + (
                            lax.broadcasted_iota(jnp.int32, weights.shape, 1) % block
                        )
                        weights = jnp.where(key_pos <= query_pos, weights, 0.0)
                    prob_cot = lax.dot_general(values, cot, nt, preferred_element_type=f32)
                    low = (weights * (prob_cot - dl[0:1, cols])).astype(bf16)
                    value_sum = value_sum + jnp.dot(
                        weights.astype(bf16), cot, preferred_element_type=f32
                    )
                    key_sum = key_sum + jnp.dot(low, query, preferred_element_type=f32)
                    dq[cols, :] += lax.dot_general(
                        low, keys, (((0,), (0,)), ((), ())), preferred_element_type=f32
                    )
                dk[seq, at, :] += key_sum
                dv[seq, at, :] += value_sum

            def body(j, _):
                step(j, False)
                return 0

            lax.fori_loop(0, mine // 2, body, 0)
            step(mine // 2, True)
            for h in range(heads):
                for i in range(per_half):
                    piece = half * per_half + i
                    at = token_rows(piece, seq, seqs, rows)
                    grad, terms = head_norm_back(
                        proj_ref[at : at + rows, h * hd : (h + 1) * hd],
                        gain_ref[...],
                        cos_ref[piece * rows : (piece + 1) * rows, :],
                        sin_ref[piece * rows : (piece + 1) * rows, :],
                        dq[h * block + i * rows : h * block + (i + 1) * rows, :] * scale,
                    )
                    low_ref[at : at + rows, h * hd : (h + 1) * hd] = grad.astype(bf16)
                    gain_total = gain_total + jnp.sum(terms, axis=0, keepdims=True)
    gg_ref[...] = gain_total

    def unsort(b, _):
        loc = loc_ref[b]
        chunk, half = loc // 2, loc % 2
        for seq in range(seqs):
            for i in range(per_half):
                at = pl.ds(((half * per_half + i) * seqs + seq) * rows, rows)
                here = pl.ds(b * block + i * rows, rows)
                dkv_ref[chunk, at, 0:hd] = (dk[seq, here, :] * scale).astype(bf16)
                dkv_ref[chunk, at, hd : 2 * hd] = dv[seq, here, :].astype(bf16)
        return 0

    lax.fori_loop(0, blocks, unsort, 0)


def attend_back(
    projected, kv_all, rotated, attention, attention_cot, log_total, query_gain, cos2, sin2, loc,
    own, heads, pieces, seqs,
):
    rows, all_cols = projected.shape
    hd = query_gain.shape[0]
    units = 2 * seqs
    block = rows // units
    keys = kv_all.shape[0] * kv_all.shape[1] // seqs
    whole = lambda *shape: pl.BlockSpec(shape, lambda i, *_: (0,) * len(shape))
    f32, bf16 = jnp.float32, jnp.bfloat16
    return pl.pallas_call(
        functools.partial(attend_back_kernel, heads, pieces, seqs, hd**-0.5),
        grid_spec=pltpu.PrefetchScalarGridSpec(
            num_scalar_prefetch=2,
            grid=(1,),
            in_specs=[
                pl.BlockSpec((rows, heads * hd), lambda i, *_: (0, 0)),
                whole(*kv_all.shape),
                whole(*rotated.shape),
                whole(rows, heads * hd),
                whole(rows, heads * hd),
                whole(*log_total.shape),
                whole(1, hd),
                whole(*cos2.shape),
                whole(*sin2.shape),
            ],
            out_specs=[
                pl.BlockSpec((rows, heads * hd), lambda i, *_: (0, 0)),
                whole(*kv_all.shape),
                whole(1, hd),
            ],
            scratch_shapes=[
                pltpu.VMEM((seqs, keys, hd), bf16),
                pltpu.VMEM((seqs, keys, hd), bf16),
                pltpu.VMEM((seqs, keys, hd), f32),
                pltpu.VMEM((seqs, keys, hd), f32),
                pltpu.VMEM((heads * block, hd), f32),
                pltpu.VMEM((heads * block, hd), bf16),
                pltpu.VMEM((8, heads * block), f32),
            ],
        ),
        out_shape=(
            jax.ShapeDtypeStruct((rows, all_cols), bf16),
            jax.ShapeDtypeStruct(kv_all.shape, bf16),
            jax.ShapeDtypeStruct((1, hd), f32),
        ),
        compiler_params=pltpu.CompilerParams(vmem_limit_bytes=60 * 1024 * 1024),
        name="attend_back",
    )(
        loc, own, projected, kv_all, rotated, attention, attention_cot, log_total,
        query_gain.reshape(1, hd), cos2, sin2,
    )


def picks_of(slots, capacity):
    return lax.broadcasted_iota(jnp.int32, (capacity, slots.shape[1]), 0) == slots


def expert_kernel(
    capacity, slot_ref, weight_ref, x_ref, c_ref, gate_ref, up_ref, down_ref,
    rows_ref, cot_ref, act_ref, gate_cot, up_cot, out_parts, row_parts, wc_ref, w_sc, cot_sc,
):
    f32, bf16 = jnp.float32, jnp.bfloat16
    nt = (((1,), (1,)), ((), ()))
    tn = (((0,), (0,)), ((), ()))
    devices = x_ref.shape[0]
    picks = [picks_of(slot_ref[d], capacity) for d in range(devices)]
    spans = [slice(d * capacity, (d + 1) * capacity) for d in range(devices)]
    for d in range(devices):
        low = picks[d].astype(bf16)
        rows_ref[spans[d], :] = jnp.dot(low, x_ref[d], preferred_element_type=f32).astype(bf16)
        cot_sc[spans[d], :] = jnp.dot(low, c_ref[d], preferred_element_type=f32).astype(bf16)
        w_sc[spans[d], :] = jnp.sum(
            jnp.where(picks[d], weight_ref[d], 0.0), axis=1, keepdims=True
        )
    rows = rows_ref[...]
    gate = jnp.dot(rows, gate_ref[...], preferred_element_type=f32)
    up = jnp.dot(rows, up_ref[...], preferred_element_type=f32)
    sigmoid = jax.nn.sigmoid(gate)
    swish = gate * sigmoid
    activation = (swish * up).astype(bf16)
    act_ref[...] = activation
    cot_ref[...] = (w_sc[...] * cot_sc[...].astype(f32)).astype(bf16)
    act_cot = lax.dot_general(cot_ref[...], down_ref[...], nt, preferred_element_type=f32)
    low_gate = (act_cot * up * sigmoid * (1.0 + gate * (1.0 - sigmoid))).astype(bf16)
    low_up = (act_cot * swish).astype(bf16)
    gate_cot[...] = low_gate
    up_cot[...] = low_up
    produced = jnp.dot(activation, down_ref[...], preferred_element_type=f32).astype(bf16)
    for d in range(devices):
        made = produced[spans[d], :].astype(f32)
        share = jnp.sum(cot_sc[spans[d], :].astype(f32) * made, axis=1, keepdims=True)
        wc_ref[d] = jnp.sum(jnp.where(picks[d], share, 0.0), axis=0, keepdims=True)
        out_parts[d] = lax.dot_general(
            picks[d].astype(bf16),
            (w_sc[spans[d], :] * made).astype(bf16),
            tn,
            preferred_element_type=f32,
        ).astype(bf16)
    row_cot = lax.dot_general(low_gate, gate_ref[...], nt, preferred_element_type=f32)
    row_cot = row_cot + lax.dot_general(low_up, up_ref[...], nt, preferred_element_type=f32)
    row_cot = row_cot.astype(bf16)
    for d in range(devices):
        row_parts[d] = lax.dot_general(
            picks[d].astype(bf16), row_cot[spans[d], :], tn, preferred_element_type=f32
        ).astype(bf16)


def expert_pass(slots, weights, tokens_all, cot_all, gate_w, up_w, down_w, capacity, per_step):
    f32, bf16 = jnp.float32, jnp.bfloat16
    devices, tokens, width = tokens_all.shape
    hidden = gate_w.shape[1]
    rows = per_step * capacity
    total = devices * capacity
    lead = lambda *shape: pl.BlockSpec(shape, lambda i: (i,) + (0,) * (len(shape) - 1))
    fixed = lambda a: pl.BlockSpec(a.shape, lambda i: (0, 0), pipeline_mode=pl.Buffered(1))
    return pl.pallas_call(
        functools.partial(expert_kernel, capacity),
        grid=(devices // per_step,),
        in_specs=[
            lead(per_step, 1, tokens),
            lead(per_step, 1, tokens),
            lead(per_step, tokens, width),
            lead(per_step, tokens, width),
            fixed(gate_w),
            fixed(up_w),
            fixed(down_w),
        ],
        out_specs=[
            lead(rows, width),
            lead(rows, width),
            lead(rows, hidden),
            lead(rows, hidden),
            lead(rows, hidden),
            lead(per_step, tokens, width),
            lead(per_step, tokens, width),
            lead(per_step, 1, tokens),
        ],
        out_shape=[
            jax.ShapeDtypeStruct((total, width), bf16),
            jax.ShapeDtypeStruct((total, width), bf16),
            jax.ShapeDtypeStruct((total, hidden), bf16),
            jax.ShapeDtypeStruct((total, hidden), bf16),
            jax.ShapeDtypeStruct((total, hidden), bf16),
            jax.ShapeDtypeStruct((devices, tokens, width), bf16),
            jax.ShapeDtypeStruct((devices, tokens, width), bf16),
            jax.ShapeDtypeStruct((devices, 1, tokens), f32),
        ],
        scratch_shapes=[pltpu.VMEM((rows, 1), f32), pltpu.VMEM((rows, width), bf16)],
        compiler_params=pltpu.CompilerParams(vmem_limit_bytes=62 * 1024 * 1024),
        name="expert_pass",
    )(slots, weights, tokens_all, cot_all, gate_w, up_w, down_w)


def product_kernel(a_ref, *refs):
    n = len(refs) // 2
    for b_ref, o_ref in zip(refs[:n], refs[n:]):
        o_ref[0] = lax.dot_general(
            a_ref[...], b_ref[...], (((0,), (0,)), ((), ())), preferred_element_type=jnp.float32
        )


def column_products(a, others, block):
    rows, k = a.shape
    return pl.pallas_call(
        product_kernel,
        grid=(k // block,),
        in_specs=[pl.BlockSpec((rows, block), lambda i: (0, i))]
        + [
            pl.BlockSpec(b.shape, lambda i: (0, 0), pipeline_mode=pl.Buffered(1)) for b in others
        ],
        out_specs=[pl.BlockSpec((1, block, b.shape[1]), lambda i: (0, i, 0)) for b in others],
        out_shape=[jax.ShapeDtypeStruct((1, k, b.shape[1]), jnp.float32) for b in others],
        compiler_params=pltpu.CompilerParams(vmem_limit_bytes=60 * 1024 * 1024),
    )(a, *others)


def own_kernels():
    return lax.axis_size("ctx") == 8 and lax.axis_size("wsh") == 4


AXIS_NAMES = {WSH_AXES: "wsh", CTX_AXES: "ctx", ALL_AXES: ("ctx", "wsh")}


def gather(shards, axes_list, ident):
    if own_kernels():
        return transfer(["gather"] * len(shards), shards, axes_list, ident)
    return [lax.all_gather(x, AXIS_NAMES[axes], axis=0) for x, axes in zip(shards, axes_list)]


def scatter(parts, axes_list, ident):
    if own_kernels():
        return transfer(["scatter"] * len(parts), parts, axes_list, ident)
    return [
        lax.psum_scatter(x, AXIS_NAMES[axes], scatter_dimension=0, tiled=False).astype(jnp.float32)
        for x, axes in zip(parts, axes_list)
    ]


def exchange(pieces):
    return lax.all_to_all(pieces, ("ctx", "wsh"), split_axis=0, concat_axis=0, tiled=True)


def to_everyone(value, device_count):
    return exchange(jnp.broadcast_to(value[None], (device_count,) + value.shape))


def experts_plain(
    slot_mine, weight_mine, moe_all, cot_all, gate_w, up_w, down_w, capacity
):
    f32, bf16 = jnp.float32, jnp.bfloat16
    device_count, _, width = moe_all.shape
    picks = slot_mine[:, None, :] == jnp.arange(capacity, dtype=jnp.int32)[None, :, None]
    picks_low = picks.astype(bf16)
    slot_weight = jnp.sum(jnp.where(picks, weight_mine[:, None, :], 0.0), axis=-1)

    def take(everyone):
        return (
            jnp.einsum("dct,dtw->dcw", picks_low, everyone, preferred_element_type=f32)
            .astype(bf16)
            .reshape(device_count * capacity, width)
        )

    def put(rows):
        return jnp.einsum(
            "dct,dcw->dtw",
            picks_low,
            rows.reshape(device_count, capacity, width),
            preferred_element_type=f32,
        ).astype(bf16)

    rows_in = take(moe_all)
    cot_rows = take(cot_all).astype(f32)
    weight_rows = slot_weight.reshape(device_count * capacity, 1)
    route_cot = (weight_rows * cot_rows).astype(bf16)
    gate_pre = jnp.dot(rows_in, gate_w, preferred_element_type=f32)
    up_pre = jnp.dot(rows_in, up_w, preferred_element_type=f32)
    sigmoid = jax.nn.sigmoid(gate_pre)
    swish = gate_pre * sigmoid
    activation = (swish * up_pre).astype(bf16)
    produced = jnp.dot(activation, down_w, preferred_element_type=f32).astype(bf16).astype(f32)
    out_parts = put((weight_rows * produced).astype(bf16))
    slot_cot = jnp.sum(cot_rows * produced, axis=-1).reshape(device_count, capacity)
    cot_mine = jnp.sum(jnp.where(picks, slot_cot[:, :, None], 0.0), axis=1)
    down_grad = jnp.einsum("rf,rd->fd", activation, route_cot, preferred_element_type=f32)
    act_cot = jnp.einsum("rd,fd->rf", route_cot, down_w, preferred_element_type=f32)
    gate_cot = (act_cot * up_pre * sigmoid * (1.0 + gate_pre * (1.0 - sigmoid))).astype(bf16)
    up_cot = (act_cot * swish).astype(bf16)
    gate_grad = jnp.einsum("rd,rf->df", rows_in, gate_cot, preferred_element_type=f32)
    up_grad = jnp.einsum("rd,rf->df", rows_in, up_cot, preferred_element_type=f32)
    row_cot = jnp.einsum("rf,df->rd", gate_cot, gate_w, preferred_element_type=f32)
    row_cot = row_cot + jnp.einsum("rf,df->rd", up_cot, up_w, preferred_element_type=f32)
    return (
        out_parts,
        cot_mine,
        put(row_cot.astype(bf16)),
        gate_grad[None],
        up_grad[None],
        down_grad[None],
    )


def local(
    inputs,
    pair_map,
    norm_gain,
    query_weight,
    key_weight,
    value_weight,
    query_gain,
    key_gain,
    out_weight,
    moe_gain,
    router,
    expert_gate,
    expert_up,
    expert_down,
    expert_ids,
    dispatch_slot,
    cotangent,
):
    f32, bf16 = jnp.float32, jnp.bfloat16
    rows_dev, seq_count, width = inputs.shape
    ctx_count = lax.axis_size("ctx")
    wsh_count = lax.axis_size("wsh")
    device_count = ctx_count * wsh_count
    head_dim = query_gain.shape[0]
    group_rows = rows_dev * wsh_count
    block_len = group_rows // 2
    seq_len = group_rows * ctx_count
    tokens = rows_dev * seq_count
    group_tokens = tokens * wsh_count
    top_count = expert_ids.shape[-1]
    expert_count = router.shape[1]
    capacity = max(2, 3 * top_count * block_len // (2 * device_count))
    positions = positions_of(pair_map, seq_len, block_len, pair_map.shape[0])
    me_ctx = lax.axis_index("ctx")
    query_pos = lax.dynamic_slice_in_dim(positions, me_ctx * group_rows, group_rows, 0)
    cosine, sine_table = rope_tables(query_pos, head_dim)
    cos2 = jnp.concatenate([cosine, cosine], axis=1)
    sin2 = jnp.concatenate([-sine_table, sine_table], axis=1)
    block_ids = jnp.arange(2 * ctx_count, dtype=jnp.int32)
    blocks_by_loc = jnp.stack([pair_map, 2 * ctx_count - 1 - pair_map], axis=1).reshape(-1)
    loc = jnp.sum(
        jnp.where(blocks_by_loc[None, :] == block_ids[:, None], block_ids[None, :], 0), axis=1
    ).astype(jnp.int32)
    own_blocks = lax.dynamic_slice_in_dim(blocks_by_loc, 2 * me_ctx, 2, 0)

    inputs_low = inputs.transpose(1, 0, 2).reshape(tokens, width)
    inputs_f = inputs_low.astype(f32)
    cot_flat = cotangent.transpose(1, 0, 2).reshape(tokens, width)
    normed_f, inverse_one = rms_forward(inputs_f, norm_gain)
    q_cols, kv_cols = query_weight.shape[1], key_weight.shape[1]
    heads_loc = q_cols // head_dim
    qkv_shard = jnp.concatenate([query_weight, key_weight, value_weight], axis=1)
    qkv_full, normed_flat = gather([qkv_shard, normed_f.astype(bf16)], [CTX_AXES, WSH_AXES], 1)
    normed_flat = normed_flat.reshape(group_tokens, width)
    qkv_full = qkv_full.reshape(width, q_cols + 2 * kv_cols)
    out_full = lax.all_gather(out_weight.T, "ctx", axis=0, tiled=True)
    cot_low, qkv_full = lax.optimization_barrier((cot_flat.astype(bf16), qkv_full))
    cot_all = lax.all_gather(cot_low, ("ctx", "wsh"), axis=0)
    projected = jnp.dot(normed_flat, qkv_full, preferred_element_type=f32)
    kv_own = kv_prep(projected, key_gain, cos2, sin2, heads_loc, wsh_count, seq_count)
    (kv_all,) = gather([kv_own], [CTX_AXES], 3)

    attention, log_total, rotated = attend(
        projected, kv_all, query_gain, cos2, sin2, loc, own_blocks, heads_loc, wsh_count, seq_count
    )
    mixed = jnp.einsum("tc,dc->td", attention, out_full, preferred_element_type=f32)
    (mixed,) = scatter([mixed.astype(bf16).reshape(wsh_count, tokens, width)], [WSH_AXES], 4)
    residual = inputs_f + mixed

    def rows_first(value):
        return value.reshape(seq_count, rows_dev, width).transpose(1, 0, 2)

    moe_normed_f, inverse_two = rms_forward(residual, moe_gain)
    moe_flat = moe_normed_f.astype(bf16)
    (moe_all,) = gather([moe_flat], [ALL_AXES], 5)
    logits = jnp.dot(moe_flat, router, preferred_element_type=f32)
    route_ids = expert_ids.transpose(1, 0, 2).reshape(tokens, top_count)
    slots = dispatch_slot.transpose(1, 0, 2).reshape(tokens, top_count)
    expert_onehot = (
        route_ids[:, :, None] == jnp.arange(expert_count, dtype=jnp.int32)[None, None, :]
    )
    named = jnp.any(expert_onehot, axis=1)
    slot_dense = jnp.sum(jnp.where(expert_onehot, slots[:, :, None] + 1, 0), axis=1) - 1
    chosen_top = jnp.max(jnp.where(named, logits, MASKED), axis=-1, keepdims=True)
    chosen_exp = jnp.where(named, jnp.exp(jnp.where(named, logits - chosen_top, 0.0)), 0.0)
    weight_dense = chosen_exp / jnp.sum(chosen_exp, axis=-1, keepdims=True)
    routing = exchange(jnp.stack([slot_dense.astype(f32).T, weight_dense.T], axis=1))
    slot_mine = routing[:, 0, :].astype(jnp.int32)
    weight_mine = routing[:, 1, :]
    gate_w, up_w, down_w = (expert_gate[0], expert_up[0], expert_down[0])
    if capacity % 16 == 0:
        rows_in, route_cot, activation, gate_cot, up_cot, out_parts, row_parts, cot_mine = (
            expert_pass(
                slot_mine[:, None],
                weight_mine[:, None],
                moe_all,
                cot_all,
                gate_w,
                up_w,
                down_w,
                capacity,
                8,
            )
        )
        cot_mine = cot_mine[:, 0]
        gate_grad, up_grad = column_products(rows_in, [gate_cot, up_cot], 256)
        (down_grad,) = column_products(activation, [route_cot], 256)
    else:
        out_parts, cot_mine, row_parts, gate_grad, up_grad, down_grad = experts_plain(
            slot_mine, weight_mine, moe_all, cot_all, gate_w, up_w, down_w, capacity
        )
    weight_cot = exchange(cot_mine).T

    chosen_cot = weight_dense * (
        weight_cot - jnp.sum(weight_dense * weight_cot, axis=-1, keepdims=True)
    )
    out_parts, down_grad = lax.optimization_barrier((out_parts, down_grad))
    logit_cot = chosen_cot.astype(bf16)
    router_part = jnp.einsum("te,td->ed", logit_cot, moe_flat, preferred_element_type=f32)
    if own_kernels():
        row_sum, moe_sum, router_sum = scatter(
            [row_parts, out_parts, router_part.reshape(device_count, -1, 128)],
            [ALL_AXES, ALL_AXES, ALL_AXES],
            6,
        )
    else:
        row_sum, moe_sum = scatter([row_parts, out_parts], [ALL_AXES, ALL_AXES], 6)
        router_grad = lax.psum(router_part, ("ctx", "wsh")).T
    outputs = rows_first((residual + moe_sum).astype(bf16))
    normed_two_cot = (
        jnp.einsum("te,de->td", logit_cot, router, preferred_element_type=f32) + row_sum
    )
    residual_norm_cot, moe_gain_grad = rms_backward(
        residual, inverse_two, moe_gain, normed_two_cot
    )
    residual_cot = cot_flat + residual_norm_cot
    residual_low = residual_cot.astype(bf16)
    (residual_flat,) = gather([residual_low], [WSH_AXES], 8)
    residual_flat = residual_flat.reshape(group_tokens, width)

    out_grad = jnp.einsum("td,tc->dc", residual_flat, attention, preferred_element_type=f32).astype(
        bf16
    )
    out_weight_grad = lax.psum_scatter(out_grad, "ctx", scatter_dimension=0, tiled=True)
    out_weight_grad = out_weight_grad.astype(f32).T
    residual_flat, _ = lax.optimization_barrier((residual_flat, out_grad))
    attention_cot = jnp.einsum(
        "td,dc->tc", residual_flat, out_full, preferred_element_type=f32
    ).astype(bf16)
    low, kv_sums, query_gain_grad = attend_back(
        projected,
        kv_all,
        rotated,
        attention,
        attention_cot,
        log_total,
        query_gain,
        cos2,
        sin2,
        loc,
        own_blocks,
        heads_loc,
        wsh_count,
        seq_count,
    )
    kv_sums, gate_grad, up_grad = lax.optimization_barrier((kv_sums, gate_grad, up_grad))
    (kv_cot,) = scatter([kv_sums], [CTX_AXES], 9)
    low, key_gain_grad = kv_back(
        projected, kv_cot, key_gain, cos2, sin2, low, heads_loc, wsh_count, seq_count
    )
    summed = jnp.einsum("tq,cq->tc", low, qkv_full, preferred_element_type=f32)
    qkv_grad = jnp.einsum("tc,tq->cq", normed_flat, low, preferred_element_type=f32).astype(bf16)
    summed = summed.astype(bf16).reshape(wsh_count, tokens, width)
    qkv_grad = qkv_grad.reshape(ctx_count, width // ctx_count, q_cols + 2 * kv_cols)
    query_gain_grad = query_gain_grad.reshape(head_dim)
    key_gain_grad = key_gain_grad.reshape(head_dim)
    early = jnp.concatenate([moe_gain_grad, query_gain_grad, key_gain_grad])
    if own_kernels():
        lanes = 128
        early = early.reshape(-1, lanes)
        many = router_sum.shape[0]
        small = jnp.pad(
            jnp.concatenate([router_sum, early]), ((0, -(many + early.shape[0]) % 16), (0, 0))
        )
        qkv_grad, normed_cot, small = transfer(
            ["scatter", "scatter", "gather"],
            [qkv_grad, summed, small],
            [CTX_AXES, WSH_AXES, ALL_AXES],
            10,
        )
        router_grad = small[:, :many].reshape(expert_count, width).T
        early = jnp.sum(small[:, many : many + early.shape[0]], axis=0).reshape(-1)
    else:
        qkv_grad, normed_cot = scatter([qkv_grad, summed], [CTX_AXES, WSH_AXES], 10)
        early = jnp.sum(to_everyone(early, device_count), axis=0)
    input_norm_cot, norm_gain_grad = rms_backward(inputs_f, inverse_one, norm_gain, normed_cot)
    norm_gain_grad = jnp.sum(to_everyone(norm_gain_grad, device_count), axis=0)
    input_grad = residual_cot + input_norm_cot
    input_grad = rows_first(input_grad)
    return (
        outputs,
        input_grad,
        norm_gain_grad,
        qkv_grad[:, :q_cols],
        qkv_grad[:, q_cols : q_cols + kv_cols],
        qkv_grad[:, q_cols + kv_cols :],
        early[width : width + head_dim],
        early[width + head_dim :],
        out_weight_grad,
        early[:width],
        router_grad,
        gate_grad,
        up_grad,
        down_grad,
    )


def solution(mesh):
    return jax.shard_map(
        local,
        mesh=mesh,
        in_specs=(
            P(("ctx", "wsh"), None, None),
            P(),
            P(),
            P("ctx", "wsh"),
            P("ctx", "wsh"),
            P("ctx", "wsh"),
            P(),
            P(),
            P("wsh", "ctx"),
            P(),
            P(),
            P(("ctx", "wsh"), None, None),
            P(("ctx", "wsh"), None, None),
            P(("ctx", "wsh"), None, None),
            P(("ctx", "wsh"), None, None),
            P(("ctx", "wsh"), None, None),
            P(("ctx", "wsh"), None, None),
        ),
        out_specs=(
            P(("ctx", "wsh"), None, None),
            P(("ctx", "wsh"), None, None),
            P(),
            P("ctx", "wsh"),
            P("ctx", "wsh"),
            P("ctx", "wsh"),
            P(),
            P(),
            P("wsh", "ctx"),
            P(),
            P(),
            P(("ctx", "wsh"), None, None),
            P(("ctx", "wsh"), None, None),
            P(("ctx", "wsh"), None, None),
        ),
        check_vma=False,
    )
```
